8 devices in a mesh: dp: 2 (over z, y), tp: 4 (over x, core).
Axes of the slice: x: 2, y: 2, z: 1, core: 2. Of those that a mesh axis runs over, the one named last changes fastest.
Arguments:
- residual: float32 [512, 2560], P('dp'), parts along dimension 0
- norm_w: bfloat16 [2, 2560], replicated
- w_in: bfloat16 [2, 2560, 2, 5120], P(None, None, None, 'tp')
- conv_w: bfloat16 [2, 4, 5120], P(None, None, 'tp')
- conv_b: bfloat16 [2, 5120], P(None, 'tp')
- w_x: bfloat16 [2, 5120, 192], P(None, 'tp')
- w_dt: bfloat16 [2, 160, 5120], P(None, None, 'tp')
- b_dt: float32 [2, 5120], P(None, 'tp')
- a_log: float32 [2, 16, 5120], P(None, None, 'tp')
- d_skip: float32 [2, 5120], P(None, 'tp')
- w_out: bfloat16 [2, 5120, 2560], P(None, 'tp')
- conv_state: bfloat16 [2, 512, 3, 5120], P(None, 'dp', None, 'tp'), parts along dimension 1
- ssm_state: float32 [2, 512, 16, 5120], P(None, 'dp', None, 'tp'), parts along dimension 1
Outputs:
- output 1: float32 [512, 2560], P('dp'), parts along dimension 0
- output 2: bfloat16 [2, 512, 3, 5120], P(None, 'dp', None, 'tp'), parts along dimension 1
- output 3: float32 [2, 512, 16, 5120], P(None, 'dp', None, 'tp'), parts along dimension 1
There are 2 independent parts. The reference program is written for one: setup_inputs(seed, part) draws one part's arguments, and reference() takes and returns one part's arrays. A program takes and returns all parts, laid end to end along the dimension named above; an argument that names none is the same for every part.
All inputs are finite; a program needn't handle non-finite values.
Results may differ from the reference program's by a relative error of at most 0.0173252.
Values are sent between devices in bfloat16 or wider.
A program may use at most 1 GiB of HBM per device.

```python
import math
import jax
import jax.numpy as jnp
from jax import lax

D = 2560
INNER = 5120
STATE = 16
RANK = 160
CONV = 4
LAYERS = 2
BATCH = 256


def setup_inputs(seed: int = 0, part: int = 0) -> dict:
    root_key = jax.random.key(seed)
    shared = jax.random.split(root_key, 10)
    part_keys = jax.random.split(jax.random.fold_in(root_key, part), 3)
    proj_width = RANK + 2 * STATE
    residual = jax.random.normal(part_keys[0], (BATCH, D), jnp.float32)
    norm_w = jax.random.uniform(shared[0], (LAYERS, D), jnp.float32, 0.5, 1.5).astype(jnp.bfloat16)
    w_in = (jax.random.normal(shared[1], (LAYERS, D, 2, INNER), jnp.float32) * D ** -0.5).astype(jnp.bfloat16)
    conv_w = (0.5 * jax.random.normal(shared[2], (LAYERS, CONV, INNER), jnp.float32)).astype(jnp.bfloat16)
    conv_b = (0.3 * jax.random.normal(shared[3], (LAYERS, INNER), jnp.float32)).astype(jnp.bfloat16)
    w_x = (jax.random.normal(shared[4], (LAYERS, INNER, proj_width), jnp.float32) * INNER ** -0.5).astype(jnp.bfloat16)
    w_dt = (jax.random.normal(shared[5], (LAYERS, RANK, INNER), jnp.float32) * (0.25 * RANK ** -0.5)).astype(jnp.bfloat16)
    dt_init = jnp.exp(jax.random.uniform(shared[6], (LAYERS, INNER), jnp.float32, math.log(0.05), math.log(0.25)))
    b_dt = dt_init + jnp.log(-jnp.expm1(-dt_init))
    a_log = jax.random.uniform(shared[7], (LAYERS, STATE, INNER), jnp.float32, -0.7, 0.7)
    d_skip = jax.random.uniform(shared[8], (LAYERS, INNER), jnp.float32, 0.5, 1.5)
    w_out = (jax.random.normal(shared[9], (LAYERS, INNER, D), jnp.float32) * INNER ** -0.5).astype(jnp.bfloat16)
    conv_state = jax.random.normal(part_keys[1], (LAYERS, BATCH, CONV - 1, INNER), jnp.float32).astype(jnp.bfloat16)
    ssm_state = 0.5 * jax.random.normal(part_keys[2], (LAYERS, BATCH, STATE, INNER), jnp.float32)
    return {'residual': residual, 'norm_w': norm_w, 'w_in': w_in, 'conv_w': conv_w, 'conv_b': conv_b, 'w_x': w_x, 'w_dt': w_dt, 'b_dt': b_dt, 'a_log': a_log, 'd_skip': d_skip, 'w_out': w_out, 'conv_state': conv_state, 'ssm_state': ssm_state}


def rms_norm(vector, epsilon):
    return vector * lax.rsqrt(jnp.mean(vector * vector, axis=-1, keepdims=True) + epsilon)


def mamba_layer(residual, params):
    norm_w, w_in, conv_w, conv_b, w_x, w_dt, b_dt, a_log, d_skip, w_out, conv_state, ssm_state = params
    hidden = (rms_norm(residual, 1e-5) * norm_w.astype(jnp.float32)).astype(jnp.bfloat16)
    x_part = jnp.dot(hidden, w_in[:, 0, :], preferred_element_type=jnp.float32).astype(jnp.bfloat16)
    z_part = jnp.dot(hidden, w_in[:, 1, :], preferred_element_type=jnp.float32).astype(jnp.bfloat16)
    window = jnp.concatenate([conv_state, x_part[:, None, :]], axis=1)
    conv_pre = jnp.sum(window.astype(jnp.float32) * conv_w.astype(jnp.float32)[None], axis=1) + conv_b.astype(jnp.float32)
    x_conv = jax.nn.silu(conv_pre).astype(jnp.bfloat16)
    proj_sum = jnp.dot(x_conv, w_x, preferred_element_type=jnp.float32)
    dt_low = rms_norm(proj_sum[:, :RANK], 1e-6).astype(jnp.bfloat16)
    b_vec = rms_norm(proj_sum[:, RANK:RANK + STATE], 1e-6)
    c_vec = rms_norm(proj_sum[:, RANK + STATE:], 1e-6)
    dt_val = jax.nn.softplus(jnp.dot(dt_low, w_dt, preferred_element_type=jnp.float32) + b_dt)
    x_float = x_conv.astype(jnp.float32)
    decay_fac = jnp.exp(dt_val[:, None, :] * -jnp.exp(a_log)[None])
    new_ssm = decay_fac * ssm_state + (dt_val * x_float)[:, None, :] * b_vec[:, :, None]
    y_val = jnp.sum(new_ssm * c_vec[:, :, None], axis=1) + d_skip * x_float
    gated_y = (y_val * jax.nn.silu(z_part.astype(jnp.float32))).astype(jnp.bfloat16)
    out_sum = jnp.dot(gated_y, w_out, preferred_element_type=jnp.float32)
    return residual + out_sum, (window[:, 1:, :], new_ssm)


def reference(residual, norm_w, w_in, conv_w, conv_b, w_x, w_dt, b_dt, a_log, d_skip, w_out, conv_state, ssm_state):
    resid_out, cache_new = lax.scan(mamba_layer, residual, (norm_w, w_in, conv_w, conv_b, w_x, w_dt, b_dt, a_log, d_skip, w_out, conv_state, ssm_state))
    return resid_out, cache_new[0], cache_new[1]
```

```python
import functools
import math

import jax
import jax.numpy as jnp
from jax import lax
from jax.experimental import pallas as pl
from jax.experimental.pallas import tpu as pltpu
from jax.sharding import PartitionSpec as P

F32 = jnp.float32
BF16 = jnp.bfloat16
ANY = pl.BlockSpec(memory_space=pl.ANY)
VMEM = pl.BlockSpec(memory_space=pltpu.VMEM)
NCH = 256
SB = 16
LOG2E = math.log2(math.e)
VLIM = 62 * 2 ** 20


def silu(v):
    return v * jax.nn.sigmoid(v)


def expand_matrix():
    row = lax.broadcasted_iota(jnp.int32, (128, 512), 0)
    col = lax.broadcasted_iota(jnp.int32, (128, 512), 1)
    target = 2 * row + jnp.where(col < 256, 0, 257)
    return jnp.where(col == target, 1.0, 0.0).astype(BF16)


def in_kernel(layer, row0, rows, has_o, *refs):
    refs = list(refs)
    res_hbm = refs.pop(0)
    pieces = [refs.pop(0) for _ in range(4)] if has_o else None
    norm_w, w_in, conv_w, conv_b, w_x, conv_st = refs[:6]
    refs = refs[6:]
    if layer > 0 or row0 > 0:
        refs.pop(0)
    z_out, xc_out, p_out, conv_out = refs[:4]
    refs = refs[4:]
    r_out = refs.pop(0) if has_o else None
    wbuf, hx, rbuf, cbuf, xbuf, rsem, wsem, csem, osem = refs
    feat = rbuf.shape[1]
    nchunk = wbuf.shape[0]
    w_flat = w_in.reshape(w_in.shape[0], 2 * feat, w_in.shape[3])

    r_rows = rows if res_hbm.shape[0] == rows else res_hbm.shape[0]
    r_src = res_hbm if r_rows == rows else res_hbm.at[pl.ds(row0, rows)]
    r_copy = pltpu.make_async_copy(r_src, rbuf, rsem)
    r_copy.start()

    def w_copy(c):
        return pltpu.make_async_copy(w_flat.at[layer, :, pl.ds(c * NCH, NCH)], wbuf.at[c], wsem.at[c])

    w_copy(0).start()
    c_copy = pltpu.make_async_copy(conv_st.at[layer, :, pl.ds(row0, rows)], cbuf, csem)
    c_copy.start()
    for c in range(1, nchunk):
        w_copy(c).start()
    r_copy.wait()
    r = rbuf[...]
    if has_o:
        core = lax.rem(lax.axis_index('tp'), 2)
        half = feat // 2
        u, up, v, vp = pieces
        lo = pl.ds(pl.multiple_of(core * half, 128), half)
        hi = pl.ds(pl.multiple_of((1 - core) * half, 128), half)
        rbuf[:, lo] = rbuf[:, lo] + (u[...].astype(F32) + v[...].astype(F32))
        rbuf[:, hi] = rbuf[:, hi] + (up[...].astype(F32) + vp[...].astype(F32))
        pltpu.make_async_copy(rbuf, r_out, osem.at[0]).start()
        r = rbuf[...]
    inv = lax.rsqrt(jnp.mean(r * r, axis=-1, keepdims=True) + 1e-5)
    h = (r * inv * norm_w[layer:layer + 1, :].astype(F32)).astype(BF16)
    ex = expand_matrix()
    for j in range(feat // 128):
        e = jnp.dot(h[:, j * 128:(j + 1) * 128], ex, preferred_element_type=F32).astype(BF16)
        hx[0:rows, j * 256:(j + 1) * 256] = e[:, :256]
        hx[rows:2 * rows, j * 256:(j + 1) * 256] = e[:, 256:]
    c_copy.wait()
    pltpu.make_async_copy(cbuf.at[pl.ds(1, 2)], conv_out.at[layer, pl.ds(0, 2), pl.ds(row0, rows)], osem.at[1]).start()
    p_acc = jnp.zeros((rows, w_x.shape[1]), F32)
    for c in range(nchunk):
        w_copy(c).wait()
        sl = slice(c * NCH, (c + 1) * NCH)
        acc = jnp.dot(hx[...], wbuf[c], preferred_element_type=F32)
        x = acc[:rows].astype(BF16)
        z_out[:, sl] = acc[rows:].astype(BF16)
        xbuf[:, sl] = x
        cw = conv_w[layer, :, sl].astype(F32)
        pre = cbuf[0, :, sl].astype(F32) * cw[0:1] + cbuf[1, :, sl].astype(F32) * cw[1:2]
        pre = pre + cbuf[2, :, sl].astype(F32) * cw[2:3] + x.astype(F32) * cw[3:4]
        pre = pre + conv_b[layer:layer + 1, sl].astype(F32)
        xc = silu(pre).astype(BF16)
        xc_out[:, sl] = xc
        p_acc = p_acc + lax.dot_general(xc, w_x[layer, :, sl], (((1,), (1,)), ((), ())), preferred_element_type=F32)
    p_out[...] = p_acc.astype(BF16)
    x_copy = pltpu.make_async_copy(xbuf, conv_out.at[layer, 2, pl.ds(row0, rows)], osem.at[2])
    x_copy.start()
    x_copy.wait()
    pltpu.make_async_copy(cbuf.at[pl.ds(1, 2)], conv_out.at[layer, pl.ds(0, 2), pl.ds(row0, rows)], osem.at[1]).wait()
    if has_o:
        pltpu.make_async_copy(rbuf, r_out, osem.at[0]).wait()


def in_call(layer, row0, rows, residual, pieces, weights, conv_st, conv_prev):
    norm_w, w_in, conv_w, conv_b, w_x = weights
    has_o = pieces is not None
    feat = residual.shape[1]
    chan = w_in.shape[3]
    args = [residual] + (list(pieces) if has_o else []) + [norm_w, w_in, conv_w, conv_b, w_x, conv_st]
    specs = [ANY] + ([VMEM] * 4 if has_o else []) + [VMEM, ANY, VMEM, VMEM, VMEM, ANY]
    alias = {}
    if layer > 0 or row0 > 0:
        alias = {len(args): 3}
        args.append(conv_prev)
        specs.append(ANY)
    outs = [jax.ShapeDtypeStruct((rows, chan), BF16), jax.ShapeDtypeStruct((rows, chan), BF16),
            jax.ShapeDtypeStruct((rows, w_x.shape[1]), BF16), jax.ShapeDtypeStruct(conv_st.shape, BF16)]
    out_specs = [VMEM, VMEM, VMEM, ANY]
    if has_o:
        outs.append(jax.ShapeDtypeStruct((rows, feat), F32))
        out_specs.append(ANY)
    nchunk = chan // NCH
    return pl.pallas_call(
        functools.partial(in_kernel, layer, row0, rows, has_o),
        out_shape=outs, in_specs=specs, out_specs=out_specs, input_output_aliases=alias,
        scratch_shapes=[
            pltpu.VMEM((nchunk, 2 * feat, NCH), BF16),
            pltpu.VMEM((2 * rows, 2 * feat), BF16),
            pltpu.VMEM((rows, feat), F32),
            pltpu.VMEM((3, rows, chan), BF16),
            pltpu.VMEM((rows, chan), BF16),
            pltpu.SemaphoreType.DMA, pltpu.SemaphoreType.DMA((nchunk,)), pltpu.SemaphoreType.DMA,
            pltpu.SemaphoreType.DMA((3,)),
        ],
        compiler_params=pltpu.CompilerParams(vmem_limit_bytes=VLIM),
        cost_estimate=pl.CostEstimate(flops=rows * 2 * feat * 2 * chan * 2, bytes_accessed=20 * 2 ** 20, transcendentals=0),
        name=f"in{layer}r{row0}",
    )(*args)


def rms(v):
    return v * lax.rsqrt(jnp.mean(v * v, axis=-1, keepdims=True) + 1e-6)


def sublane_sums(parts):
    sub = lax.broadcasted_iota(jnp.int32, parts[0].shape, 0)
    for step in (4, 2, 1):
        keep = (sub & step) == 0
        half = len(parts) // 2
        parts = [jnp.where(keep, parts[k], parts[k + half])
                 + pltpu.roll(jnp.where(keep, parts[k + half], parts[k]), step, 0) if step == 4 else
                 jnp.where(keep, parts[k], parts[k + half])
                 + jnp.where(keep, pltpu.roll(parts[k], 8 - step, 0), pltpu.roll(parts[k + half], step, 0))
                 for k in range(half)]
    return parts[0]


def s_kernel(layer, row0, rows, aliased, *refs):
    (st, p0, p1, p2, p3, xc_ref, z_ref, w_dt, b_dt, a_log, d_skip, w_out) = refs[:12]
    refs = list(refs[12:])
    if aliased:
        refs.pop(0)
    st_out, mine, theirs = refs[:3]
    dt_s, dtx_s, bc_s, a_s, y_s, part, wo, wsem = refs[3:]
    step = pl.program_id(0)
    chan = dt_s.shape[1]
    rank = w_dt.shape[1]
    nst = a_s.shape[0]
    w_copy = pltpu.make_async_copy(w_out.at[layer], wo, wsem)

    @pl.when(step == 0)
    def _():
        w_copy.start()
        p = (p0[...].astype(F32) + p1[...].astype(F32)) + (p2[...].astype(F32) + p3[...].astype(F32))
        low = rms(p[:, :rank]).astype(BF16)
        pre = jnp.dot(low, w_dt[0], preferred_element_type=F32) + b_dt[layer:layer + 1, :]
        dt = jnp.maximum(pre, 0.0) + jnp.log1p(jnp.exp(-jnp.abs(pre)))
        dt_s[...] = dt
        dtx_s[...] = dt * xc_ref[...].astype(F32)
        bc_s[:, 0:nst] = rms(p[:, rank:rank + nst])
        bc_s[:, nst:2 * nst] = rms(p[:, rank + nst:])
        a_s[...] = -jnp.exp(a_log[0]) * LOG2E

    base = pl.multiple_of(step * SB, SB)
    sl = pl.ds(base, SB)
    dt = dt_s[sl, :]
    dtx = dtx_s[sl, :]
    bc = bc_s[sl, :]
    lane = lax.broadcasted_iota(jnp.int32, (nst, 128), 1)
    row = lax.broadcasted_iota(jnp.int32, (nst, 128), 0)
    a2 = a_s[...]
    tiles = chan // 128
    for b in range(SB):
        bcb = jnp.broadcast_to(bc[b:b + 1, :], (nst, 128))
        bcol = jnp.sum(jnp.where(lane == row, bcb, 0.0), axis=1, keepdims=True)
        ccol = jnp.sum(jnp.where(lane == row + nst, bcb, 0.0), axis=1, keepdims=True)
        s = jnp.exp2(dt[b:b + 1, :] * a2) * st[0, b] + dtx[b:b + 1, :] * bcol
        st_out[0, b] = s
        t = s * ccol
        part[b] = t[0:8] + t[8:16]
    for g in range(SB // 8):
        y_s[pl.ds(base + 8 * g, 8), :] = sublane_sums([part[8 * g + k] for k in range(8)])

    @pl.when(step == pl.num_programs(0) - 1)
    def _():
        y = y_s[...] + d_skip[layer:layer + 1, :] * xc_ref[...].astype(F32)
        yg = (y * silu(z_ref[...].astype(F32))).astype(BF16)
        core = lax.rem(lax.axis_index('tp'), 2)
        half = wo.shape[1] // 2
        w_copy.wait()
        mine[...] = jnp.dot(yg, wo[:, pl.ds(pl.multiple_of(core * half, 128), half)], preferred_element_type=F32)
        theirs[...] = jnp.dot(yg, wo[:, pl.ds(pl.multiple_of((1 - core) * half, 128), half)],
                              preferred_element_type=F32).astype(BF16)


def s_call(layer, row0, rows, state, p_list, xc, z, weights, prev):
    w_dt, b_dt, a_log, d_skip, w_out = weights
    chan = w_dt.shape[2]
    nst = a_log.shape[1]
    feat = w_out.shape[2]
    off = row0 // SB

    def whole(a):
        return pl.BlockSpec(a.shape, lambda i: (0,) * a.ndim)

    def layered(a):
        return pl.BlockSpec((1,) + a.shape[1:], lambda i: (layer,) + (0,) * (a.ndim - 1))

    st_spec = pl.BlockSpec((1, SB, nst, chan), lambda i: (layer, i + off, 0, 0))
    args = [state] + list(p_list) + [xc, z, w_dt, b_dt, a_log, d_skip, w_out]
    specs = [st_spec] + [whole(p) for p in p_list] + [whole(xc), whole(z), layered(w_dt), whole(b_dt), layered(a_log),
                                                     whole(d_skip), ANY]
    alias = {}
    if prev is not None:
        alias = {len(args): 0}
        args.append(prev)
        specs.append(ANY)
    return pl.pallas_call(
        functools.partial(s_kernel, layer, row0, rows, prev is not None),
        grid=(rows // SB,),
        out_shape=[jax.ShapeDtypeStruct(state.shape, F32), jax.ShapeDtypeStruct((rows, feat // 2), F32),
                   jax.ShapeDtypeStruct((rows, feat // 2), BF16)],
        in_specs=specs,
        out_specs=[st_spec, pl.BlockSpec((rows, feat // 2), lambda i: (0, 0)),
                   pl.BlockSpec((rows, feat // 2), lambda i: (0, 0))],
        input_output_aliases=alias,
        scratch_shapes=[
            pltpu.VMEM((rows, chan), F32), pltpu.VMEM((rows, chan), F32), pltpu.VMEM((rows, 128), F32),
            pltpu.VMEM((nst, chan), F32), pltpu.VMEM((rows, chan), F32), pltpu.VMEM((SB, 8, chan), F32),
            pltpu.VMEM(w_out.shape[1:], BF16), pltpu.SemaphoreType.DMA,
        ],
        compiler_params=pltpu.CompilerParams(vmem_limit_bytes=VLIM),
        cost_estimate=pl.CostEstimate(flops=rows * 8 * 10 ** 7, bytes_accessed=rows * 164 * 1024 + 8 * 2 ** 20,
                                      transcendentals=0),
        name=f"s{layer}r{row0}",
    )(*args)


def fin_kernel(r_ref, u, up, v, vp, out):
    core = lax.rem(lax.axis_index('tp'), 2)
    half = u.shape[1]
    lo = pl.ds(pl.multiple_of(core * half, 128), half)
    hi = pl.ds(pl.multiple_of((1 - core) * half, 128), half)
    out[:, lo] = r_ref[:, lo] + (u[...].astype(F32) + v[...].astype(F32))
    out[:, hi] = r_ref[:, hi] + (up[...].astype(F32) + vp[...].astype(F32))


def fin_call(r1, pieces):
    rows, feat = r1.shape
    blk = 64
    spec = pl.BlockSpec((blk, feat), lambda i: (i, 0))
    hspec = pl.BlockSpec((blk, feat // 2), lambda i: (i, 0))
    return pl.pallas_call(
        fin_kernel, grid=(rows // blk,), out_shape=jax.ShapeDtypeStruct(r1.shape, F32),
        in_specs=[spec] + [hspec] * 4, out_specs=spec, name="fin",
    )(r1, *pieces)


PART = [(0, 1), (1, 0), (2, 3), (3, 2)]
CROSS = [(0, 2), (2, 0), (1, 3), (3, 1)]
DIAG = [(0, 3), (3, 0), (1, 2), (2, 1)]


def exchange(mine, theirs):
    got = lax.ppermute(theirs, 'tp', PART)
    u = (mine + got.astype(F32)).astype(BF16)
    v = lax.ppermute(u, 'tp', CROSS)
    up = lax.ppermute(u, 'tp', PART)
    vp = lax.ppermute(v, 'tp', PART)
    return u, up, v, vp


def solution(mesh):
    def step(residual, norm_w, w_in, conv_w, conv_b, w_x, w_dt, b_dt, a_log, d_skip, w_out, conv_state, ssm_state):
        w_xt = jnp.transpose(w_x, (0, 2, 1))
        conv_t = jnp.transpose(conv_state, (0, 2, 1, 3))
        in_w = (norm_w, w_in, conv_w, conv_b, w_xt)
        s_w = (w_dt, b_dt, a_log, d_skip, w_out)
        rows = residual.shape[0]
        r = residual
        conv_out = None
        ssm_out = None
        pieces = None
        for layer in range(norm_w.shape[0]):
            got = in_call(layer, 0, rows, r, pieces, in_w, conv_t, conv_out)
            z, xc, p, conv_out = got[:4]
            if pieces is not None:
                r = got[4]
            p_list = [p, lax.ppermute(p, 'tp', PART), lax.ppermute(p, 'tp', CROSS), lax.ppermute(p, 'tp', DIAG)]
            ssm_out, mine, theirs = s_call(layer, 0, rows, ssm_state, p_list, xc, z, s_w, ssm_out)
            pieces = exchange(mine, theirs)
        out = fin_call(r, pieces)
        return out, jnp.transpose(conv_out, (0, 2, 1, 3)), ssm_out

    cache_spec = P(None, 'dp', None, 'tp')
    in_specs = (P('dp', None), P(None, None), P(None, None, None, 'tp'), P(None, None, 'tp'), P(None, 'tp'), P(None, 'tp', None), P(None, None, 'tp'), P(None, 'tp'), P(None, None, 'tp'), P(None, 'tp'), P(None, 'tp', None), cache_spec, cache_spec)
    out_specs = (P('dp', None), cache_spec, cache_spec)
    return jax.shard_map(step, mesh=mesh, in_specs=in_specs, out_specs=out_specs, check_vma=False)
```

```python
import functools
import math

import jax
import jax.numpy as jnp
from jax import lax
from jax.experimental import pallas as pl
from jax.experimental.pallas import tpu as pltpu
from jax.sharding import PartitionSpec as P

F32 = jnp.float32
BF16 = jnp.bfloat16
ANY = pl.BlockSpec(memory_space=pl.ANY)
VMEM = pl.BlockSpec(memory_space=pltpu.VMEM)
NCH = 256
SB = 16
HALF = 128
LOG2E = math.log2(math.e)
MESH = pl.DeviceIdType.MESH


def silu(v):
    return v * jax.nn.sigmoid(v)


def expand_matrix():
    row = lax.broadcasted_iota(jnp.int32, (128, 512), 0)
    col = lax.broadcasted_iota(jnp.int32, (128, 512), 1)
    target = 2 * row + jnp.where(col < 256, 0, 257)
    return jnp.where(col == target, 1.0, 0.0).astype(BF16)


def in_kernel(layer, has_o, *refs):
    refs = list(refs)
    res_hbm = refs.pop(0)
    pieces = [[refs.pop(0) for _ in range(4)] for _ in range(2)] if has_o else None
    norm_w, w_in, conv_w, conv_b, w_x, conv_st = refs[:6]
    refs = refs[6:]
    if layer > 0:
        refs.pop(0)
    z_out, xc_out, p_out, conv_out = refs[:4]
    refs = refs[4:]
    r_out = refs.pop(0) if has_o else None
    wbuf, hx, rbuf, cbuf, xbuf, rsem, wsem, csem, osem = refs
    rows, feat = rbuf.shape
    nchunk = wbuf.shape[0]
    w_flat = w_in.reshape(w_in.shape[0], 2 * feat, w_in.shape[3])

    r_copy = pltpu.make_async_copy(res_hbm, rbuf, rsem)
    c_copy = pltpu.make_async_copy(conv_st.at[layer], cbuf, csem)
    state_copy = pltpu.make_async_copy(cbuf.at[pl.ds(1, 2)], conv_out.at[layer, pl.ds(0, 2)], osem.at[1])
    x_copy = pltpu.make_async_copy(xbuf, conv_out.at[layer, 2], osem.at[2])

    def w_copy(c):
        return pltpu.make_async_copy(w_flat.at[layer, :, pl.ds(c * NCH, NCH)], wbuf.at[c], wsem.at[c])

    r_copy.start()
    w_copy(0).start()
    w_copy(1).start()
    r_copy.wait()
    c_copy.start()
    if has_o:
        core = lax.rem(lax.axis_index('tp'), 2)
        half = feat // 2
        lo = pl.ds(pl.multiple_of(core * half, 128), half)
        hi = pl.ds(pl.multiple_of((1 - core) * half, 128), half)
        for k, (u, up, v, vp) in enumerate(pieces):
            rs = slice(k * HALF, (k + 1) * HALF)
            rbuf[rs, lo] = rbuf[rs, lo] + (u[...].astype(F32) + v[...].astype(F32))
            rbuf[rs, hi] = rbuf[rs, hi] + (up[...].astype(F32) + vp[...].astype(F32))
        pltpu.make_async_copy(rbuf, r_out, osem.at[0]).start()
    r = rbuf[...]
    inv = lax.rsqrt(jnp.mean(r * r, axis=-1, keepdims=True) + 1e-5)
    h = (r * inv * norm_w[layer:layer + 1, :].astype(F32)).astype(BF16)
    ex = expand_matrix()
    for j in range(feat // 128):
        e = jnp.dot(h[:, j * 128:(j + 1) * 128], ex, preferred_element_type=F32).astype(BF16)
        hx[0:rows, j * 256:(j + 1) * 256] = e[:, :256]
        hx[rows:2 * rows, j * 256:(j + 1) * 256] = e[:, 256:]
    c_copy.wait()
    state_copy.start()
    p_acc = jnp.zeros((w_x.shape[1], rows), F32)
    for c in range(nchunk):
        w_copy(c).wait()
        if c + 2 < nchunk:
            w_copy(c + 2).start()
        sl = slice(c * NCH, (c + 1) * NCH)
        acc = jnp.dot(hx[...], wbuf[c], preferred_element_type=F32)
        x = acc[:rows].astype(BF16)
        z_out[:, sl] = acc[rows:].astype(BF16)
        xbuf[:, sl] = x
        cw = conv_w[layer, :, sl].astype(F32)
        pre = cbuf[0, :, sl].astype(F32) * cw[0:1] + cbuf[1, :, sl].astype(F32) * cw[1:2]
        pre = pre + cbuf[2, :, sl].astype(F32) * cw[2:3] + x.astype(F32) * cw[3:4]
        pre = pre + conv_b[layer:layer + 1, sl].astype(F32)
        xc = silu(pre).astype(BF16)
        xc_out[:, sl] = xc
        p_acc = p_acc + lax.dot_general(w_x[layer, :, sl], xc, (((1,), (1,)), ((), ())), preferred_element_type=F32)
    p_out[...] = p_acc.astype(BF16)
    x_copy.start()
    x_copy.wait()
    state_copy.wait()
    if has_o:
        pltpu.make_async_copy(rbuf, r_out, osem.at[0]).wait()


def in_call(layer, residual, pieces, weights, conv_st, conv_prev):
    norm_w, w_in, conv_w, conv_b, w_x = weights
    has_o = pieces is not None
    rows, feat = residual.shape
    chan = w_in.shape[3]
    flat = [a for half in pieces for a in half] if has_o else []
    args = [residual] + flat + [norm_w, w_in, conv_w, conv_b, w_x, conv_st]
    specs = [ANY] + [VMEM] * len(flat) + [VMEM, ANY, VMEM, VMEM, VMEM, ANY]
    alias = {}
    if layer > 0:
        alias = {len(args): 3}
        args.append(conv_prev)
        specs.append(ANY)
    outs = [pltpu.VMEM((rows, chan), BF16), pltpu.VMEM((rows, chan), BF16),
            pltpu.VMEM((w_x.shape[1], rows), BF16), jax.ShapeDtypeStruct(conv_st.shape, BF16)]
    out_specs = [VMEM, VMEM, VMEM, ANY]
    if has_o:
        outs.append(jax.ShapeDtypeStruct((rows, feat), F32))
        out_specs.append(ANY)
    nchunk = chan // NCH
    return pl.pallas_call(
        functools.partial(in_kernel, layer, has_o),
        out_shape=outs, in_specs=specs, out_specs=out_specs, input_output_aliases=alias,
        scratch_shapes=[
            pltpu.VMEM((nchunk, 2 * feat, NCH), BF16),
            pltpu.VMEM((2 * rows, 2 * feat), BF16),
            pltpu.VMEM((rows, feat), F32),
            pltpu.VMEM((3, rows, chan), BF16),
            pltpu.VMEM((rows, chan), BF16),
            pltpu.SemaphoreType.DMA, pltpu.SemaphoreType.DMA((nchunk,)), pltpu.SemaphoreType.DMA,
            pltpu.SemaphoreType.DMA((3,)),
        ],
        compiler_params=pltpu.CompilerParams(vmem_limit_bytes=40 * 2 ** 20),
        cost_estimate=pl.CostEstimate(flops=rows * 2 * feat * 2 * chan * 2, bytes_accessed=20 * 2 ** 20, transcendentals=0),
        name=f"in{layer}",
    )(*args)


def rms0(v):
    return v * lax.rsqrt(jnp.mean(v * v, axis=0, keepdims=True) + 1e-6)


def sublane_sums(parts):
    sub = lax.broadcasted_iota(jnp.int32, parts[0].shape, 0)
    for step in (4, 2, 1):
        keep = (sub & step) == 0
        half = len(parts) // 2
        parts = [jnp.where(keep, parts[k], parts[k + half])
                 + pltpu.roll(jnp.where(keep, parts[k + half], parts[k]), step, 0) if step == 4 else
                 jnp.where(keep, parts[k], parts[k + half])
                 + jnp.where(keep, pltpu.roll(parts[k], 8 - step, 0), pltpu.roll(parts[k + half], step, 0))
                 for k in range(half)]
    return parts[0]


def k_kernel(layer, pt, xc_ref, z_ref, w_dt, b_dt, a_log, d_skip, w_out, state,
             st, ua, ub, upa, upb, va, vpa,
             dt_s, dtx_s, bc_s, a_s, y_s, part, wo, mine, theirs, got, p_sw, p_cs, p_v,
             stsem, wsem, ssem, rsem):
    me = lax.axis_index('tp')
    core = lax.rem(me, 2)
    partner = me + 1 - 2 * core
    other = lax.rem(me + 2, 4)
    rows, chan = dt_s.shape
    rank = w_dt.shape[1]
    nst = a_s.shape[0]
    nblk = rows // SB

    barrier = pltpu.get_barrier_semaphore()
    for dev in (partner, other):
        pl.semaphore_signal(barrier, inc=1, device_id={'tp': dev}, device_id_type=MESH)

    def st_copy(i):
        rs = pl.ds(i * SB, SB)
        return pltpu.make_async_copy(state.at[layer, rs], st.at[rs], stsem.at[i])

    for i in range(nblk):
        st_copy(i).start()
    w_copy = pltpu.make_async_copy(w_out.at[layer], wo, wsem)
    w_copy.start()

    def send(src, dst, k, dev):
        return pltpu.make_async_remote_copy(src_ref=src, dst_ref=dst, send_sem=ssem.at[k], recv_sem=rsem.at[k],
                                            device_id={'tp': dev}, device_id_type=MESH)

    pl.semaphore_wait(barrier, 2)
    p1 = send(pt, p_sw, 0, partner)
    p1.start()
    a_s[...] = -jnp.exp(a_log[layer]) * LOG2E
    p1.wait_recv()
    p_cs[...] = (pt[...].astype(F32) + p_sw[...].astype(F32)).astype(BF16)
    p2 = send(p_cs, p_v, 1, other)
    p2.start()
    p2.wait_recv()
    p = p_cs[...].astype(F32) + p_v[...].astype(F32)
    low = rms0(p[:rank]).astype(BF16)
    pre = lax.dot_general(low, w_dt[layer], (((0,), (0,)), ((), ())), preferred_element_type=F32)
    pre = pre + b_dt[layer:layer + 1, :]
    dt = jnp.maximum(pre, 0.0) + jnp.log1p(jnp.exp(-jnp.abs(pre)))
    dt_s[...] = dt
    dtx_s[...] = dt * xc_ref[...].astype(F32)
    bc = jnp.concatenate([rms0(p[rank:rank + nst]), rms0(p[rank + nst:])], axis=0)
    bc_s[:, 0:2 * nst] = jnp.transpose(bc)

    lane = lax.broadcasted_iota(jnp.int32, (nst, 128), 1)
    row = lax.broadcasted_iota(jnp.int32, (nst, 128), 0)

    def block(i, carry):
        st_copy(i).wait()
        base = pl.multiple_of(i * SB, SB)
        sl = pl.ds(base, SB)
        dt = dt_s[sl, :]
        dtx = dtx_s[sl, :]
        bc = bc_s[sl, :]
        a2 = a_s[...]
        for b in range(SB):
            bcb = jnp.broadcast_to(bc[b:b + 1, :], (nst, 128))
            bcol = jnp.sum(jnp.where(lane == row, bcb, 0.0), axis=1, keepdims=True)
            ccol = jnp.sum(jnp.where(lane == row + nst, bcb, 0.0), axis=1, keepdims=True)
            s = jnp.exp2(dt[b:b + 1, :] * a2) * st[base + b] + dtx[b:b + 1, :] * bcol
            st[base + b] = s
            t = s * ccol
            part[b] = t[0:8] + t[8:16]
        for g in range(SB // 8):
            y_s[pl.ds(base + 8 * g, 8), :] = sublane_sums([part[8 * g + k] for k in range(8)])
        return carry

    half = wo.shape[1] // 2
    lo = pl.ds(pl.multiple_of(core * half, 128), half)
    hi = pl.ds(pl.multiple_of((1 - core) * half, 128), half)

    def project(k):
        rs = pl.ds(k * HALF, HALF)
        y = y_s[rs, :] + d_skip[layer:layer + 1, :] * xc_ref[rs, :].astype(F32)
        yg = (y * silu(z_ref[rs, :].astype(F32))).astype(BF16)
        theirs[k] = jnp.dot(yg, wo[:, hi], preferred_element_type=F32).astype(BF16)
        red = send(theirs.at[k], got.at[k], 2 + k, partner)
        red.start()
        mine[k] = jnp.dot(yg, wo[:, lo], preferred_element_type=F32)
        return red

    lax.fori_loop(0, nblk // 2, block, 0)
    w_copy.wait()
    red_a = project(0)
    lax.fori_loop(nblk // 2, 5 * nblk // 8, block, 0)
    red_a.wait_recv()
    ua[...] = (mine[0] + got[0].astype(F32)).astype(BF16)
    cross_a = send(ua, va, 4, other)
    cross_a.start()
    up_a = send(ua, upa, 5, partner)
    up_a.start()
    lax.fori_loop(5 * nblk // 8, nblk, block, 0)
    red_b = project(1)
    red_b.wait_recv()
    ub[...] = (mine[1] + got[1].astype(F32)).astype(BF16)
    up_b = send(ub, upb, 6, partner)
    up_b.start()
    cross_a.wait_recv()
    fwd_a = send(va, vpa, 7, partner)
    fwd_a.start()
    for c in (up_a, up_b, fwd_a):
        c.wait_recv()
    for c in (p1, p2, red_a, red_b, cross_a, up_a, up_b, fwd_a):
        c.wait_send()


def k_call(layer, pt, xc, z, weights, state):
    w_dt, b_dt, a_log, d_skip, w_out = weights
    rows, chan = xc.shape
    nst = a_log.shape[1]
    feat = w_out.shape[2]
    half = feat // 2
    piece = pltpu.VMEM((HALF, half), BF16)
    ins = [pltpu.with_memory_space_constraint(a, pltpu.VMEM) for a in (pt, xc, z)]
    return pl.pallas_call(
        functools.partial(k_kernel, layer),
        out_shape=[pltpu.VMEM((rows, nst, chan), F32)] + [piece] * 6,
        in_specs=[VMEM] * 7 + [ANY, ANY], out_specs=[VMEM] * 7,
        scratch_shapes=[
            pltpu.VMEM((rows, chan), F32), pltpu.VMEM((rows, chan), F32), pltpu.VMEM((rows, 128), F32),
            pltpu.VMEM((nst, chan), F32), pltpu.VMEM((rows, chan), F32), pltpu.VMEM((SB, 8, chan), F32),
            pltpu.VMEM((chan, feat), BF16), pltpu.VMEM((2, HALF, half), F32), pltpu.VMEM((2, HALF, half), BF16),
            pltpu.VMEM((2, HALF, half), BF16), pltpu.VMEM(pt.shape, BF16), pltpu.VMEM(pt.shape, BF16),
            pltpu.VMEM(pt.shape, BF16),
            pltpu.SemaphoreType.DMA((rows // SB,)), pltpu.SemaphoreType.DMA, pltpu.SemaphoreType.DMA((8,)),
            pltpu.SemaphoreType.DMA((8,)),
        ],
        compiler_params=pltpu.CompilerParams(vmem_limit_bytes=26 * 2 ** 20, collective_id=layer, has_side_effects=True),
        cost_estimate=pl.CostEstimate(flops=2 * 10 ** 10, bytes_accessed=28 * 2 ** 20, transcendentals=0),
        name=f"k{layer}",
    )(*ins, w_dt, b_dt, a_log, d_skip, w_out, state)


def w_kernel(layer, st, *refs):
    out, sem = refs[-2:]
    step = st.shape[0] // 8

    def copy(i):
        rs = pl.ds(i * step, step)
        return pltpu.make_async_copy(st.at[rs], out.at[layer, rs], sem.at[i])

    for i in range(8):
        copy(i).start()
    for i in range(8):
        copy(i).wait()


def w_call(layer, st, shape, prev):
    args = [pltpu.with_memory_space_constraint(st, pltpu.VMEM)]
    specs = [VMEM]
    alias = {}
    if prev is not None:
        alias = {1: 0}
        args.append(prev)
        specs.append(ANY)
    return pl.pallas_call(
        functools.partial(w_kernel, layer), out_shape=jax.ShapeDtypeStruct(shape, F32),
        in_specs=specs, out_specs=ANY, input_output_aliases=alias,
        scratch_shapes=[pltpu.SemaphoreType.DMA((8,))],
        compiler_params=pltpu.CompilerParams(vmem_limit_bytes=2 ** 20),
        cost_estimate=pl.CostEstimate(flops=2 * 10 ** 10, bytes_accessed=42 * 2 ** 20, transcendentals=0),
        name=f"w{layer}",
    )(*args)


def fin_kernel(r_ref, *refs):
    out = refs[-1]
    core = lax.rem(lax.axis_index('tp'), 2)
    half = out.shape[1] // 2
    lo = pl.ds(pl.multiple_of(core * half, 128), half)
    hi = pl.ds(pl.multiple_of((1 - core) * half, 128), half)
    for k in range(2):
        u, up, v, vp = refs[4 * k:4 * k + 4]
        rs = slice(k * HALF, (k + 1) * HALF)
        out[rs, lo] = r_ref[rs, lo] + (u[...].astype(F32) + v[...].astype(F32))
        out[rs, hi] = r_ref[rs, hi] + (up[...].astype(F32) + vp[...].astype(F32))


def fin_call(r1, pieces):
    return pl.pallas_call(
        fin_kernel, out_shape=jax.ShapeDtypeStruct(r1.shape, F32), in_specs=[VMEM] * 9, out_specs=VMEM,
        compiler_params=pltpu.CompilerParams(vmem_limit_bytes=16 * 2 ** 20), name="fin",
    )(r1, *pieces[0], *pieces[1])


PART = [(0, 1), (1, 0), (2, 3), (3, 2)]
CROSS = [(0, 2), (2, 0), (1, 3), (3, 1)]


def solution(mesh):
    def step(residual, norm_w, w_in, conv_w, conv_b, w_x, w_dt, b_dt, a_log, d_skip, w_out, conv_state, ssm_state):
        w_xt = jnp.transpose(w_x, (0, 2, 1))
        conv_t = jnp.transpose(conv_state, (0, 2, 1, 3))
        in_w = (norm_w, w_in, conv_w, conv_b, w_xt)
        s_w = (w_dt, b_dt, a_log, d_skip, w_out)
        r = residual
        conv_out = None
        ssm_out = None
        pieces = None
        for layer in range(norm_w.shape[0]):
            got = in_call(layer, r, pieces, in_w, conv_t, conv_out)
            z, xc, pt, conv_out = got[:4]
            if pieces is not None:
                r = got[4]
            st, ua, ub, upa, upb, va, vpa = k_call(layer, pt, xc, z, s_w, ssm_state)
            vb = lax.ppermute(ub, 'tp', CROSS)
            ssm_out = w_call(layer, st, ssm_state.shape, ssm_out)
            vpb = lax.ppermute(vb, 'tp', PART)
            pieces = ((ua, upa, va, vpa), (ub, upb, vb, vpb))
        out = fin_call(r, pieces)
        return out, jnp.transpose(conv_out, (0, 2, 1, 3)), ssm_out

    cache_spec = P(None, 'dp', None, 'tp')
    in_specs = (P('dp', None), P(None, None), P(None, None, None, 'tp'), P(None, None, 'tp'), P(None, 'tp'), P(None, 'tp', None), P(None, None, 'tp'), P(None, 'tp'), P(None, None, 'tp'), P(None, 'tp'), P(None, 'tp', None), cache_spec, cache_spec)
    out_specs = (P('dp', None), cache_spec, cache_spec)
    return jax.shard_map(step, mesh=mesh, in_specs=in_specs, out_specs=out_specs, check_vma=False)
```

```python
import functools
import math

import jax
import jax.numpy as jnp
from jax import lax
from jax.experimental import pallas as pl
from jax.experimental.pallas import tpu as pltpu
from jax.sharding import PartitionSpec as P

F32 = jnp.float32
BF16 = jnp.bfloat16
ANY = pl.BlockSpec(memory_space=pltpu.HBM)
VMEM = pl.BlockSpec(memory_space=pltpu.VMEM)
NCH = 256
SB = 16
HALF = 128
LOG2E = math.log2(math.e)
MESH = pl.DeviceIdType.MESH


def silu(v):
    return v * jax.nn.sigmoid(v)


def expand_matrix():
    row = lax.broadcasted_iota(jnp.int32, (128, 512), 0)
    col = lax.broadcasted_iota(jnp.int32, (128, 512), 1)
    target = 2 * row + jnp.where(col < 256, 0, 257)
    return jnp.where(col == target, 1.0, 0.0).astype(BF16)


def in_kernel(layer, has_o, *refs):
    refs = list(refs)
    res_hbm = refs.pop(0)
    pieces = [[refs.pop(0) for _ in range(4)] for _ in range(2)] if has_o else None
    norm_w, w_in, conv_w, conv_b, w_x, conv_st = refs[:6]
    refs = refs[6:]
    if layer > 0:
        refs = refs[2:]
    z_out, xc_out, p_out, conv_out = refs[:4]
    refs = refs[4:]
    r_out = refs.pop(0) if has_o else None
    wbuf, hx, hbuf, ex_s, p_acc, rbuf, cbuf, xbuf, rsem, wsem, csem, osem = refs
    rows, feat = rbuf.shape
    nchunk = wbuf.shape[0]
    w_flat = w_in.reshape(w_in.shape[0], 2 * feat, w_in.shape[3])

    r_copy = pltpu.make_async_copy(res_hbm, rbuf, rsem)
    c_copy = pltpu.make_async_copy(conv_st.at[layer], cbuf, csem)
    state_copy = pltpu.make_async_copy(cbuf.at[pl.ds(1, 2)], conv_out.at[layer, pl.ds(0, 2)], osem.at[1])
    x_copy = pltpu.make_async_copy(xbuf, conv_out.at[layer, 2], osem.at[2])

    def w_copy(c):
        cols = pl.ds(pl.multiple_of(c * NCH, NCH), NCH)
        return pltpu.make_async_copy(w_flat.at[layer, :, cols], wbuf.at[c], wsem.at[c])

    r_copy.start()
    w_copy(0).start()
    w_copy(1).start()
    ex_s[...] = expand_matrix()
    p_acc[...] = jnp.zeros_like(p_acc)
    r_copy.wait()
    c_copy.start()
    nw = norm_w[layer:layer + 1, :].astype(F32)
    half = feat // 2
    if has_o:
        core = lax.rem(lax.axis_index('tp'), 2)
        lo = pl.ds(pl.multiple_of(core * half, 128), half)
        hi = pl.ds(pl.multiple_of((1 - core) * half, 128), half)

        for k, (u, up, v, vp) in enumerate(pieces):
            def add(i, carry, k=k, u=u, up=up, v=v, vp=vp):
                src = pl.ds(pl.multiple_of(i * 32, 32), 32)
                dst = pl.ds(pl.multiple_of(i * 32, 32) + k * HALF, 32)
                rbuf[dst, lo] = rbuf[dst, lo] + (u[src, :].astype(F32) + v[src, :].astype(F32))
                rbuf[dst, hi] = rbuf[dst, hi] + (up[src, :].astype(F32) + vp[src, :].astype(F32))
                return carry

            lax.fori_loop(0, HALF // 32, add, 0)
        pltpu.make_async_copy(rbuf, r_out, osem.at[0]).start()

    def norm(i, carry):
        rs = pl.ds(pl.multiple_of(i * 32, 32), 32)
        r = rbuf[rs, :]
        inv = lax.rsqrt(jnp.mean(r * r, axis=-1, keepdims=True) + 1e-5)
        hbuf[rs, :] = (r * inv * nw).astype(BF16)
        return carry

    lax.fori_loop(0, rows // 32, norm, 0)

    def expand(j, carry):
        e = jnp.dot(hbuf[:, pl.ds(pl.multiple_of(j * 128, 128), 128)], ex_s[...], preferred_element_type=F32).astype(BF16)
        cols = pl.ds(pl.multiple_of(j * 256, 256), 256)
        hx[0:rows, cols] = e[:, :256]
        hx[rows:2 * rows, cols] = e[:, 256:]
        return carry

    lax.fori_loop(0, feat // 128, expand, 0)
    c_copy.wait()
    state_copy.start()

    def chunk(c, carry):
        w_copy(c).wait()

        @pl.when(c + 2 < nchunk)
        def _():
            w_copy(c + 2).start()

        sl = pl.ds(pl.multiple_of(c * NCH, NCH), NCH)
        acc = jnp.dot(hx[...], wbuf[c], preferred_element_type=F32)
        x = acc[:rows].astype(BF16)
        z_out[:, sl] = acc[rows:].astype(BF16)
        xbuf[:, sl] = x
        cw = conv_w[layer, :, sl].astype(F32)
        pre = cbuf[0, :, sl].astype(F32) * cw[0:1] + cbuf[1, :, sl].astype(F32) * cw[1:2]
        pre = pre + cbuf[2, :, sl].astype(F32) * cw[2:3] + x.astype(F32) * cw[3:4]
        pre = pre + conv_b[layer:layer + 1, sl].astype(F32)
        xc = silu(pre).astype(BF16)
        xc_out[:, sl] = xc
        p_acc[...] += lax.dot_general(w_x[layer, :, sl], xc, (((1,), (1,)), ((), ())), preferred_element_type=F32)
        return carry

    lax.fori_loop(0, nchunk, chunk, 0)
    x_copy.start()
    p_out[...] = p_acc[...].astype(BF16)
    x_copy.wait()
    state_copy.wait()
    if has_o:
        pltpu.make_async_copy(rbuf, r_out, osem.at[0]).wait()


def in_call(layer, residual, pieces, weights, conv_st, conv_prev, ssm_prev):
    norm_w, w_in, conv_w, conv_b, w_x = weights
    has_o = pieces is not None
    rows, feat = residual.shape
    chan = w_in.shape[3]
    flat = [a for half in pieces for a in half] if has_o else []
    args = [residual] + flat + [norm_w, w_in, conv_w, conv_b, w_x, conv_st]
    specs = [ANY] + [VMEM] * len(flat) + [VMEM, ANY, VMEM, VMEM, VMEM, ANY]
    alias = {}
    if layer > 0:
        alias = {len(args): 3}
        args += [conv_prev, ssm_prev]
        specs += [ANY, ANY]
    outs = [pltpu.VMEM((rows, chan), BF16), pltpu.VMEM((rows, chan), BF16),
            pltpu.VMEM((w_x.shape[1], rows), BF16), jax.ShapeDtypeStruct(conv_st.shape, BF16)]
    out_specs = [VMEM, VMEM, VMEM, ANY]
    if has_o:
        outs.append(jax.ShapeDtypeStruct((rows, feat), F32))
        out_specs.append(ANY)
    nchunk = chan // NCH
    return pl.pallas_call(
        functools.partial(in_kernel, layer, has_o),
        out_shape=outs, in_specs=specs, out_specs=out_specs, input_output_aliases=alias,
        scratch_shapes=[
            pltpu.VMEM((nchunk, 2 * feat, NCH), BF16),
            pltpu.VMEM((2 * rows, 2 * feat), BF16),
            pltpu.VMEM((rows, feat), BF16),
            pltpu.VMEM((128, 512), BF16),
            pltpu.VMEM((w_x.shape[1], rows), F32),
            pltpu.VMEM((rows, feat), F32),
            pltpu.VMEM((3, rows, chan), BF16),
            pltpu.VMEM((rows, chan), BF16),
            pltpu.SemaphoreType.DMA, pltpu.SemaphoreType.DMA((nchunk,)), pltpu.SemaphoreType.DMA,
            pltpu.SemaphoreType.DMA((3,)),
        ],
        compiler_params=pltpu.CompilerParams(vmem_limit_bytes=60 * 2 ** 20),
        cost_estimate=pl.CostEstimate(flops=rows * 2 * feat * 2 * chan * 2, bytes_accessed=20 * 2 ** 20, transcendentals=0),
        name=f"in{layer}",
    )(*args)


def rms0(v):
    return v * lax.rsqrt(jnp.mean(v * v, axis=0, keepdims=True) + 1e-6)


def sublane_sums(parts):
    sub = lax.broadcasted_iota(jnp.int32, parts[0].shape, 0)
    for step in (4, 2, 1):
        keep = (sub & step) == 0
        half = len(parts) // 2
        parts = [jnp.where(keep, parts[k], parts[k + half])
                 + pltpu.roll(jnp.where(keep, parts[k + half], parts[k]), step, 0) if step == 4 else
                 jnp.where(keep, parts[k], parts[k + half])
                 + jnp.where(keep, pltpu.roll(parts[k], 8 - step, 0), pltpu.roll(parts[k + half], step, 0))
                 for k in range(half)]
    return parts[0]


def k_kernel(layer, pt, xc_ref, z_ref, w_dt, b_dt, a_log, d_skip, w_out, state,
             st, ua, ub, upa, upb, va, vpa,
             dt_s, dtx_s, bc_s, a_s, y_s, part, wo, mine, theirs, got, p_sw, p_cs, p_v,
             stsem, wsem, ssem, rsem):
    me = lax.axis_index('tp')
    core = lax.rem(me, 2)
    partner = me + 1 - 2 * core
    other = lax.rem(me + 2, 4)
    rows, chan = dt_s.shape
    rank = w_dt.shape[1]
    nst = a_s.shape[0]
    nblk = rows // SB

    barrier = pltpu.get_barrier_semaphore()
    for dev in (partner, other):
        pl.semaphore_signal(barrier, inc=1, device_id={'tp': dev}, device_id_type=MESH)

    def st_copy(i):
        rs = pl.ds(i * SB, SB)
        return pltpu.make_async_copy(state.at[layer, rs], st.at[rs], stsem.at[i])

    for i in range(nblk):
        st_copy(i).start()
    w_copy = pltpu.make_async_copy(w_out.at[layer], wo, wsem)
    w_copy.start()

    def send(src, dst, k, dev):
        return pltpu.make_async_remote_copy(src_ref=src, dst_ref=dst, send_sem=ssem.at[k], recv_sem=rsem.at[k],
                                            device_id={'tp': dev}, device_id_type=MESH)

    pl.semaphore_wait(barrier, 2)
    p1 = send(pt, p_sw, 0, partner)
    p1.start()
    a_s[...] = -jnp.exp(a_log[layer]) * LOG2E
    p1.wait_recv()
    p_cs[...] = (pt[...].astype(F32) + p_sw[...].astype(F32)).astype(BF16)
    p2 = send(p_cs, p_v, 1, other)
    p2.start()
    p2.wait_recv()
    p = p_cs[...].astype(F32) + p_v[...].astype(F32)
    low = rms0(p[:rank]).astype(BF16)
    pre = lax.dot_general(low, w_dt[layer], (((0,), (0,)), ((), ())), preferred_element_type=F32)
    pre = pre + b_dt[layer:layer + 1, :]
    dt = jnp.maximum(pre, 0.0) + jnp.log1p(jnp.exp(-jnp.abs(pre)))
    dt_s[...] = dt
    dtx_s[...] = dt * xc_ref[...].astype(F32)
    bc = jnp.concatenate([rms0(p[rank:rank + nst]), rms0(p[rank + nst:])], axis=0)
    bc_s[:, 0:2 * nst] = jnp.transpose(bc)

    lane = lax.broadcasted_iota(jnp.int32, (nst, 128), 1)
    row = lax.broadcasted_iota(jnp.int32, (nst, 128), 0)
    half = wo.shape[1] // 2
    lo = pl.ds(pl.multiple_of(core * half, 128), half)
    hi = pl.ds(pl.multiple_of((1 - core) * half, 128), half)
    qrows = rows // 4
    per_q = nblk // 4

    def red(q):
        return send(theirs.at[q], got.at[q], 2 + q, partner)

    def part_of(q):
        u, up = ((ua, upa), (ub, upb))[q // 2]
        rs = pl.ds((q % 2) * qrows, qrows)
        return u.at[rs], up.at[rs]

    def cross(q):
        rs = pl.ds(q * qrows, qrows)
        return send(ua.at[rs], va.at[rs], 6 + q, other)

    def to_partner(q):
        u, up = part_of(q)
        return send(u, up, 8 + q, partner)

    def forward(q):
        rs = pl.ds(q * qrows, qrows)
        return send(va.at[rs], vpa.at[rs], 12 + q, partner)

    def reduce_quarter(q):
        red(q).wait_recv()
        u, _ = part_of(q)
        u[...] = (mine[q] + got[q].astype(F32)).astype(BF16)
        if q < 2:
            cross(q).start()
        to_partner(q).start()

    def block(i, carry):
        st_copy(i).wait()
        base = pl.multiple_of(i * SB, SB)
        sl = pl.ds(base, SB)
        ybase = pl.multiple_of(lax.rem(i, per_q) * SB, SB)
        dt = dt_s[sl, :]
        dtx = dtx_s[sl, :]
        bc = bc_s[sl, :]
        a2 = a_s[...]
        for b in range(SB):
            bcb = jnp.broadcast_to(bc[b:b + 1, :], (nst, 128))
            bcol = jnp.sum(jnp.where(lane == row, bcb, 0.0), axis=1, keepdims=True)
            ccol = jnp.sum(jnp.where(lane == row + nst, bcb, 0.0), axis=1, keepdims=True)
            s = jnp.exp2(dt[b:b + 1, :] * a2) * st[base + b] + dtx[b:b + 1, :] * bcol
            st[base + b] = s
            t = s * ccol
            part[b] = t[0:8] + t[8:16]
        for g in range(SB // 8):
            y_s[pl.ds(ybase + 8 * g, 8), :] = sublane_sums([part[8 * g + k] for k in range(8)])

        @pl.when(i == per_q - 1)
        def _():
            w_copy.wait()

        @pl.when(lax.rem(i, per_q) == per_q - 1)
        def _():
            q = i // per_q
            rs = pl.ds(pl.multiple_of(q * qrows, qrows), qrows)
            y = y_s[...] + d_skip[layer:layer + 1, :] * xc_ref[rs, :].astype(F32)
            yg = (y * silu(z_ref[rs, :].astype(F32))).astype(BF16)
            theirs[q] = jnp.dot(yg, wo[:, hi], preferred_element_type=F32).astype(BF16)
            red(q).start()
            mine[q] = jnp.dot(yg, wo[:, lo], preferred_element_type=F32)

        for q in range(3):
            @pl.when(i == (q + 1) * per_q + 1)
            def _(q=q):
                reduce_quarter(q)

        return carry

    lax.fori_loop(0, nblk, block, 0)
    reduce_quarter(3)
    for q in range(2):
        cross(q).wait_recv()
        forward(q).start()
    for q in range(4):
        to_partner(q).wait_recv()
    for q in range(2):
        forward(q).wait_recv()
    p1.wait_send()
    p2.wait_send()
    for q in range(4):
        red(q).wait_send()
        to_partner(q).wait_send()
    for q in range(2):
        cross(q).wait_send()
        forward(q).wait_send()


def k_call(layer, pt, xc, z, weights, state):
    w_dt, b_dt, a_log, d_skip, w_out = weights
    rows, chan = xc.shape
    nst = a_log.shape[1]
    feat = w_out.shape[2]
    half = feat // 2
    piece = pltpu.VMEM((HALF, half), BF16)
    ins = [pltpu.with_memory_space_constraint(a, pltpu.VMEM) for a in (pt, xc, z)]
    return pl.pallas_call(
        functools.partial(k_kernel, layer),
        out_shape=[pltpu.VMEM((rows, nst, chan), F32)] + [piece] * 6,
        in_specs=[VMEM] * 7 + [ANY, ANY], out_specs=[VMEM] * 7,
        scratch_shapes=[
            pltpu.VMEM((rows, chan), F32), pltpu.VMEM((rows, chan), F32), pltpu.VMEM((rows, 128), F32),
            pltpu.VMEM((nst, chan), F32), pltpu.VMEM((rows // 4, chan), F32), pltpu.VMEM((SB, 8, chan), F32),
            pltpu.VMEM((chan, feat), BF16), pltpu.VMEM((4, rows // 4, half), F32), pltpu.VMEM((4, rows // 4, half), BF16),
            pltpu.VMEM((4, rows // 4, half), BF16), pltpu.VMEM(pt.shape, BF16), pltpu.VMEM(pt.shape, BF16),
            pltpu.VMEM(pt.shape, BF16),
            pltpu.SemaphoreType.DMA((rows // SB,)), pltpu.SemaphoreType.DMA, pltpu.SemaphoreType.DMA((14,)),
            pltpu.SemaphoreType.DMA((14,)),
        ],
        compiler_params=pltpu.CompilerParams(vmem_limit_bytes=26 * 2 ** 20, collective_id=layer, has_side_effects=True),
        cost_estimate=pl.CostEstimate(flops=2 * 10 ** 10, bytes_accessed=28 * 2 ** 20, transcendentals=0),
        name=f"k{layer}",
    )(*ins, w_dt, b_dt, a_log, d_skip, w_out, state)


def w_kernel(layer, st, *refs):
    out, flag, sem = refs[-3:]
    flag[...] = jnp.zeros_like(flag)
    step = st.shape[0] // 8

    def copy(i):
        rs = pl.ds(i * step, step)
        return pltpu.make_async_copy(st.at[rs], out.at[layer, rs], sem.at[i])

    for i in range(8):
        copy(i).start()
    for i in range(8):
        copy(i).wait()


def w_call(layer, st, shape, prev):
    args = [pltpu.with_memory_space_constraint(st, pltpu.VMEM)]
    specs = [VMEM]
    alias = {}
    if prev is not None:
        alias = {1: 0}
        args.append(prev)
        specs.append(ANY)
    return pl.pallas_call(
        functools.partial(w_kernel, layer),
        out_shape=[jax.ShapeDtypeStruct(shape, F32), jax.ShapeDtypeStruct((8, 128), F32)],
        in_specs=specs, out_specs=[ANY, VMEM], input_output_aliases=alias,
        scratch_shapes=[pltpu.SemaphoreType.DMA((8,))],
        compiler_params=pltpu.CompilerParams(vmem_limit_bytes=2 ** 20),
        cost_estimate=pl.CostEstimate(flops=2 * 10 ** 10, bytes_accessed=42 * 2 ** 20, transcendentals=0),
        name=f"w{layer}",
    )(*args)


def fin_kernel(r_ref, *refs):
    out = refs[-1]
    core = lax.rem(lax.axis_index('tp'), 2)
    half = out.shape[1] // 2
    lo = pl.ds(pl.multiple_of(core * half, 128), half)
    hi = pl.ds(pl.multiple_of((1 - core) * half, 128), half)
    for k in range(2):
        u, up, v, vp = refs[4 * k:4 * k + 4]
        rs = slice(k * HALF, (k + 1) * HALF)
        out[rs, lo] = r_ref[rs, lo] + (u[...].astype(F32) + v[...].astype(F32))
        out[rs, hi] = r_ref[rs, hi] + (up[...].astype(F32) + vp[...].astype(F32))


def fin_call(r1, pieces):
    return pl.pallas_call(
        fin_kernel, out_shape=jax.ShapeDtypeStruct(r1.shape, F32), in_specs=[VMEM] * 9, out_specs=VMEM,
        compiler_params=pltpu.CompilerParams(vmem_limit_bytes=16 * 2 ** 20), name="fin",
    )(r1, *pieces[0], *pieces[1])


PART = [(0, 1), (1, 0), (2, 3), (3, 2)]
CROSS = [(0, 2), (2, 0), (1, 3), (3, 1)]


def solution(mesh):
    def step(residual, norm_w, w_in, conv_w, conv_b, w_x, w_dt, b_dt, a_log, d_skip, w_out, conv_state, ssm_state):
        w_xt = jnp.transpose(w_x, (0, 2, 1))
        conv_t = jnp.transpose(conv_state, (0, 2, 1, 3))
        in_w = (norm_w, w_in, conv_w, conv_b, w_xt)
        s_w = (w_dt, b_dt, a_log, d_skip, w_out)
        r = residual
        conv_out = None
        ssm_out = None
        pieces = None
        for layer in range(norm_w.shape[0]):
            got = in_call(layer, r, pieces, in_w, conv_t, conv_out, ssm_out)
            z, xc, pt, conv_out = got[:4]
            if pieces is not None:
                r = got[4]
            st, ua, ub, upa, upb, va, vpa = k_call(layer, pt, xc, z, s_w, ssm_state)
            vb = lax.ppermute(ub, 'tp', CROSS)
            ssm_out, flag = w_call(layer, st, ssm_state.shape, ssm_out)
            vb, _ = lax.optimization_barrier((vb, flag))
            vpb = lax.ppermute(vb, 'tp', PART)
            pieces = ((ua, upa, va, vpa), (ub, upb, vb, vpb))
        out = fin_call(r, pieces)
        return out, jnp.transpose(conv_out, (0, 2, 1, 3)), ssm_out

    cache_spec = P(None, 'dp', None, 'tp')
    in_specs = (P('dp', None), P(None, None), P(None, None, None, 'tp'), P(None, None, 'tp'), P(None, 'tp'), P(None, 'tp', None), P(None, None, 'tp'), P(None, 'tp'), P(None, None, 'tp'), P(None, 'tp'), P(None, 'tp', None), cache_spec, cache_spec)
    out_specs = (P('dp', None), cache_spec, cache_spec)
    return jax.shard_map(step, mesh=mesh, in_specs=in_specs, out_specs=out_specs, check_vma=False)
```

```python
import functools
import math

import jax
import jax.numpy as jnp
from jax import lax
from jax.experimental import pallas as pl
from jax.experimental.pallas import tpu as pltpu
from jax.sharding import PartitionSpec as P


F32 = jnp.float32
BF16 = jnp.bfloat16
ANY = pl.BlockSpec(memory_space=pltpu.HBM)
VMEM = pl.BlockSpec(memory_space=pltpu.VMEM)
NCH = 256
SB = 16
HALF = 128
LOG2E = math.log2(math.e)
MESH = pl.DeviceIdType.MESH


def silu(v):
    return v * jax.nn.sigmoid(v)


def expand_matrix():
    row = lax.broadcasted_iota(jnp.int32, (128, 512), 0)
    col = lax.broadcasted_iota(jnp.int32, (128, 512), 1)
    target = 2 * row + jnp.where(col < 256, 0, 257)
    return jnp.where(col == target, 1.0, 0.0).astype(BF16)


def in_kernel(layer, has_o, *refs):
    refs = list(refs)
    res_hbm = refs.pop(0)
    pieces = [[refs.pop(0) for _ in range(4)] for _ in range(2)] if has_o else None
    norm_w, w_in, conv_w, conv_b, w_x, conv_st = refs[:6]
    refs = refs[6:]
    if layer > 0:
        refs = refs[2:]
    z_out, xc_out, p_out, conv_out = refs[:4]
    refs = refs[4:]
    r_out = refs.pop(0) if has_o else None
    wbuf, hx, hbuf, ex_s, p_acc, rbuf, cbuf, xbuf, rsem, wsem, csem, osem, xsem = refs
    rows, feat = rbuf.shape
    nchunk = wbuf.shape[0]
    w_flat = w_in.reshape(w_in.shape[0], 2 * feat, w_in.shape[3])

    r_copy = pltpu.make_async_copy(res_hbm, rbuf, rsem)
    c_copy = pltpu.make_async_copy(conv_st.at[layer], cbuf, csem)
    state_copy = pltpu.make_async_copy(cbuf.at[pl.ds(1, 2)], conv_out.at[layer, pl.ds(0, 2)], osem.at[1])

    def cols_of(c):
        return pl.ds(pl.multiple_of(c * NCH, NCH), NCH)

    def x_copy(c):
        return pltpu.make_async_copy(xbuf.at[:, cols_of(c)], conv_out.at[layer, 2, :, cols_of(c)], xsem.at[c])

    def w_copy(c):
        cols = cols_of(c)
        return pltpu.make_async_copy(w_flat.at[layer, :, cols], wbuf.at[c], wsem.at[c])

    r_copy.start()
    w_copy(0).start()
    ex_s[...] = expand_matrix()
    p_acc[...] = jnp.zeros_like(p_acc)
    r_copy.wait()
    w_copy(1).start()
    c_copy.start()
    w_copy(2).start()
    nw = norm_w[layer:layer + 1, :].astype(F32)
    half = feat // 2
    if has_o:
        core = lax.rem(lax.axis_index('tp'), 2)
        lo = pl.ds(pl.multiple_of(core * half, 128), half)
        hi = pl.ds(pl.multiple_of((1 - core) * half, 128), half)

        for k, (u, up, v, vp) in enumerate(pieces):
            def add(i, carry, k=k, u=u, up=up, v=v, vp=vp):
                src = pl.ds(pl.multiple_of(i * 32, 32), 32)
                dst = pl.ds(pl.multiple_of(i * 32, 32) + k * HALF, 32)
                rbuf[dst, lo] = rbuf[dst, lo] + (u[src, :].astype(F32) + v[src, :].astype(F32))
                rbuf[dst, hi] = rbuf[dst, hi] + (up[src, :].astype(F32) + vp[src, :].astype(F32))
                return carry

            lax.fori_loop(0, HALF // 32, add, 0)
        pltpu.make_async_copy(rbuf, r_out, osem.at[0]).start()

    def norm(i, carry):
        rs = pl.ds(pl.multiple_of(i * 32, 32), 32)
        r = rbuf[rs, :]
        inv = lax.rsqrt(jnp.mean(r * r, axis=-1, keepdims=True) + 1e-5)
        hbuf[rs, :] = (r * inv * nw).astype(BF16)
        return carry

    lax.fori_loop(0, rows // 32, norm, 0)

    def expand(j, carry):
        for t in range(4):
            src = pl.ds(pl.multiple_of(j * 512 + t * 128, 128), 128)
            e = jnp.dot(hbuf[:, src], ex_s[...], preferred_element_type=F32).astype(BF16)
            cols = pl.ds(pl.multiple_of(j * 1024 + t * 256, 256), 256)
            hx[0:rows, cols] = e[:, :256]
            hx[rows:2 * rows, cols] = e[:, 256:]
        return carry

    lax.fori_loop(0, feat // 512, expand, 0)
    c_copy.wait()
    state_copy.start()

    def chunk(c, carry):
        w_copy(c).wait()

        @pl.when(c + 3 < nchunk)
        def _():
            w_copy(c + 3).start()

        sl = cols_of(c)
        acc = jnp.dot(hx[...], wbuf[c], preferred_element_type=F32)
        x = acc[:rows].astype(BF16)
        z_out[:, sl] = acc[rows:].astype(BF16)
        xbuf[:, sl] = x
        x_copy(c).start()
        cw = conv_w[layer, :, sl].astype(F32)
        pre = cbuf[0, :, sl].astype(F32) * cw[0:1] + cbuf[1, :, sl].astype(F32) * cw[1:2]
        pre = pre + cbuf[2, :, sl].astype(F32) * cw[2:3] + x.astype(F32) * cw[3:4]
        pre = pre + conv_b[layer:layer + 1, sl].astype(F32)
        xc = silu(pre).astype(BF16)
        xc_out[:, sl] = xc
        p_acc[...] += lax.dot_general(w_x[layer, :, sl], xc, (((1,), (1,)), ((), ())), preferred_element_type=F32)
        return carry

    lax.fori_loop(0, nchunk, chunk, 0)
    p_out[...] = p_acc[...].astype(BF16)
    for c in range(nchunk):
        x_copy(c).wait()
    state_copy.wait()
    if has_o:
        pltpu.make_async_copy(rbuf, r_out, osem.at[0]).wait()


def in_call(layer, residual, pieces, weights, conv_st, conv_prev, ssm_prev):
    norm_w, w_in, conv_w, conv_b, w_x = weights
    has_o = pieces is not None
    rows, feat = residual.shape
    chan = w_in.shape[3]
    flat = [a for half in pieces for a in half] if has_o else []
    args = [residual] + flat + [norm_w, w_in, conv_w, conv_b, w_x, conv_st]
    specs = [ANY] + [VMEM] * len(flat) + [VMEM, ANY, VMEM, VMEM, VMEM, ANY]
    alias = {}
    if layer > 0:
        alias = {len(args): 3}
        args += [conv_prev, ssm_prev]
        specs += [ANY, ANY]
    outs = [pltpu.VMEM((rows, chan), BF16), pltpu.VMEM((rows, chan), BF16),
            pltpu.VMEM((w_x.shape[1], rows), BF16), jax.ShapeDtypeStruct(conv_st.shape, BF16)]
    out_specs = [VMEM, VMEM, VMEM, ANY]
    if has_o:
        outs.append(jax.ShapeDtypeStruct((rows, feat), F32))
        out_specs.append(ANY)
    nchunk = chan // NCH
    return pl.pallas_call(
        functools.partial(in_kernel, layer, has_o),
        out_shape=outs, in_specs=specs, out_specs=out_specs, input_output_aliases=alias,
        scratch_shapes=[
            pltpu.VMEM((nchunk, 2 * feat, NCH), BF16),
            pltpu.VMEM((2 * rows, 2 * feat), BF16),
            pltpu.VMEM((rows, feat), BF16),
            pltpu.VMEM((128, 512), BF16),
            pltpu.VMEM((w_x.shape[1], rows), F32),
            pltpu.VMEM((rows, feat), F32),
            pltpu.VMEM((3, rows, chan), BF16),
            pltpu.VMEM((rows, chan), BF16),
            pltpu.SemaphoreType.DMA, pltpu.SemaphoreType.DMA((nchunk,)), pltpu.SemaphoreType.DMA,
            pltpu.SemaphoreType.DMA((2,)), pltpu.SemaphoreType.DMA((nchunk,)),
        ],
        compiler_params=pltpu.CompilerParams(vmem_limit_bytes=60 * 2 ** 20),
        cost_estimate=pl.CostEstimate(flops=rows * 2 * feat * 2 * chan * 2, bytes_accessed=20 * 2 ** 20, transcendentals=0),
    )(*args)


def rms0(v):
    return v * lax.rsqrt(jnp.mean(v * v, axis=0, keepdims=True) + 1e-6)


def sublane_sums(parts):
    sub = lax.broadcasted_iota(jnp.int32, parts[0].shape, 0)
    for step in (4, 2, 1):
        keep = (sub & step) == 0
        half = len(parts) // 2
        parts = [jnp.where(keep, parts[k], parts[k + half])
                 + pltpu.roll(jnp.where(keep, parts[k + half], parts[k]), step, 0) if step == 4 else
                 jnp.where(keep, parts[k], parts[k + half])
                 + jnp.where(keep, pltpu.roll(parts[k], 8 - step, 0), pltpu.roll(parts[k + half], step, 0))
                 for k in range(half)]
    return parts[0]


def k_kernel(layer, pt, xc_ref, z_ref, w_dt, b_dt, a_log, d_skip, w_out, state,
             st, ua, ub, upa, upb, va, vpa,
             dt_s, dtx_s, bc_s, a_s, y_s, part, wo, mine, theirs, got, p_sw, p_cs, p_v,
             stsem, wsem, ssem, rsem):
    me = lax.axis_index('tp')
    core = lax.rem(me, 2)
    partner = me + 1 - 2 * core
    other = lax.rem(me + 2, 4)
    rows, _ = dt_s.shape
    rank = w_dt.shape[1]
    nst = a_s.shape[0]
    nblk = rows // SB

    barrier = pltpu.get_barrier_semaphore()
    for dev in (partner, other):
        pl.semaphore_signal(barrier, inc=1, device_id={'tp': dev}, device_id_type=MESH)

    def st_copy(i):
        rs = pl.ds(i * SB, SB)
        return pltpu.make_async_copy(state.at[layer, rs], st.at[rs], stsem.at[i])

    w_copy = pltpu.make_async_copy(w_out.at[layer], wo, wsem)
    for i in range(nblk):
        if i == nblk // 4:
            w_copy.start()
        st_copy(i).start()

    def send(src, dst, k, dev):
        return pltpu.make_async_remote_copy(src_ref=src, dst_ref=dst, send_sem=ssem.at[k], recv_sem=rsem.at[k],
                                            device_id={'tp': dev}, device_id_type=MESH)

    pl.semaphore_wait(barrier, 2)
    p1 = send(pt, p_sw, 0, partner)
    p1.start()
    a_s[...] = -jnp.exp(a_log[layer]) * LOG2E
    p1.wait_recv()
    p_cs[...] = (pt[...].astype(F32) + p_sw[...].astype(F32)).astype(BF16)
    p2 = send(p_cs, p_v, 1, other)
    p2.start()
    p2.wait_recv()
    p = p_cs[...].astype(F32) + p_v[...].astype(F32)
    low = rms0(p[:rank]).astype(BF16)
    pre = lax.dot_general(low, w_dt[layer], (((0,), (0,)), ((), ())), preferred_element_type=F32)
    pre = pre + b_dt[layer:layer + 1, :]
    dt = jnp.maximum(pre, 0.0) + jnp.log1p(jnp.exp(-jnp.abs(pre)))
    dt_s[...] = dt
    dtx_s[...] = dt * xc_ref[...].astype(F32)
    bc = jnp.concatenate([rms0(p[rank:rank + nst]), rms0(p[rank + nst:])], axis=0)
    bc_s[:, 0:2 * nst] = jnp.transpose(bc)

    lane = lax.broadcasted_iota(jnp.int32, (nst, 128), 1)
    row = lax.broadcasted_iota(jnp.int32, (nst, 128), 0)
    half = wo.shape[1] // 2
    lo = pl.ds(pl.multiple_of(core * half, 128), half)
    hi = pl.ds(pl.multiple_of((1 - core) * half, 128), half)
    qrows = rows // 4
    per_q = nblk // 4

    def red(q):
        return send(theirs.at[q], got.at[q], 2 + q, partner)

    def part_of(q):
        u, up = ((ua, upa), (ub, upb))[q // 2]
        rs = pl.ds((q % 2) * qrows, qrows)
        return u.at[rs], up.at[rs]

    def cross(q):
        rs = pl.ds(q * qrows, qrows)
        return send(ua.at[rs], va.at[rs], 6 + q, other)

    def to_partner(q):
        u, up = part_of(q)
        return send(u, up, 8 + q, partner)

    def forward(q):
        rs = pl.ds(q * qrows, qrows)
        return send(va.at[rs], vpa.at[rs], 12 + q, partner)

    def reduce_quarter(q):
        red(q).wait_recv()
        u, _ = part_of(q)
        u[...] = (mine[q] + got[q].astype(F32)).astype(BF16)
        if q < 2:
            cross(q).start()
        to_partner(q).start()

    def block(i, carry):
        st_copy(i).wait()
        base = pl.multiple_of(i * SB, SB)
        sl = pl.ds(base, SB)
        ybase = pl.multiple_of(lax.rem(i, per_q) * SB, SB)
        dt = dt_s[sl, :]
        dtx = dtx_s[sl, :]
        bc = bc_s[sl, :]
        a2 = a_s[...]
        for b in range(SB):
            bcb = jnp.broadcast_to(bc[b:b + 1, :], (nst, 128))
            bcol = jnp.sum(jnp.where(lane == row, bcb, 0.0), axis=1, keepdims=True)
            ccol = jnp.sum(jnp.where(lane == row + nst, bcb, 0.0), axis=1, keepdims=True)
            s = jnp.exp2(dt[b:b + 1, :] * a2) * st[base + b] + dtx[b:b + 1, :] * bcol
            st[base + b] = s
            t = s * ccol
            part[b] = t[0:8] + t[8:16]
        for g in range(SB // 8):
            y_s[pl.ds(ybase + 8 * g, 8), :] = sublane_sums([part[8 * g + k] for k in range(8)])

        @pl.when(i == per_q - 1)
        def _():
            w_copy.wait()

        @pl.when(lax.rem(i, per_q) == per_q - 1)
        def _():
            q = i // per_q
            rs = pl.ds(pl.multiple_of(q * qrows, qrows), qrows)
            y = y_s[...] + d_skip[layer:layer + 1, :] * xc_ref[rs, :].astype(F32)
            yg = (y * silu(z_ref[rs, :].astype(F32))).astype(BF16)
            theirs[q] = jnp.dot(yg, wo[:, hi], preferred_element_type=F32).astype(BF16)
            red(q).start()
            mine[q] = jnp.dot(yg, wo[:, lo], preferred_element_type=F32)

        for q in range(3):
            @pl.when(i == (q + 1) * per_q + 1)
            def _(q=q):
                reduce_quarter(q)

        return carry

    lax.fori_loop(0, nblk, block, 0)
    reduce_quarter(3)
    for q in range(2):
        cross(q).wait_recv()
        forward(q).start()
    for q in range(4):
        to_partner(q).wait_recv()
    for q in range(2):
        forward(q).wait_recv()
    p1.wait_send()
    p2.wait_send()
    for q in range(4):
        red(q).wait_send()
        to_partner(q).wait_send()
    for q in range(2):
        cross(q).wait_send()
        forward(q).wait_send()


def k_call(layer, pt, xc, z, weights, state):
    w_dt, b_dt, a_log, d_skip, w_out = weights
    rows, chan = xc.shape
    nst = a_log.shape[1]
    feat = w_out.shape[2]
    half = feat // 2
    piece = pltpu.VMEM((HALF, half), BF16)
    ins = [pltpu.with_memory_space_constraint(a, pltpu.VMEM) for a in (pt, xc, z)]
    return pl.pallas_call(
        functools.partial(k_kernel, layer),
        out_shape=[pltpu.VMEM((rows, nst, chan), F32)] + [piece] * 6,
        in_specs=[VMEM] * 7 + [ANY, ANY], out_specs=[VMEM] * 7,
        scratch_shapes=[
            pltpu.VMEM((rows, chan), F32), pltpu.VMEM((rows, chan), F32), pltpu.VMEM((rows, 128), F32),
            pltpu.VMEM((nst, chan), F32), pltpu.VMEM((rows // 4, chan), F32), pltpu.VMEM((SB, 8, chan), F32),
            pltpu.VMEM((chan, feat), BF16), pltpu.VMEM((4, rows // 4, half), F32), pltpu.VMEM((4, rows // 4, half), BF16),
            pltpu.VMEM((4, rows // 4, half), BF16), pltpu.VMEM(pt.shape, BF16), pltpu.VMEM(pt.shape, BF16),
            pltpu.VMEM(pt.shape, BF16),
            pltpu.SemaphoreType.DMA((rows // SB,)), pltpu.SemaphoreType.DMA, pltpu.SemaphoreType.DMA((14,)),
            pltpu.SemaphoreType.DMA((14,)),
        ],
        compiler_params=pltpu.CompilerParams(vmem_limit_bytes=26 * 2 ** 20, collective_id=layer, has_side_effects=True),
        cost_estimate=pl.CostEstimate(flops=2 * 10 ** 10, bytes_accessed=28 * 2 ** 20, transcendentals=0),
    )(*ins, w_dt, b_dt, a_log, d_skip, w_out, state)


def w_kernel(layer, st, *refs):
    out, sem = refs[-2:]
    step = st.shape[0] // 8

    def copy(i):
        rs = pl.ds(i * step, step)
        return pltpu.make_async_copy(st.at[rs], out.at[layer, rs], sem.at[i])

    for i in range(8):
        copy(i).start()
    for i in range(8):
        copy(i).wait()


def w_call(layer, st, shape, prev):
    args = [pltpu.with_memory_space_constraint(st, pltpu.VMEM)]
    specs = [VMEM]
    alias = {}
    if prev is not None:
        alias = {1: 0}
        args.append(prev)
        specs.append(ANY)
    return pl.pallas_call(
        functools.partial(w_kernel, layer),
        out_shape=jax.ShapeDtypeStruct(shape, F32), in_specs=specs, out_specs=ANY, input_output_aliases=alias,
        scratch_shapes=[pltpu.SemaphoreType.DMA((8,))],
        compiler_params=pltpu.CompilerParams(vmem_limit_bytes=2 ** 20),
        cost_estimate=pl.CostEstimate(flops=2 * 10 ** 10, bytes_accessed=42 * 2 ** 20, transcendentals=0),
    )(*args)


def fin_kernel(r_ref, *refs):
    out = refs[-1]
    core = lax.rem(lax.axis_index('tp'), 2)
    half = out.shape[1] // 2
    lo = pl.ds(pl.multiple_of(core * half, 128), half)
    hi = pl.ds(pl.multiple_of((1 - core) * half, 128), half)
    for k in range(2):
        u, up, v, vp = refs[4 * k:4 * k + 4]
        rs = slice(k * HALF, (k + 1) * HALF)
        out[rs, lo] = r_ref[rs, lo] + (u[...].astype(F32) + v[...].astype(F32))
        out[rs, hi] = r_ref[rs, hi] + (up[...].astype(F32) + vp[...].astype(F32))


def fin_call(r1, pieces):
    return pl.pallas_call(
        fin_kernel, out_shape=jax.ShapeDtypeStruct(r1.shape, F32), in_specs=[VMEM] * 9, out_specs=VMEM,
        compiler_params=pltpu.CompilerParams(vmem_limit_bytes=16 * 2 ** 20), name="fin",
    )(r1, *pieces[0], *pieces[1])


PART = [(0, 1), (1, 0), (2, 3), (3, 2)]
CROSS = [(0, 2), (2, 0), (1, 3), (3, 1)]


def solution(mesh):
    def step(residual, norm_w, w_in, conv_w, conv_b, w_x, w_dt, b_dt, a_log, d_skip, w_out, conv_state, ssm_state):
        w_xt = jnp.transpose(w_x, (0, 2, 1))
        conv_t = jnp.transpose(conv_state, (0, 2, 1, 3))
        in_w = (norm_w, w_in, conv_w, conv_b, w_xt)
        s_w = (w_dt, b_dt, a_log, d_skip, w_out)
        r = residual
        conv_out = None
        ssm_out = None
        pieces = None
        for layer in range(norm_w.shape[0]):
            got = in_call(layer, r, pieces, in_w, conv_t, conv_out, ssm_out)
            z, xc, pt, conv_out = got[:4]
            if pieces is not None:
                r = got[4]
            st, ua, ub, upa, upb, va, vpa = k_call(layer, pt, xc, z, s_w, ssm_state)
            vb = lax.ppermute(ub, 'tp', CROSS)
            ssm_out = w_call(layer, st, ssm_state.shape, ssm_out)
            vpb = lax.ppermute(vb, 'tp', PART)
            pieces = ((ua, upa, va, vpa), (ub, upb, vb, vpb))
        out = fin_call(r, pieces)
        return out, jnp.transpose(conv_out, (0, 2, 1, 3)), ssm_out

    cache_spec = P(None, 'dp', None, 'tp')
    in_specs = (P('dp', None), P(None, None), P(None, None, None, 'tp'), P(None, None, 'tp'), P(None, 'tp'), P(None, 'tp', None), P(None, None, 'tp'), P(None, 'tp'), P(None, None, 'tp'), P(None, 'tp'), P(None, 'tp', None), cache_spec, cache_spec)
    out_specs = (P('dp', None), cache_spec, cache_spec)
    return jax.shard_map(step, mesh=mesh, in_specs=in_specs, out_specs=out_specs, check_vma=False)
```

```python
import functools
import math

import jax
import jax.numpy as jnp
from jax import lax
from jax.experimental import pallas as pl
from jax.experimental.pallas import tpu as pltpu
from jax.sharding import PartitionSpec as P


F32 = jnp.float32
BF16 = jnp.bfloat16
ANY = pl.BlockSpec(memory_space=pltpu.HBM)
VMEM = pl.BlockSpec(memory_space=pltpu.VMEM)
NCH = 256
SB = 16
HALF = 128
LOG2E = math.log2(math.e)
MESH = pl.DeviceIdType.MESH


def silu(v):
    return v * jax.nn.sigmoid(v)


def expand_matrix():
    row = lax.broadcasted_iota(jnp.int32, (128, 512), 0)
    col = lax.broadcasted_iota(jnp.int32, (128, 512), 1)
    target = 2 * row + jnp.where(col < 256, 0, 257)
    return jnp.where(col == target, 1.0, 0.0).astype(BF16)


def rms0(v):
    return v * lax.rsqrt(jnp.mean(v * v, axis=0, keepdims=True) + 1e-6)


def sublane_sums(parts):
    sub = lax.broadcasted_iota(jnp.int32, parts[0].shape, 0)
    for step in (4, 2, 1):
        keep = (sub & step) == 0
        half = len(parts) // 2
        parts = [jnp.where(keep, parts[k], parts[k + half])
                 + pltpu.roll(jnp.where(keep, parts[k + half], parts[k]), step, 0) if step == 4 else
                 jnp.where(keep, parts[k], parts[k + half])
                 + jnp.where(keep, pltpu.roll(parts[k], 8 - step, 0), pltpu.roll(parts[k + half], step, 0))
                 for k in range(half)]
    return parts[0]


def layer_kernel(layer, has_o, *refs):
    refs = list(refs)
    res = refs.pop(0)
    pieces = [refs.pop(0) for _ in range(7)] if has_o else None
    (norm_w, w_in, conv_w, conv_b, w_x, conv_st, w_dt, b_dt, a_log, d_skip, w_out, state) = refs[:12]
    refs = refs[12:]
    st, cw, ua, ub, upa, upb, va, vpa = refs[:8]
    refs = refs[8:]
    r_out = refs.pop(0) if has_o else None
    (wbuf, hx, hbuf, ex_s, p_acc, p_own, p_sw, p_cs, p_v, rbuf, cold, z_s, xc_s, dt_s, bc_s, a_s, y_s, part,
     mine_a, mine_b, theirs_a, theirs_b, got_a, got_b, vpb, lsem, wsem, stsem, osem, ssem, rsem) = refs
    _, feat = rbuf.shape
    nchunk = wbuf.shape[0]
    chan = z_s.shape[1]
    rank = w_dt.shape[1]
    nst = a_s.shape[0]
    nblk = HALF // SB
    half = feat // 2
    quarter = HALF // 2
    w_flat = w_in.reshape(w_in.shape[0], 2 * feat, w_in.shape[3])

    me = lax.axis_index('tp')
    core = lax.rem(me, 2)
    partner = me + 1 - 2 * core
    other = lax.rem(me + 2, 4)
    lo = pl.ds(pl.multiple_of(core * half, 128), half)
    hi = pl.ds(pl.multiple_of((1 - core) * half, 128), half)

    barrier = pltpu.get_barrier_semaphore()
    for dev in (partner, other):
        pl.semaphore_signal(barrier, inc=1, device_id={'tp': dev}, device_id_type=MESH)

    def send(src, dst, k, dev):
        return pltpu.make_async_remote_copy(src_ref=src, dst_ref=dst, send_sem=ssem.at[k], recv_sem=rsem.at[k],
                                            device_id={'tp': dev}, device_id_type=MESH)

    def cols_of(c):
        return pl.ds(pl.multiple_of(c * NCH, NCH), NCH)

    def half_rows(k):
        return pl.ds(k * HALF, HALF)

    def r_copy(k):
        return pltpu.make_async_copy(res.at[half_rows(k)], rbuf.at[half_rows(k)], lsem.at[k])

    old_copy = pltpu.make_async_copy(conv_st.at[layer, 0], cold, lsem.at[2])
    win_copy = pltpu.make_async_copy(conv_st.at[layer, pl.ds(1, 2)], cw.at[pl.ds(0, 2)], lsem.at[3])

    def w_copy(c):
        return pltpu.make_async_copy(w_flat.at[layer, :, cols_of(c)], wbuf.at[c], wsem.at[c])

    def st_copy(i):
        rs = pl.ds(i * SB, SB)
        return pltpu.make_async_copy(state.at[layer, rs], st.at[rs], stsem.at[i])

    def out_tile(j):
        return wbuf.at[j // 4, pl.ds(pl.multiple_of(lax.rem(j, 4) * chan, 128), chan)]

    def o_copy(j):
        return pltpu.make_async_copy(w_out.at[layer, :, cols_of(j)], out_tile(j), osem.at[j])

    r_copy(0).start()
    w_copy(0).start()
    r_copy(1).start()
    w_copy(1).start()
    old_copy.start()
    win_copy.start()
    w_copy(2).start()
    ex_s[...] = expand_matrix()
    a_s[...] = -jnp.exp(a_log[layer]) * LOG2E
    nw = norm_w[layer:layer + 1, :].astype(F32)
    pl.semaphore_wait(barrier, 2)
    relay = None
    if has_o:
        relay = send(pieces[6], vpb, 14, partner)
        relay.start()

    def p_first(k):
        return send(p_own.at[k], p_sw.at[k], k, partner)

    def p_second(k):
        return send(p_cs.at[k], p_v.at[k], 2 + k, other)

    def p_middle(k):
        p_first(k).wait_recv()
        p_cs[k] = (p_own[k].astype(F32) + p_sw[k].astype(F32)).astype(BF16)
        p_second(k).start()

    for k in range(2):
        r_copy(k).wait()
        if has_o:
            if k == 0:
                u, up, v, vp = pieces[0:4]
            else:
                u, up, v, vp = pieces[4], pieces[5], pieces[6], vpb
                relay.wait_recv()

            def add(i, carry, k=k, u=u, up=up, v=v, vp=vp):
                src = pl.ds(pl.multiple_of(i * 32, 32), 32)
                dst = pl.ds(pl.multiple_of(i * 32, 32) + k * HALF, 32)
                rbuf[dst, lo] = rbuf[dst, lo] + (u[src, :].astype(F32) + v[src, :].astype(F32))
                rbuf[dst, hi] = rbuf[dst, hi] + (up[src, :].astype(F32) + vp[src, :].astype(F32))
                return carry

            lax.fori_loop(0, HALF // 32, add, 0)
            pltpu.make_async_copy(rbuf.at[half_rows(k)], r_out.at[half_rows(k)], lsem.at[4 + k]).start()

        def norm(i, carry, k=k):
            off = pl.multiple_of(i * 32, 32)
            r = rbuf[pl.ds(off + k * HALF, 32), :]
            inv = lax.rsqrt(jnp.mean(r * r, axis=-1, keepdims=True) + 1e-5)
            hbuf[pl.ds(off, 32), :] = (r * inv * nw).astype(BF16)
            return carry

        lax.fori_loop(0, HALF // 32, norm, 0)

        def expand(j, carry):
            for t in range(4):
                src = pl.ds(pl.multiple_of(j * 512 + t * 128, 128), 128)
                e = jnp.dot(hbuf[:, src], ex_s[...], preferred_element_type=F32).astype(BF16)
                cols = pl.ds(pl.multiple_of(j * 1024 + t * 256, 256), 256)
                hx[0:HALF, cols] = e[:, :256]
                hx[HALF:2 * HALF, cols] = e[:, 256:]
            return carry

        lax.fori_loop(0, feat // 512, expand, 0)
        if k == 0:
            old_copy.wait()
            win_copy.wait()
        p_acc[...] = jnp.zeros_like(p_acc)

        def chunk(c, carry, k=k):
            if k == 0:
                w_copy(c).wait()

                @pl.when(c + 3 < nchunk)
                def _():
                    w_copy(c + 3).start()
            else:
                for t in range(3):
                    st_copy(3 * c + t).start()

            sl = cols_of(c)
            rs = half_rows(k)
            acc = jnp.dot(hx[...], wbuf[c], preferred_element_type=F32)
            x = acc[:HALF].astype(BF16)
            z_s[rs, sl] = acc[HALF:].astype(BF16)
            cw[2, rs, sl] = x
            taps = conv_w[layer, :, sl].astype(F32)
            pre = cold[rs, sl].astype(F32) * taps[0:1] + cw[0, rs, sl].astype(F32) * taps[1:2]
            pre = pre + cw[1, rs, sl].astype(F32) * taps[2:3] + x.astype(F32) * taps[3:4]
            pre = pre + conv_b[layer:layer + 1, sl].astype(F32)
            xc = silu(pre).astype(BF16)
            xc_s[rs, sl] = xc
            p_acc[...] += lax.dot_general(w_x[layer, :, sl], xc, (((1,), (1,)), ((), ())), preferred_element_type=F32)
            if k == 1:
                @pl.when(c < 2)
                def _():
                    for t in range(4):
                        o_copy(4 * c + t).start()

                @pl.when(c == 2)
                def _():
                    for t in range(2):
                        o_copy(8 + t).start()
                    p_middle(0)

            return carry

        lax.fori_loop(0, nchunk, chunk, 0)
        p_own[k] = p_acc[...].astype(BF16)
        p_first(k).start()
    st_copy(2 * nblk - 1).start()

    def red_a(q):
        return send(theirs_a.at[q], got_a.at[q], 4 + q, partner)

    red_b = send(theirs_b, got_b, 6, partner)

    def quarter_rows(q):
        return pl.ds(q * quarter, quarter)

    def cross(q):
        return send(ua.at[quarter_rows(q)], va.at[quarter_rows(q)], 7 + q, other)

    def up_a(q):
        return send(ua.at[quarter_rows(q)], upa.at[quarter_rows(q)], 9 + q, partner)

    up_b = send(ub, upb, 11, partner)

    def forward(q):
        return send(va.at[quarter_rows(q)], vpa.at[quarter_rows(q)], 12 + q, partner)

    def reduce_a(q):
        red_a(q).wait_recv()
        ua[quarter_rows(q), :] = (mine_a[q] + got_a[q].astype(F32)).astype(BF16)
        cross(q).start()
        up_a(q).start()

    lane = lax.broadcasted_iota(jnp.int32, (nst, 128), 1)
    row = lax.broadcasted_iota(jnp.int32, (nst, 128), 0)

    def gated(rs, y):
        y = y + d_skip[layer:layer + 1, :] * xc_s[rs, :].astype(F32)
        return (y * silu(z_s[rs, :].astype(F32))).astype(BF16)

    def project(yg, first, dst, dtype):
        for t in range(half // NCH):
            j = first * (half // NCH) + t
            dst[:, t * NCH:(t + 1) * NCH] = jnp.dot(yg, out_tile(j)[...], preferred_element_type=F32).astype(dtype)

    for k in range(2):
        p_second(k).wait_recv()
        p = p_cs[k].astype(F32) + p_v[k].astype(F32)
        low = rms0(p[:rank]).astype(BF16)
        pre = lax.dot_general(low, w_dt[layer], (((0,), (0,)), ((), ())), preferred_element_type=F32)
        pre = pre + b_dt[layer:layer + 1, :]
        dt_s[...] = jnp.maximum(pre, 0.0) + jnp.log1p(jnp.exp(-jnp.abs(pre)))
        bc = jnp.concatenate([rms0(p[rank:rank + nst]), rms0(p[rank + nst:])], axis=0)
        bc_s[:, 0:2 * nst] = jnp.transpose(bc)

        def block(i, carry, k=k):
            st_copy(i + k * nblk).wait()
            local = pl.multiple_of(i * SB, SB)
            base = local + k * HALF
            dt = dt_s[pl.ds(local, SB), :]
            dtx = dt * xc_s[pl.ds(base, SB), :].astype(F32)
            bc = bc_s[pl.ds(local, SB), :]
            a2 = a_s[...]
            for b in range(SB):
                bcb = jnp.broadcast_to(bc[b:b + 1, :], (nst, 128))
                bcol = jnp.sum(jnp.where(lane == row, bcb, 0.0), axis=1, keepdims=True)
                ccol = jnp.sum(jnp.where(lane == row + nst, bcb, 0.0), axis=1, keepdims=True)
                s = jnp.exp2(dt[b:b + 1, :] * a2) * st[base + b] + dtx[b:b + 1, :] * bcol
                st[base + b] = s
                t = s * ccol
                part[b] = t[0:8] + t[8:16]
            for g in range(SB // 8):
                y_s[pl.ds(local + 8 * g, 8), :] = sublane_sums([part[8 * g + n] for n in range(8)])

            if k == 0:
                @pl.when(i == 2)
                def _():
                    p_middle(1)

                @pl.when(i == nblk // 2 - 1)
                def _():
                    for j in range(feat // NCH):
                        o_copy(j).wait()

                @pl.when(lax.rem(i, nblk // 2) == nblk // 2 - 1)
                def _():
                    q = i // (nblk // 2)
                    rs = pl.ds(pl.multiple_of(q * quarter, quarter), quarter)
                    yg = gated(rs, y_s[rs, :])
                    project(yg, 1 - core, theirs_a.at[q], BF16)
                    red_a(q).start()
                    project(yg, core, mine_a.at[q], F32)

                @pl.when(i == nblk // 2 + 1)
                def _():
                    reduce_a(0)
            else:
                @pl.when(i == 1)
                def _():
                    reduce_a(1)

            return carry

        lax.fori_loop(0, nblk, block, 0)

    yg = gated(half_rows(1), y_s[...])
    project(yg, 1 - core, theirs_b, BF16)
    red_b.start()
    project(yg, core, mine_b, F32)
    cross(0).wait_recv()
    forward(0).start()
    red_b.wait_recv()
    ub[...] = (mine_b[...] + got_b[...].astype(F32)).astype(BF16)
    up_b.start()
    cross(1).wait_recv()
    forward(1).start()
    for q in range(2):
        up_a(q).wait_recv()
    up_b.wait_recv()
    for q in range(2):
        forward(q).wait_recv()
    for k in range(2):
        p_first(k).wait_send()
        p_second(k).wait_send()
        red_a(k).wait_send()
        cross(k).wait_send()
        up_a(k).wait_send()
        forward(k).wait_send()
    red_b.wait_send()
    up_b.wait_send()
    if has_o:
        relay.wait_send()
        for k in range(2):
            pltpu.make_async_copy(rbuf.at[half_rows(k)], r_out.at[half_rows(k)], lsem.at[4 + k]).wait()


def layer_call(layer, residual, pieces, weights, conv_st, state):
    norm_w, w_in, conv_w, conv_b, w_x, w_dt, b_dt, a_log, d_skip, w_out = weights
    has_o = pieces is not None
    rows, feat = residual.shape
    chan = w_in.shape[3]
    nst = a_log.shape[1]
    half = feat // 2
    nproj = w_x.shape[1]
    nchunk = chan // NCH
    flat = list(pieces) if has_o else []
    args = [residual] + flat + [norm_w, w_in, conv_w, conv_b, w_x, conv_st, w_dt, b_dt, a_log, d_skip, w_out, state]
    specs = [ANY] + [VMEM] * len(flat) + [VMEM, ANY, VMEM, VMEM, VMEM, ANY, VMEM, VMEM, VMEM, VMEM, ANY, ANY]
    piece = pltpu.VMEM((HALF, half), BF16)
    outs = [pltpu.VMEM((rows, nst, chan), F32), pltpu.VMEM((3, rows, chan), BF16)] + [piece] * 6
    out_specs = [VMEM] * 8
    if has_o:
        outs.append(jax.ShapeDtypeStruct((rows, feat), F32))
        out_specs.append(ANY)
    vm = pltpu.VMEM
    dma = pltpu.SemaphoreType.DMA
    quarter = HALF // 2
    return pl.pallas_call(
        functools.partial(layer_kernel, layer, has_o),
        out_shape=outs, in_specs=specs, out_specs=out_specs,
        scratch_shapes=[
            vm((nchunk, 2 * feat, NCH), BF16), vm((2 * HALF, 2 * feat), BF16), vm((HALF, feat), BF16), vm((128, 512), BF16),
            vm((nproj, HALF), F32), vm((2, nproj, HALF), BF16), vm((2, nproj, HALF), BF16), vm((2, nproj, HALF), BF16),
            vm((2, nproj, HALF), BF16), vm((rows, feat), F32), vm((rows, chan), BF16), vm((rows, chan), BF16),
            vm((rows, chan), BF16), vm((HALF, chan), F32), vm((HALF, 128), F32), vm((nst, chan), F32), vm((HALF, chan), F32),
            vm((SB, 8, chan), F32), vm((2, quarter, half), F32), vm((HALF, half), F32), vm((2, quarter, half), BF16),
            vm((HALF, half), BF16), vm((2, quarter, half), BF16), vm((HALF, half), BF16), vm((HALF, half), BF16),
            dma((6,)), dma((nchunk,)), dma((rows // SB,)), dma((feat // NCH,)), dma((15,)), dma((15,)),
        ],
        compiler_params=pltpu.CompilerParams(vmem_limit_bytes=34 * 2 ** 20, collective_id=layer, has_side_effects=True),
        cost_estimate=pl.CostEstimate(flops=2 * 10 ** 10, bytes_accessed=46 * 2 ** 20, transcendentals=0),
    )(*args)


def w_kernel(layer, st, cw, *refs):
    ssm_out, conv_out, sem = refs[-3:]
    step = st.shape[0] // 8

    def copy(i):
        rs = pl.ds(i * step, step)
        return pltpu.make_async_copy(st.at[rs], ssm_out.at[layer, rs], sem.at[i])

    c_copy = pltpu.make_async_copy(cw, conv_out.at[layer], sem.at[8])
    for i in range(8):
        copy(i).start()
    c_copy.start()
    for i in range(8):
        copy(i).wait()
    c_copy.wait()


def w_call(layer, st, cw, shapes, prev):
    args = [pltpu.with_memory_space_constraint(a, pltpu.VMEM) for a in (st, cw)]
    specs = [VMEM, VMEM]
    alias = {}
    if prev is not None:
        alias = {2: 0, 3: 1}
        args += list(prev)
        specs += [ANY, ANY]
    return pl.pallas_call(
        functools.partial(w_kernel, layer),
        out_shape=[jax.ShapeDtypeStruct(shapes[0], F32), jax.ShapeDtypeStruct(shapes[1], BF16)],
        in_specs=specs, out_specs=[ANY, ANY], input_output_aliases=alias,
        scratch_shapes=[pltpu.SemaphoreType.DMA((9,))],
        compiler_params=pltpu.CompilerParams(vmem_limit_bytes=2 ** 20),
        cost_estimate=pl.CostEstimate(flops=2 * 10 ** 10, bytes_accessed=42 * 2 ** 20, transcendentals=0),
    )(*args)


def fin_kernel(r_ref, *refs):
    out = refs[-1]
    core = lax.rem(lax.axis_index('tp'), 2)
    half = out.shape[1] // 2
    lo = pl.ds(pl.multiple_of(core * half, 128), half)
    hi = pl.ds(pl.multiple_of((1 - core) * half, 128), half)
    for k in range(2):
        u, up, v, vp = refs[4 * k:4 * k + 4]
        rs = slice(k * HALF, (k + 1) * HALF)
        out[rs, lo] = r_ref[rs, lo] + (u[...].astype(F32) + v[...].astype(F32))
        out[rs, hi] = r_ref[rs, hi] + (up[...].astype(F32) + vp[...].astype(F32))


def fin_call(r1, pieces):
    return pl.pallas_call(
        fin_kernel, out_shape=jax.ShapeDtypeStruct(r1.shape, F32), in_specs=[VMEM] * 9, out_specs=VMEM,
        compiler_params=pltpu.CompilerParams(vmem_limit_bytes=16 * 2 ** 20), name="fin",
    )(r1, *pieces[0], *pieces[1])


PART = [(0, 1), (1, 0), (2, 3), (3, 2)]
CROSS = [(0, 2), (2, 0), (1, 3), (3, 1)]


def solution(mesh):
    def step(residual, norm_w, w_in, conv_w, conv_b, w_x, w_dt, b_dt, a_log, d_skip, w_out, conv_state, ssm_state):
        w_xt = jnp.transpose(w_x, (0, 2, 1))
        conv_t = jnp.transpose(conv_state, (0, 2, 1, 3))
        weights = (norm_w, w_in, conv_w, conv_b, w_xt, w_dt, b_dt, a_log, d_skip, w_out)
        shapes = (ssm_state.shape, conv_t.shape)
        r = residual
        written = None
        pieces = None
        for layer in range(norm_w.shape[0]):
            got = layer_call(layer, r, pieces, weights, conv_t, ssm_state)
            st, cw, ua, ub, upa, upb, va, vpa = got[:8]
            if pieces is not None:
                r = got[8]
            vb = lax.ppermute(ub, 'tp', CROSS)
            written = w_call(layer, st, cw, shapes, written)
            pieces = (ua, upa, va, vpa, ub, upb, vb)
        pieces = (pieces[:4], pieces[4:] + (lax.ppermute(pieces[6], 'tp', PART),))
        ssm_out, conv_out = written
        out = fin_call(r, pieces)
        return out, jnp.transpose(conv_out, (0, 2, 1, 3)), ssm_out

    cache_spec = P(None, 'dp', None, 'tp')
    in_specs = (P('dp', None), P(None, None), P(None, None, None, 'tp'), P(None, None, 'tp'), P(None, 'tp'), P(None, 'tp', None), P(None, None, 'tp'), P(None, 'tp'), P(None, None, 'tp'), P(None, 'tp'), P(None, 'tp', None), cache_spec, cache_spec)
    out_specs = (P('dp', None), cache_spec, cache_spec)
    return jax.shard_map(step, mesh=mesh, in_specs=in_specs, out_specs=out_specs, check_vma=False)
```

```python
import functools
import math

import jax
import jax.numpy as jnp
from jax import lax
from jax.experimental import pallas as pl
from jax.experimental.pallas import tpu as pltpu
from jax.sharding import PartitionSpec as P


F32 = jnp.float32
BF16 = jnp.bfloat16
ANY = pl.BlockSpec(memory_space=pltpu.HBM)
VMEM = pl.BlockSpec(memory_space=pltpu.VMEM)
NCH = 256
SB = 16
HALF = 128
LOG2E = math.log2(math.e)
MESH = pl.DeviceIdType.MESH


def silu(v):
    return v * jax.nn.sigmoid(v)


def expand_matrix():
    row = lax.broadcasted_iota(jnp.int32, (128, 512), 0)
    col = lax.broadcasted_iota(jnp.int32, (128, 512), 1)
    target = 2 * row + jnp.where(col < 256, 0, 257)
    return jnp.where(col == target, 1.0, 0.0).astype(BF16)


def rms0(v):
    return v * lax.rsqrt(jnp.mean(v * v, axis=0, keepdims=True) + 1e-6)


def sublane_sums(parts):
    sub = lax.broadcasted_iota(jnp.int32, parts[0].shape, 0)
    for step in (4, 2, 1):
        keep = (sub & step) == 0
        half = len(parts) // 2
        parts = [jnp.where(keep, parts[k], parts[k + half])
                 + pltpu.roll(jnp.where(keep, parts[k + half], parts[k]), step, 0) if step == 4 else
                 jnp.where(keep, parts[k], parts[k + half])
                 + jnp.where(keep, pltpu.roll(parts[k], 8 - step, 0), pltpu.roll(parts[k + half], step, 0))
                 for k in range(half)]
    return parts[0]


def add_pieces(rbuf, start, sides, u, up, v, vp):
    lo, hi = sides

    def add(i, carry):
        src = pl.ds(pl.multiple_of(i * 32, 32), 32)
        dst = pl.ds(pl.multiple_of(i * 32, 32) + start, 32)
        rbuf[dst, lo] = rbuf[dst, lo] + (u[src, :].astype(F32) + v[src, :].astype(F32))
        rbuf[dst, hi] = rbuf[dst, hi] + (up[src, :].astype(F32) + vp[src, :].astype(F32))
        return carry

    lax.fori_loop(0, HALF // 32, add, 0)


def norm_expand(rbuf, start, norm_row, hbuf, ex_s, hx):
    nw = norm_row.astype(F32)
    feat = rbuf.shape[1]

    def norm(i, carry):
        off = pl.multiple_of(i * 32, 32)
        r = rbuf[pl.ds(off + start, 32), :]
        inv = lax.rsqrt(jnp.mean(r * r, axis=-1, keepdims=True) + 1e-5)
        hbuf[pl.ds(off, 32), :] = (r * inv * nw).astype(BF16)
        return carry

    lax.fori_loop(0, HALF // 32, norm, 0)

    def expand(j, carry):
        for t in range(4):
            src = pl.ds(pl.multiple_of(j * 512 + t * 128, 128), 128)
            e = jnp.dot(hbuf[:, src], ex_s[...], preferred_element_type=F32).astype(BF16)
            cols = pl.ds(pl.multiple_of(j * 1024 + t * 256, 256), 256)
            hx[0:HALF, cols] = e[:, :256]
            hx[HALF:2 * HALF, cols] = e[:, 256:]
        return carry

    lax.fori_loop(0, feat // 512, expand, 0)


def cols_of(c):
    return pl.ds(pl.multiple_of(c * NCH, NCH), NCH)


def in_chunk(layer, c, hx, wbuf, conv_w, conv_b, window, z_out, xc_out):
    old0, old1, old2, x_out = window
    sl = cols_of(c)
    acc = jnp.dot(hx[...], wbuf[c], preferred_element_type=F32)
    x = acc[:HALF].astype(BF16)
    z_out[:, sl] = acc[HALF:].astype(BF16)
    x_out[:, sl] = x
    taps = conv_w[layer, :, sl].astype(F32)
    pre = old0[:, sl].astype(F32) * taps[0:1] + old1[:, sl].astype(F32) * taps[1:2]
    pre = pre + old2[:, sl].astype(F32) * taps[2:3] + x.astype(F32) * taps[3:4]
    pre = pre + conv_b[layer:layer + 1, sl].astype(F32)
    xc_out[:, sl] = silu(pre).astype(BF16)


def x_project(w_x_layer, xc):
    return lax.dot_general(w_x_layer, xc, (((1,), (1,)), ((), ())), preferred_element_type=F32).astype(BF16)


def halves_of(core, half):
    return (pl.ds(pl.multiple_of(core * half, 128), half), pl.ds(pl.multiple_of((1 - core) * half, 128), half))


def layer_kernel(layer, first, *refs):
    refs = list(refs)
    res = refs.pop(0)
    if not first:
        ub_in, vb_in, z_a, xc_a, p_a = refs[:5]
        refs = refs[5:]
    (norm_w, w_in, conv_w, conv_b, w_x, conv_st, w_dt, b_dt, a_log, d_skip, w_out, state) = refs[:12]
    refs = refs[12:]
    st, cw, ua, ub, upa, va, vpa = refs[:7]
    refs = refs[7:]
    r_out = None if first else refs.pop(0)
    (wbuf, hx, hbuf, ex_s, p_own, p_sw, p_cs, p_v, rbuf, cold, z_s, xc_s, dt_s, bc_s, a_s, y_s, part,
     mine_a, mine_b, theirs_a, theirs_b, got_a, got_b, upb, vpb, lsem, wsem, stsem, osem, ssem, rsem) = refs
    feat = rbuf.shape[1]
    nchunk = wbuf.shape[0]
    chan = z_s.shape[1]
    rank = w_dt.shape[1]
    nst = a_s.shape[0]
    nblk = HALF // SB
    half = feat // 2
    quarter = HALF // 2
    w_flat = w_in.reshape(w_in.shape[0], 2 * feat, w_in.shape[3])
    in_halves = (0, 1) if first else (1,)

    me = lax.axis_index('tp')
    core = lax.rem(me, 2)
    partner = me + 1 - 2 * core
    other = lax.rem(me + 2, 4)
    barrier = pltpu.get_barrier_semaphore()
    for dev in (partner, other):
        pl.semaphore_signal(barrier, inc=1, device_id={'tp': dev}, device_id_type=MESH)

    def send(src, dst, k, dev):
        return pltpu.make_async_remote_copy(src_ref=src, dst_ref=dst, send_sem=ssem.at[k], recv_sem=rsem.at[k],
                                            device_id={'tp': dev}, device_id_type=MESH)

    def half_rows(k):
        return pl.ds(k * HALF, HALF)

    def held_rows(k):
        return pl.ds(k * HALF if first else 0, HALF)

    def r_copy(k):
        return pltpu.make_async_copy(res.at[half_rows(k)], rbuf.at[held_rows(k)], lsem.at[k])

    nwin = cold.shape[0]
    win_rows = pl.ds(0 if first else HALF, nwin)
    old_copy = pltpu.make_async_copy(conv_st.at[layer, 0, win_rows], cold, lsem.at[2])
    win_copy = pltpu.make_async_copy(conv_st.at[layer, pl.ds(1, 2), win_rows], cw.at[pl.ds(0, 2)], lsem.at[3])

    def w_copy(c):
        return pltpu.make_async_copy(w_flat.at[layer, :, cols_of(c)], wbuf.at[c], wsem.at[c])

    def st_copy(i):
        rs = pl.ds(i * SB, SB)
        return pltpu.make_async_copy(state.at[layer, rs], st.at[rs], stsem.at[i])

    def out_tile(j):
        return wbuf.at[j // 4, pl.ds(pl.multiple_of(lax.rem(j, 4) * chan, 128), chan)]

    def o_copy(j):
        return pltpu.make_async_copy(w_out.at[layer, :, cols_of(j)], out_tile(j), osem.at[j])

    r_copy(in_halves[0]).start()
    w_copy(0).start()
    if first:
        r_copy(1).start()
    w_copy(1).start()
    old_copy.start()
    win_copy.start()
    w_copy(2).start()
    ex_s[...] = expand_matrix()
    a_s[...] = -jnp.exp(a_log[layer]) * LOG2E
    pl.semaphore_wait(barrier, 2)
    relays = []
    if not first:
        relays = [send(vb_in, vpb, 11, partner), send(ub_in, upb, 14, partner)]
        for c in relays:
            c.start()

    def p_first(k):
        return send(p_own.at[k], p_sw.at[k], k, partner)

    def p_second(k):
        return send(p_cs.at[k], p_v.at[k], 2 + k, other)

    def p_middle(k):
        p_first(k).wait_recv()
        p_cs[k] = (p_own[k].astype(F32) + p_sw[k].astype(F32)).astype(BF16)
        p_second(k).start()

    if not first:
        p_own[0] = p_a[...]
        p_first(0).start()
        xc_s[0:HALF, :] = xc_a[...]
        z_s[0:HALF, :] = z_a[...]
    for k in in_halves:
        start = k * HALF if first else 0
        r_copy(k).wait()
        if not first:
            for c in relays:
                c.wait_recv()
            add_pieces(rbuf, start, halves_of(core, half), ub_in, upb, vb_in, vpb)
            pltpu.make_async_copy(rbuf, r_out, lsem.at[4]).start()
        norm_expand(rbuf, start, norm_w[layer:layer + 1, :], hbuf, ex_s, hx)
        if k == in_halves[0]:
            old_copy.wait()
            win_copy.wait()

        def chunk(c, carry, k=k):
            if k == in_halves[0]:
                w_copy(c).wait()

                @pl.when(c + 3 < nchunk)
                def _():
                    w_copy(c + 3).start()

            if k == 1:
                for t in range(3):
                    st_copy(3 * c + t).start()
            held = held_rows(k)
            window = (cold.at[held], cw.at[0, held], cw.at[1, held], cw.at[2, held])
            in_chunk(layer, c, hx, wbuf, conv_w, conv_b, window, z_s.at[half_rows(k)], xc_s.at[half_rows(k)])
            if k == 1:
                @pl.when(c < 2)
                def _():
                    for t in range(4):
                        o_copy(4 * c + t).start()

                @pl.when(c == 2)
                def _():
                    for t in range(2):
                        o_copy(8 + t).start()
                    p_middle(0)

            return carry

        lax.fori_loop(0, nchunk, chunk, 0)
        p_own[k] = x_project(w_x[layer], xc_s[half_rows(k), :])
        p_first(k).start()
    st_copy(2 * nblk - 1).start()

    def red_a(q):
        return send(theirs_a.at[q], got_a.at[q], 4 + q, partner)

    red_b = send(theirs_b, got_b, 6, partner)

    def quarter_rows(q):
        return pl.ds(q * quarter, quarter)

    def cross(q):
        return send(ua.at[quarter_rows(q)], va.at[quarter_rows(q)], 7 + q, other)

    def up_a(q):
        return send(ua.at[quarter_rows(q)], upa.at[quarter_rows(q)], 9 + q, partner)

    def forward(q):
        return send(va.at[quarter_rows(q)], vpa.at[quarter_rows(q)], 12 + q, partner)

    def reduce_a(q):
        red_a(q).wait_recv()
        ua[quarter_rows(q), :] = (mine_a[q] + got_a[q].astype(F32)).astype(BF16)
        cross(q).start()
        up_a(q).start()

    lane = lax.broadcasted_iota(jnp.int32, (nst, 128), 1)
    row = lax.broadcasted_iota(jnp.int32, (nst, 128), 0)

    def gated(rs, y):
        y = y + d_skip[layer:layer + 1, :] * xc_s[rs, :].astype(F32)
        return (y * silu(z_s[rs, :].astype(F32))).astype(BF16)

    def project(yg, first, dst, dtype):
        for t in range(half // NCH):
            j = first * (half // NCH) + t
            dst[:, t * NCH:(t + 1) * NCH] = jnp.dot(yg, out_tile(j)[...], preferred_element_type=F32).astype(dtype)

    for k in range(2):
        p_second(k).wait_recv()
        p = p_cs[k].astype(F32) + p_v[k].astype(F32)
        low = rms0(p[:rank]).astype(BF16)
        pre = lax.dot_general(low, w_dt[layer], (((0,), (0,)), ((), ())), preferred_element_type=F32)
        pre = pre + b_dt[layer:layer + 1, :]
        dt_s[...] = jnp.maximum(pre, 0.0) + jnp.log1p(jnp.exp(-jnp.abs(pre)))
        bc = jnp.concatenate([rms0(p[rank:rank + nst]), rms0(p[rank + nst:])], axis=0)
        bc_s[:, 0:2 * nst] = jnp.transpose(bc)

        def block(i, carry, k=k):
            st_copy(i + k * nblk).wait()
            local = pl.multiple_of(i * SB, SB)
            base = local + k * HALF
            dt = dt_s[pl.ds(local, SB), :]
            dtx = dt * xc_s[pl.ds(base, SB), :].astype(F32)
            bc = bc_s[pl.ds(local, SB), :]
            a2 = a_s[...]
            for b in range(SB):
                bcb = jnp.broadcast_to(bc[b:b + 1, :], (nst, 128))
                bcol = jnp.sum(jnp.where(lane == row, bcb, 0.0), axis=1, keepdims=True)
                ccol = jnp.sum(jnp.where(lane == row + nst, bcb, 0.0), axis=1, keepdims=True)
                s = jnp.exp2(dt[b:b + 1, :] * a2) * st[base + b] + dtx[b:b + 1, :] * bcol
                st[base + b] = s
                t = s * ccol
                part[b] = t[0:8] + t[8:16]
            for g in range(SB // 8):
                y_s[pl.ds(local + 8 * g, 8), :] = sublane_sums([part[8 * g + n] for n in range(8)])

            if k == 0:
                @pl.when(i == 2)
                def _():
                    p_middle(1)

                @pl.when(i == nblk // 2 - 1)
                def _():
                    for j in range(feat // NCH):
                        o_copy(j).wait()

                @pl.when(lax.rem(i, nblk // 2) == nblk // 2 - 1)
                def _():
                    q = i // (nblk // 2)
                    rs = pl.ds(pl.multiple_of(q * quarter, quarter), quarter)
                    yg = gated(rs, y_s[rs, :])
                    project(yg, 1 - core, theirs_a.at[q], BF16)
                    red_a(q).start()
                    project(yg, core, mine_a.at[q], F32)

                @pl.when(i == nblk // 2 + 1)
                def _():
                    reduce_a(0)
            else:
                @pl.when(i == 1)
                def _():
                    reduce_a(1)

            return carry

        lax.fori_loop(0, nblk, block, 0)

    yg = gated(half_rows(1), y_s[...])
    project(yg, 1 - core, theirs_b, BF16)
    red_b.start()
    project(yg, core, mine_b, F32)
    cross(0).wait_recv()
    forward(0).start()
    red_b.wait_recv()
    ub[...] = (mine_b[...] + got_b[...].astype(F32)).astype(BF16)
    cross(1).wait_recv()
    forward(1).start()
    for q in range(2):
        up_a(q).wait_recv()
    for q in range(2):
        forward(q).wait_recv()
    for k in range(2):
        p_first(k).wait_send()
        p_second(k).wait_send()
        red_a(k).wait_send()
        cross(k).wait_send()
        up_a(k).wait_send()
        forward(k).wait_send()
    red_b.wait_send()
    for c in relays:
        c.wait_send()
    if not first:
        pltpu.make_async_copy(rbuf, r_out, lsem.at[4]).wait()


def layer_call(layer, residual, ready, weights, conv_st, state):
    norm_w, w_in, conv_w, conv_b, w_x, w_dt, b_dt, a_log, d_skip, w_out = weights
    first = ready is None
    rows, feat = residual.shape
    chan = w_in.shape[3]
    nst = a_log.shape[1]
    half = feat // 2
    nproj = w_x.shape[1]
    nchunk = chan // NCH
    flat = [] if first else list(ready)
    held = rows if first else HALF
    args = [residual] + flat + [norm_w, w_in, conv_w, conv_b, w_x, conv_st, w_dt, b_dt, a_log, d_skip, w_out, state]
    specs = [ANY] + [VMEM] * len(flat) + [VMEM, ANY, VMEM, VMEM, VMEM, ANY, VMEM, VMEM, VMEM, VMEM, ANY, ANY]
    piece = pltpu.VMEM((HALF, half), BF16)
    outs = [pltpu.VMEM((rows, nst, chan), F32), pltpu.VMEM((3, held, chan), BF16)] + [piece] * 5
    out_specs = [VMEM] * 7
    if not first:
        outs.append(jax.ShapeDtypeStruct((HALF, feat), F32))
        out_specs.append(ANY)
    vm = pltpu.VMEM
    dma = pltpu.SemaphoreType.DMA
    quarter = HALF // 2
    return pl.pallas_call(
        functools.partial(layer_kernel, layer, first),
        out_shape=outs, in_specs=specs, out_specs=out_specs,
        scratch_shapes=[
            vm((nchunk, 2 * feat, NCH), BF16), vm((2 * HALF, 2 * feat), BF16), vm((HALF, feat), BF16), vm((128, 512), BF16),
            vm((2, nproj, HALF), BF16), vm((2, nproj, HALF), BF16), vm((2, nproj, HALF), BF16),
            vm((2, nproj, HALF), BF16), vm((held, feat), F32), vm((held, chan), BF16), vm((rows, chan), BF16),
            vm((rows, chan), BF16), vm((HALF, chan), F32), vm((HALF, 128), F32), vm((nst, chan), F32), vm((HALF, chan), F32),
            vm((SB, 8, chan), F32), vm((2, quarter, half), F32), vm((HALF, half), F32), vm((2, quarter, half), BF16),
            vm((HALF, half), BF16), vm((2, quarter, half), BF16), vm((HALF, half), BF16), vm((HALF, half), BF16),
            vm((HALF, half), BF16),
            dma((5,)), dma((nchunk,)), dma((rows // SB,)), dma((feat // NCH,)), dma((15,)), dma((15,)),
        ],
        compiler_params=pltpu.CompilerParams(vmem_limit_bytes=34 * 2 ** 20, collective_id=layer, has_side_effects=True),
        cost_estimate=pl.CostEstimate(flops=2 * 10 ** 10, bytes_accessed=46 * 2 ** 20, transcendentals=0),
    )(*args)


def mid_kernel(layer, st, cw, res, ua, upa, va, vpa, norm_w, w_in, conv_w, conv_b, w_x, conv_st,
               ssm_out, conv_out, z_a, xc_a, p_a, cw_a, r_a,
               wbuf, hx, hbuf, ex_s, rbuf, cold, lsem, wsem, sem):
    feat = rbuf.shape[1]
    nchunk = wbuf.shape[0]
    nxt = layer + 1
    w_flat = w_in.reshape(w_in.shape[0], 2 * feat, w_in.shape[3])
    rows_a = pl.ds(0, HALF)

    def w_copy(c):
        return pltpu.make_async_copy(w_flat.at[nxt, :, cols_of(c)], wbuf.at[c], wsem.at[c])

    def st_copy(i):
        rs = pl.ds(i * SB, SB)
        return pltpu.make_async_copy(st.at[rs], ssm_out.at[layer, rs], sem.at[i])

    nst = st.shape[0] // SB
    r_copy = pltpu.make_async_copy(res.at[rows_a], rbuf, lsem.at[0])
    old_copy = pltpu.make_async_copy(conv_st.at[nxt, 0, rows_a], cold, lsem.at[1])
    win_copy = pltpu.make_async_copy(conv_st.at[nxt, pl.ds(1, 2), rows_a], cw_a.at[pl.ds(0, 2)], lsem.at[2])
    r_back = pltpu.make_async_copy(rbuf, r_a, lsem.at[3])
    c_copy = pltpu.make_async_copy(cw, conv_out.at[layer], lsem.at[4])
    r_copy.start()
    w_copy(0).start()
    old_copy.start()
    win_copy.start()
    w_copy(1).start()
    w_copy(2).start()
    ex_s[...] = expand_matrix()
    core = lax.rem(lax.axis_index('tp'), 2)
    r_copy.wait()
    st_copy(nst - 1).start()
    c_copy.start()
    add_pieces(rbuf, 0, halves_of(core, feat // 2), ua, upa, va, vpa)
    r_back.start()
    norm_expand(rbuf, 0, norm_w[nxt:nxt + 1, :], hbuf, ex_s, hx)
    old_copy.wait()
    win_copy.wait()
    window = (cold, cw_a.at[0], cw_a.at[1], cw_a.at[2])

    def chunk(c, carry):
        w_copy(c).wait()

        @pl.when(c + 3 < nchunk)
        def _():
            w_copy(c + 3).start()

        for t in range(3):
            st_copy(3 * c + t).start()
        in_chunk(nxt, c, hx, wbuf, conv_w, conv_b, window, z_a, xc_a)
        return carry

    lax.fori_loop(0, nchunk, chunk, 0)
    p_a[...] = x_project(w_x[nxt], xc_a[...])
    c_copy.wait()
    r_back.wait()
    for i in range(nst):
        st_copy(i).wait()


def mid_call(layer, st, cw, residual, pieces, weights, conv_st, shapes):
    norm_w, w_in, conv_w, conv_b, w_x = weights[:5]
    feat = residual.shape[1]
    chan = w_in.shape[3]
    nchunk = chan // NCH
    vm = pltpu.VMEM
    dma = pltpu.SemaphoreType.DMA
    args = [pltpu.with_memory_space_constraint(a, pltpu.VMEM) for a in (st, cw)]
    args += [residual, *pieces, norm_w, w_in, conv_w, conv_b, w_x, conv_st]
    return pl.pallas_call(
        functools.partial(mid_kernel, layer),
        out_shape=[jax.ShapeDtypeStruct(shapes[0], F32), jax.ShapeDtypeStruct(shapes[1], BF16),
                   vm((HALF, chan), BF16), vm((HALF, chan), BF16), vm((w_x.shape[1], HALF), BF16),
                   vm((3, HALF, chan), BF16), jax.ShapeDtypeStruct((HALF, feat), F32)],
        in_specs=[VMEM, VMEM, ANY] + [VMEM] * 4 + [VMEM, ANY, VMEM, VMEM, VMEM, ANY],
        out_specs=[ANY, ANY, VMEM, VMEM, VMEM, VMEM, ANY],
        scratch_shapes=[vm((nchunk, 2 * feat, NCH), BF16), vm((2 * HALF, 2 * feat), BF16), vm((HALF, feat), BF16),
                        vm((128, 512), BF16), vm((HALF, feat), F32), vm((HALF, chan), BF16),
                        dma((5,)), dma((nchunk,)), dma((st.shape[0] // SB,))],
        compiler_params=pltpu.CompilerParams(vmem_limit_bytes=22 * 2 ** 20),
        cost_estimate=pl.CostEstimate(flops=2 * 10 ** 10, bytes_accessed=42 * 2 ** 20, transcendentals=0),
    )(*args)


def w_kernel(layer, st, cw_a, cw_b, ssm_prev, conv_prev, ssm_out, conv_out, sem):
    def copy(i):
        rs = pl.ds(i * SB, SB)
        return pltpu.make_async_copy(st.at[rs], ssm_out.at[layer, rs], sem.at[i])

    n = st.shape[0] // SB
    copies = [copy(i) for i in range(n)]
    for k, src in enumerate((cw_a, cw_b)):
        copies.append(pltpu.make_async_copy(src, conv_out.at[layer, :, pl.ds(k * HALF, HALF)], sem.at[n + k]))
    for c in copies:
        c.start()
    for c in copies:
        c.wait()


def w_call(layer, st, cw_a, cw_b, prev):
    args = [pltpu.with_memory_space_constraint(a, pltpu.VMEM) for a in (st, cw_a, cw_b)]
    return pl.pallas_call(
        functools.partial(w_kernel, layer),
        out_shape=[jax.ShapeDtypeStruct(a.shape, a.dtype) for a in prev],
        in_specs=[VMEM, VMEM, VMEM, ANY, ANY], out_specs=[ANY, ANY], input_output_aliases={3: 0, 4: 1},
        scratch_shapes=[pltpu.SemaphoreType.DMA((st.shape[0] // SB + 2,))],
        compiler_params=pltpu.CompilerParams(vmem_limit_bytes=2 ** 20),
        cost_estimate=pl.CostEstimate(flops=2 * 10 ** 10, bytes_accessed=42 * 2 ** 20, transcendentals=0),
    )(*args, *prev)


def fin_kernel(r_a, r_b, *refs):
    out = refs[-1]
    core = lax.rem(lax.axis_index('tp'), 2)
    half = out.shape[1] // 2
    lo = pl.ds(pl.multiple_of(core * half, 128), half)
    hi = pl.ds(pl.multiple_of((1 - core) * half, 128), half)
    for k in range(2):
        u, up, v, vp = refs[4 * k:4 * k + 4]
        rs = slice(k * HALF, (k + 1) * HALF)
        r = (r_a, r_b)[k]
        out[rs, lo] = r[:, lo] + (u[...].astype(F32) + v[...].astype(F32))
        out[rs, hi] = r[:, hi] + (up[...].astype(F32) + vp[...].astype(F32))


def fin_call(r_a, r_b, pieces):
    return pl.pallas_call(
        fin_kernel, out_shape=jax.ShapeDtypeStruct((2 * HALF, r_a.shape[1]), F32), in_specs=[VMEM] * 10, out_specs=VMEM,
        compiler_params=pltpu.CompilerParams(vmem_limit_bytes=16 * 2 ** 20), name="fin",
    )(r_a, r_b, *pieces[0], *pieces[1])


PART = [(0, 1), (1, 0), (2, 3), (3, 2)]
CROSS = [(0, 2), (2, 0), (1, 3), (3, 1)]


def solution(mesh):
    def step(residual, norm_w, w_in, conv_w, conv_b, w_x, w_dt, b_dt, a_log, d_skip, w_out, conv_state, ssm_state):
        w_xt = jnp.transpose(w_x, (0, 2, 1))
        conv_t = jnp.transpose(conv_state, (0, 2, 1, 3))
        weights = (norm_w, w_in, conv_w, conv_b, w_xt, w_dt, b_dt, a_log, d_skip, w_out)
        shapes = (ssm_state.shape, conv_t.shape)
        st, cw, ua, ub, upa, va, vpa = layer_call(0, residual, None, weights, conv_t, ssm_state)
        vb = lax.ppermute(ub, 'tp', CROSS)
        *written, z_a, xc_a, p_a, cw_a, r_a = mid_call(0, st, cw, residual, (ua, upa, va, vpa), weights, conv_t, shapes)
        ready = (ub, vb, z_a, xc_a, p_a)
        st, cw_b, ua, ub, upa, va, vpa, r_b = layer_call(1, residual, ready, weights, conv_t, ssm_state)
        vb = lax.ppermute(ub, 'tp', CROSS)
        upb = lax.ppermute(ub, 'tp', PART)
        ssm_out, conv_out = w_call(1, st, cw_a, cw_b, written)
        vpb = lax.ppermute(vb, 'tp', PART)
        out = fin_call(r_a, r_b, ((ua, upa, va, vpa), (ub, upb, vb, vpb)))
        return out, jnp.transpose(conv_out, (0, 2, 1, 3)), ssm_out

    cache_spec = P(None, 'dp', None, 'tp')
    in_specs = (P('dp', None), P(None, None), P(None, None, None, 'tp'), P(None, None, 'tp'), P(None, 'tp'), P(None, 'tp', None), P(None, None, 'tp'), P(None, 'tp'), P(None, None, 'tp'), P(None, 'tp'), P(None, 'tp', None), cache_spec, cache_spec)
    out_specs = (P('dp', None), cache_spec, cache_spec)
    return jax.shard_map(step, mesh=mesh, in_specs=in_specs, out_specs=out_specs, check_vma=False)
```

```python
import functools
import math

import jax
import jax.numpy as jnp
from jax import lax
from jax.experimental import pallas as pl
from jax.experimental.pallas import tpu as pltpu
from jax.sharding import PartitionSpec as P


F32 = jnp.float32
BF16 = jnp.bfloat16
ANY = pl.BlockSpec(memory_space=pltpu.HBM)
VMEM = pl.BlockSpec(memory_space=pltpu.VMEM)
NCH = 256
SB = 16
HALF = 128
LOG2E = math.log2(math.e)
MESH = pl.DeviceIdType.MESH


def silu(v):
    return v * jax.nn.sigmoid(v)


def expand_matrix():
    row = lax.broadcasted_iota(jnp.int32, (128, 512), 0)
    col = lax.broadcasted_iota(jnp.int32, (128, 512), 1)
    target = 2 * row + jnp.where(col < 256, 0, 257)
    return jnp.where(col == target, 1.0, 0.0).astype(BF16)


def rms0(v):
    return v * lax.rsqrt(jnp.mean(v * v, axis=0, keepdims=True) + 1e-6)


def sublane_sums(parts):
    sub = lax.broadcasted_iota(jnp.int32, parts[0].shape, 0)
    for step in (4, 2, 1):
        keep = (sub & step) == 0
        half = len(parts) // 2
        parts = [jnp.where(keep, parts[k], parts[k + half])
                 + pltpu.roll(jnp.where(keep, parts[k + half], parts[k]), step, 0) if step == 4 else
                 jnp.where(keep, parts[k], parts[k + half])
                 + jnp.where(keep, pltpu.roll(parts[k], 8 - step, 0), pltpu.roll(parts[k + half], step, 0))
                 for k in range(half)]
    return parts[0]


def add_pieces(rbuf, start, sides, u, up, v, vp):
    lo, hi = sides

    def add(i, carry):
        src = pl.ds(pl.multiple_of(i * 32, 32), 32)
        dst = pl.ds(pl.multiple_of(i * 32, 32) + start, 32)
        rbuf[dst, lo] = rbuf[dst, lo] + (u[src, :].astype(F32) + v[src, :].astype(F32))
        rbuf[dst, hi] = rbuf[dst, hi] + (up[src, :].astype(F32) + vp[src, :].astype(F32))
        return carry

    lax.fori_loop(0, HALF // 32, add, 0)


def norm_expand(rbuf, start, norm_row, hbuf, ex_s, hx):
    nw = norm_row.astype(F32)
    feat = rbuf.shape[1]

    def norm(i, carry):
        off = pl.multiple_of(i * 32, 32)
        r = rbuf[pl.ds(off + start, 32), :]
        inv = lax.rsqrt(jnp.mean(r * r, axis=-1, keepdims=True) + 1e-5)
        hbuf[pl.ds(off, 32), :] = (r * inv * nw).astype(BF16)
        return carry

    lax.fori_loop(0, HALF // 32, norm, 0)

    def expand(j, carry):
        for t in range(4):
            src = pl.ds(pl.multiple_of(j * 512 + t * 128, 128), 128)
            e = jnp.dot(hbuf[:, src], ex_s[...], preferred_element_type=F32).astype(BF16)
            cols = pl.ds(pl.multiple_of(j * 1024 + t * 256, 256), 256)
            hx[0:HALF, cols] = e[:, :256]
            hx[HALF:2 * HALF, cols] = e[:, 256:]
        return carry

    lax.fori_loop(0, feat // 512, expand, 0)


def cols_of(c):
    return pl.ds(pl.multiple_of(c * NCH, NCH), NCH)


def in_chunk(layer, c, hx, wbuf, conv_w, conv_b, window, z_out, xc_out):
    old0, old1, old2, x_out = window
    sl = cols_of(c)
    acc = jnp.dot(hx[...], wbuf[c], preferred_element_type=F32)
    x = acc[:HALF].astype(BF16)
    z_out[:, sl] = acc[HALF:].astype(BF16)
    x_out[:, sl] = x
    taps = conv_w[layer, :, sl].astype(F32)
    pre = old0[:, sl].astype(F32) * taps[0:1] + old1[:, sl].astype(F32) * taps[1:2]
    pre = pre + old2[:, sl].astype(F32) * taps[2:3] + x.astype(F32) * taps[3:4]
    pre = pre + conv_b[layer:layer + 1, sl].astype(F32)
    xc_out[:, sl] = silu(pre).astype(BF16)


def x_project(w_x_layer, xc):
    return lax.dot_general(w_x_layer, xc, (((1,), (1,)), ((), ())), preferred_element_type=F32).astype(BF16)


def halves_of(core, half):
    return (pl.ds(pl.multiple_of(core * half, 128), half), pl.ds(pl.multiple_of((1 - core) * half, 128), half))


def layer_kernel(layer, first, *refs):
    refs = list(refs)
    res = refs.pop(0)
    if not first:
        ub_in, vb_in, z_a, xc_a, p_a = refs[:5]
        refs = refs[5:]
    (norm_w, w_in, conv_w, conv_b, w_x, conv_st, w_dt, b_dt, a_log, d_skip, w_out, state) = refs[:12]
    refs = refs[12:]
    st, cw, ua, ub, upa, va, vpa = refs[:7]
    refs = refs[7:]
    r_out = None if first else refs.pop(0)
    (wbuf, hx, hbuf, ex_s, p_own, p_sw, p_cs, p_v, rbuf, cold, z_s, xc_s, dt_s, bc_s, a_s, y_s, part,
     mine_a, mine_b, theirs_a, theirs_b, got_a, got_b, upb, vpb, lsem, wsem, stsem, osem, ssem, rsem) = refs
    feat = rbuf.shape[1]
    nchunk = wbuf.shape[0]
    chan = z_s.shape[1]
    rank = w_dt.shape[1]
    nst = a_s.shape[0]
    nblk = HALF // SB
    half = feat // 2
    quarter = HALF // 2
    w_flat = w_in.reshape(w_in.shape[0], 2 * feat, w_in.shape[3])
    in_halves = (0, 1) if first else (1,)

    me = lax.axis_index('tp')
    core = lax.rem(me, 2)
    partner = me + 1 - 2 * core
    other = lax.rem(me + 2, 4)
    barrier = pltpu.get_barrier_semaphore()
    for dev in (partner, other):
        pl.semaphore_signal(barrier, inc=1, device_id={'tp': dev}, device_id_type=MESH)

    def send(src, dst, k, dev):
        return pltpu.make_async_remote_copy(src_ref=src, dst_ref=dst, send_sem=ssem.at[k], recv_sem=rsem.at[k],
                                            device_id={'tp': dev}, device_id_type=MESH)

    def half_rows(k):
        return pl.ds(k * HALF, HALF)

    def held_rows(k):
        return pl.ds(k * HALF if first else 0, HALF)

    def r_copy(k):
        return pltpu.make_async_copy(res.at[half_rows(k)], rbuf.at[held_rows(k)], lsem.at[k])

    nwin = cold.shape[0]
    win_rows = pl.ds(0 if first else HALF, nwin)
    old_copy = pltpu.make_async_copy(conv_st.at[layer, 0, win_rows], cold, lsem.at[2])
    win_copy = pltpu.make_async_copy(conv_st.at[layer, pl.ds(1, 2), win_rows], cw.at[pl.ds(0, 2)], lsem.at[3])

    def w_copy(c):
        return pltpu.make_async_copy(w_flat.at[layer, :, cols_of(c)], wbuf.at[c], wsem.at[c])

    def st_copy(i):
        rs = pl.ds(i * SB, SB)
        return pltpu.make_async_copy(state.at[layer, rs], st.at[rs], stsem.at[i])

    def out_tile(j):
        return wbuf.at[j // 4, pl.ds(pl.multiple_of(lax.rem(j, 4) * chan, 128), chan)]

    def o_copy(j):
        return pltpu.make_async_copy(w_out.at[layer, :, cols_of(j)], out_tile(j), osem.at[j])

    r_copy(in_halves[0]).start()
    w_copy(0).start()
    if first:
        r_copy(1).start()
    w_copy(1).start()
    old_copy.start()
    win_copy.start()
    w_copy(2).start()
    ex_s[...] = expand_matrix()
    a_s[...] = -jnp.exp(a_log[layer]) * LOG2E
    pl.semaphore_wait(barrier, 2)
    relays = []
    if not first:
        relays = [send(vb_in, vpb, 11, partner), send(ub_in, upb, 14, partner)]
        for c in relays:
            c.start()

    def p_first(k):
        return send(p_own.at[k], p_sw.at[k], k, partner)

    def p_second(k):
        return send(p_cs.at[k], p_v.at[k], 2 + k, other)

    def p_middle(k):
        p_first(k).wait_recv()
        p_cs[k] = (p_own[k].astype(F32) + p_sw[k].astype(F32)).astype(BF16)
        p_second(k).start()

    if not first:
        p_own[0] = p_a[...]
        p_first(0).start()
        xc_s[0:HALF, :] = xc_a[...]
        z_s[0:HALF, :] = z_a[...]
    for k in in_halves:
        start = k * HALF if first else 0
        r_copy(k).wait()
        if not first:
            for c in relays:
                c.wait_recv()
            add_pieces(rbuf, start, halves_of(core, half), ub_in, upb, vb_in, vpb)
            pltpu.make_async_copy(rbuf, r_out, lsem.at[4]).start()
        norm_expand(rbuf, start, norm_w[layer:layer + 1, :], hbuf, ex_s, hx)
        if k == in_halves[0]:
            old_copy.wait()
            win_copy.wait()

        def chunk(c, carry, k=k):
            if k == in_halves[0]:
                w_copy(c).wait()

                @pl.when(c + 3 < nchunk)
                def _():
                    w_copy(c + 3).start()

            if k == 1:
                for t in range(3):
                    st_copy(3 * c + t).start()
            held = held_rows(k)
            window = (cold.at[held], cw.at[0, held], cw.at[1, held], cw.at[2, held])
            in_chunk(layer, c, hx, wbuf, conv_w, conv_b, window, z_s.at[half_rows(k)], xc_s.at[half_rows(k)])
            if k == 1:
                @pl.when(c < 2)
                def _():
                    for t in range(4):
                        o_copy(4 * c + t).start()

                @pl.when(c == 2)
                def _():
                    for t in range(2):
                        o_copy(8 + t).start()
                    p_middle(0)

            return carry

        lax.fori_loop(0, nchunk, chunk, 0)
        p_own[k] = x_project(w_x[layer], xc_s[half_rows(k), :])
        p_first(k).start()
    st_copy(2 * nblk - 1).start()

    def red_a(q):
        return send(theirs_a.at[q], got_a.at[q], 4 + q, partner)

    red_b = send(theirs_b, got_b, 6, partner)

    def quarter_rows(q):
        return pl.ds(q * quarter, quarter)

    def cross(q):
        return send(ua.at[quarter_rows(q)], va.at[quarter_rows(q)], 7 + q, other)

    def up_a(q):
        return send(ua.at[quarter_rows(q)], upa.at[quarter_rows(q)], 9 + q, partner)

    def forward(q):
        return send(va.at[quarter_rows(q)], vpa.at[quarter_rows(q)], 12 + q, partner)

    def reduce_a(q):
        red_a(q).wait_recv()
        ua[quarter_rows(q), :] = (mine_a[q] + got_a[q].astype(F32)).astype(BF16)
        cross(q).start()
        up_a(q).start()

    lane = lax.broadcasted_iota(jnp.int32, (nst, 128), 1)
    row = lax.broadcasted_iota(jnp.int32, (nst, 128), 0)

    def gated(rs, y):
        y = y + d_skip[layer:layer + 1, :] * xc_s[rs, :].astype(F32)
        return (y * silu(z_s[rs, :].astype(F32))).astype(BF16)

    def project(yg, first, dst, dtype):
        for t in range(half // NCH):
            j = first * (half // NCH) + t
            dst[:, t * NCH:(t + 1) * NCH] = jnp.dot(yg, out_tile(j)[...], preferred_element_type=F32).astype(dtype)

    for k in range(2):
        p_second(k).wait_recv()
        p = p_cs[k].astype(F32) + p_v[k].astype(F32)
        low = rms0(p[:rank]).astype(BF16)
        pre = lax.dot_general(low, w_dt[layer], (((0,), (0,)), ((), ())), preferred_element_type=F32)
        pre = pre + b_dt[layer:layer + 1, :]
        dt_s[...] = jnp.maximum(pre, 0.0) + jnp.log1p(jnp.exp(-jnp.abs(pre)))
        bc = jnp.concatenate([rms0(p[rank:rank + nst]), rms0(p[rank + nst:])], axis=0)
        bc_s[:, 0:2 * nst] = jnp.transpose(bc)

        def block(i, carry, k=k):
            st_copy(i + k * nblk).wait()
            local = pl.multiple_of(i * SB, SB)
            base = local + k * HALF
            dt = dt_s[pl.ds(local, SB), :]
            dtx = dt * xc_s[pl.ds(base, SB), :].astype(F32)
            bc = bc_s[pl.ds(local, SB), :]
            a2 = a_s[...]
            for b in range(SB):
                bcb = jnp.broadcast_to(bc[b:b + 1, :], (nst, 128))
                bcol = jnp.sum(jnp.where(lane == row, bcb, 0.0), axis=1, keepdims=True)
                ccol = jnp.sum(jnp.where(lane == row + nst, bcb, 0.0), axis=1, keepdims=True)
                s = jnp.exp2(dt[b:b + 1, :] * a2) * st[base + b] + dtx[b:b + 1, :] * bcol
                st[base + b] = s
                t = s * ccol
                part[b] = t[0:8] + t[8:16]
            for g in range(SB // 8):
                y_s[pl.ds(local + 8 * g, 8), :] = sublane_sums([part[8 * g + n] for n in range(8)])

            if k == 0:
                @pl.when(i == 2)
                def _():
                    p_middle(1)

                @pl.when(i == nblk // 2 - 1)
                def _():
                    for j in range(feat // NCH):
                        o_copy(j).wait()

                @pl.when(lax.rem(i, nblk // 2) == nblk // 2 - 1)
                def _():
                    q = i // (nblk // 2)
                    rs = pl.ds(pl.multiple_of(q * quarter, quarter), quarter)
                    yg = gated(rs, y_s[rs, :])
                    project(yg, 1 - core, theirs_a.at[q], BF16)
                    red_a(q).start()
                    project(yg, core, mine_a.at[q], F32)

                @pl.when(i == nblk // 2 + 1)
                def _():
                    reduce_a(0)
            else:
                @pl.when(i == 1)
                def _():
                    reduce_a(1)

            return carry

        lax.fori_loop(0, nblk, block, 0)

    yg = gated(half_rows(1), y_s[...])
    project(yg, 1 - core, theirs_b, BF16)
    red_b.start()
    project(yg, core, mine_b, F32)
    cross(0).wait_recv()
    forward(0).start()
    red_b.wait_recv()
    ub[...] = (mine_b[...] + got_b[...].astype(F32)).astype(BF16)
    cross(1).wait_recv()
    forward(1).start()
    for q in range(2):
        up_a(q).wait_recv()
    for q in range(2):
        forward(q).wait_recv()
    for k in range(2):
        p_first(k).wait_send()
        p_second(k).wait_send()
        red_a(k).wait_send()
        cross(k).wait_send()
        up_a(k).wait_send()
        forward(k).wait_send()
    red_b.wait_send()
    for c in relays:
        c.wait_send()
    if not first:
        pltpu.make_async_copy(rbuf, r_out, lsem.at[4]).wait()


def layer_call(layer, residual, ready, weights, conv_st, state):
    norm_w, w_in, conv_w, conv_b, w_x, w_dt, b_dt, a_log, d_skip, w_out = weights
    first = ready is None
    rows, feat = residual.shape
    chan = w_in.shape[3]
    nst = a_log.shape[1]
    half = feat // 2
    nproj = w_x.shape[1]
    nchunk = chan // NCH
    flat = [] if first else [pltpu.with_memory_space_constraint(a, pltpu.VMEM) for a in ready]
    held = rows if first else HALF
    args = [residual] + flat + [norm_w, w_in, conv_w, conv_b, w_x, conv_st, w_dt, b_dt, a_log, d_skip, w_out, state]
    specs = [ANY] + [VMEM] * len(flat) + [VMEM, ANY, VMEM, VMEM, VMEM, ANY, VMEM, VMEM, VMEM, VMEM, ANY, ANY]
    piece = pltpu.VMEM((HALF, half), BF16)
    outs = [pltpu.VMEM((rows, nst, chan), F32), pltpu.VMEM((3, held, chan), BF16)] + [piece] * 5
    out_specs = [VMEM] * 7
    if not first:
        outs.append(jax.ShapeDtypeStruct((HALF, feat), F32))
        out_specs.append(ANY)
    vm = pltpu.VMEM
    dma = pltpu.SemaphoreType.DMA
    quarter = HALF // 2
    return pl.pallas_call(
        functools.partial(layer_kernel, layer, first),
        out_shape=outs, in_specs=specs, out_specs=out_specs,
        scratch_shapes=[
            vm((nchunk, 2 * feat, NCH), BF16), vm((2 * HALF, 2 * feat), BF16), vm((HALF, feat), BF16), vm((128, 512), BF16),
            vm((2, nproj, HALF), BF16), vm((2, nproj, HALF), BF16), vm((2, nproj, HALF), BF16),
            vm((2, nproj, HALF), BF16), vm((held, feat), F32), vm((held, chan), BF16), vm((rows, chan), BF16),
            vm((rows, chan), BF16), vm((HALF, chan), F32), vm((HALF, 128), F32), vm((nst, chan), F32), vm((HALF, chan), F32),
            vm((SB, 8, chan), F32), vm((2, quarter, half), F32), vm((HALF, half), F32), vm((2, quarter, half), BF16),
            vm((HALF, half), BF16), vm((2, quarter, half), BF16), vm((HALF, half), BF16), vm((HALF, half), BF16),
            vm((HALF, half), BF16),
            dma((5,)), dma((nchunk,)), dma((rows // SB,)), dma((feat // NCH,)), dma((15,)), dma((15,)),
        ],
        compiler_params=pltpu.CompilerParams(vmem_limit_bytes=34 * 2 ** 20, collective_id=layer, has_side_effects=True),
        cost_estimate=pl.CostEstimate(flops=2 * 10 ** 10, bytes_accessed=46 * 2 ** 20, transcendentals=0),
    )(*args)


def mid_kernel(layer, st, cw, res, ua, upa, va, vpa, norm_w, w_in, conv_w, conv_b, w_x, conv_st,
               ssm_out, conv_out, z_a, xc_a, p_a, cw_a, r_a,
               wbuf, hx, hbuf, ex_s, rbuf, cold, lsem, wsem, sem):
    feat = rbuf.shape[1]
    nchunk = wbuf.shape[0]
    nxt = layer + 1
    w_flat = w_in.reshape(w_in.shape[0], 2 * feat, w_in.shape[3])
    rows_a = pl.ds(0, HALF)

    def w_copy(c):
        return pltpu.make_async_copy(w_flat.at[nxt, :, cols_of(c)], wbuf.at[c], wsem.at[c])

    def st_copy(i):
        rs = pl.ds(i * SB, SB)
        return pltpu.make_async_copy(st.at[rs], ssm_out.at[layer, rs], sem.at[i])

    nst = st.shape[0] // SB
    r_copy = pltpu.make_async_copy(res.at[rows_a], rbuf, lsem.at[0])
    old_copy = pltpu.make_async_copy(conv_st.at[nxt, 0, rows_a], cold, lsem.at[1])
    win_copy = pltpu.make_async_copy(conv_st.at[nxt, pl.ds(1, 2), rows_a], cw_a.at[pl.ds(0, 2)], lsem.at[2])
    r_back = pltpu.make_async_copy(rbuf, r_a, lsem.at[3])
    c_copy = pltpu.make_async_copy(cw, conv_out.at[layer], lsem.at[4])
    r_copy.start()
    w_copy(0).start()
    old_copy.start()
    win_copy.start()
    w_copy(1).start()
    w_copy(2).start()
    ex_s[...] = expand_matrix()
    core = lax.rem(lax.axis_index('tp'), 2)
    r_copy.wait()
    st_copy(nst - 1).start()
    c_copy.start()
    add_pieces(rbuf, 0, halves_of(core, feat // 2), ua, upa, va, vpa)
    r_back.start()
    norm_expand(rbuf, 0, norm_w[nxt:nxt + 1, :], hbuf, ex_s, hx)
    old_copy.wait()
    win_copy.wait()
    window = (cold, cw_a.at[0], cw_a.at[1], cw_a.at[2])

    def chunk(c, carry):
        w_copy(c).wait()

        @pl.when(c + 3 < nchunk)
        def _():
            w_copy(c + 3).start()

        for t in range(3):
            st_copy(3 * c + t).start()
        in_chunk(nxt, c, hx, wbuf, conv_w, conv_b, window, z_a, xc_a)
        return carry

    lax.fori_loop(0, nchunk, chunk, 0)
    p_a[...] = x_project(w_x[nxt], xc_a[...])
    c_copy.wait()
    r_back.wait()
    for i in range(nst):
        st_copy(i).wait()


def mid_call(layer, st, cw, residual, pieces, weights, conv_st, shapes):
    norm_w, w_in, conv_w, conv_b, w_x = weights[:5]
    feat = residual.shape[1]
    chan = w_in.shape[3]
    nchunk = chan // NCH
    vm = pltpu.VMEM
    dma = pltpu.SemaphoreType.DMA
    st, cw, *pieces = [pltpu.with_memory_space_constraint(a, pltpu.VMEM) for a in (st, cw, *pieces)]
    args = [st, cw, residual, *pieces, norm_w, w_in, conv_w, conv_b, w_x, conv_st]
    return pl.pallas_call(
        functools.partial(mid_kernel, layer),
        out_shape=[jax.ShapeDtypeStruct(shapes[0], F32), jax.ShapeDtypeStruct(shapes[1], BF16),
                   vm((HALF, chan), BF16), vm((HALF, chan), BF16), vm((w_x.shape[1], HALF), BF16),
                   vm((3, HALF, chan), BF16), jax.ShapeDtypeStruct((HALF, feat), F32)],
        in_specs=[VMEM, VMEM, ANY] + [VMEM] * 4 + [VMEM, ANY, VMEM, VMEM, VMEM, ANY],
        out_specs=[ANY, ANY, VMEM, VMEM, VMEM, VMEM, ANY],
        scratch_shapes=[vm((nchunk, 2 * feat, NCH), BF16), vm((2 * HALF, 2 * feat), BF16), vm((HALF, feat), BF16),
                        vm((128, 512), BF16), vm((HALF, feat), F32), vm((HALF, chan), BF16),
                        dma((5,)), dma((nchunk,)), dma((st.shape[0] // SB,))],
        compiler_params=pltpu.CompilerParams(vmem_limit_bytes=34 * 2 ** 20),
        cost_estimate=pl.CostEstimate(flops=2 * 10 ** 10, bytes_accessed=42 * 2 ** 20, transcendentals=0),
    )(*args)


def w_kernel(layer, st, cw_a, cw_b, ssm_prev, conv_prev, ssm_out, conv_out, sem):
    def copy(i):
        rs = pl.ds(i * SB, SB)
        return pltpu.make_async_copy(st.at[rs], ssm_out.at[layer, rs], sem.at[i])

    n = st.shape[0] // SB
    copies = [copy(i) for i in range(n)]
    for k, src in enumerate((cw_a, cw_b)):
        copies.append(pltpu.make_async_copy(src, conv_out.at[layer, :, pl.ds(k * HALF, HALF)], sem.at[n + k]))
    for c in copies:
        c.start()
    for c in copies:
        c.wait()


def w_call(layer, st, cw_a, cw_b, prev):
    args = [pltpu.with_memory_space_constraint(a, pltpu.VMEM) for a in (st, cw_a, cw_b)]
    return pl.pallas_call(
        functools.partial(w_kernel, layer),
        out_shape=[jax.ShapeDtypeStruct(a.shape, a.dtype) for a in prev],
        in_specs=[VMEM, VMEM, VMEM, ANY, ANY], out_specs=[ANY, ANY], input_output_aliases={3: 0, 4: 1},
        scratch_shapes=[pltpu.SemaphoreType.DMA((st.shape[0] // SB + 2,))],
        compiler_params=pltpu.CompilerParams(vmem_limit_bytes=2 ** 20),
        cost_estimate=pl.CostEstimate(flops=2 * 10 ** 10, bytes_accessed=42 * 2 ** 20, transcendentals=0),
    )(*args, *prev)


def fin_kernel(r_a, r_b, *refs):
    out = refs[-1]
    core = lax.rem(lax.axis_index('tp'), 2)
    half = out.shape[1] // 2
    lo = pl.ds(pl.multiple_of(core * half, 128), half)
    hi = pl.ds(pl.multiple_of((1 - core) * half, 128), half)
    for k in range(2):
        u, up, v, vp = refs[4 * k:4 * k + 4]
        rs = slice(k * HALF, (k + 1) * HALF)
        r = (r_a, r_b)[k]
        out[rs, lo] = r[:, lo] + (u[...].astype(F32) + v[...].astype(F32))
        out[rs, hi] = r[:, hi] + (up[...].astype(F32) + vp[...].astype(F32))


def fin_call(r_a, r_b, pieces):
    return pl.pallas_call(
        fin_kernel, out_shape=jax.ShapeDtypeStruct((2 * HALF, r_a.shape[1]), F32), in_specs=[VMEM] * 10, out_specs=VMEM,
        compiler_params=pltpu.CompilerParams(vmem_limit_bytes=16 * 2 ** 20), name="fin",
    )(r_a, r_b, *pieces[0], *pieces[1])


PART = [(0, 1), (1, 0), (2, 3), (3, 2)]
CROSS = [(0, 2), (2, 0), (1, 3), (3, 1)]


def solution(mesh):
    def step(residual, norm_w, w_in, conv_w, conv_b, w_x, w_dt, b_dt, a_log, d_skip, w_out, conv_state, ssm_state):
        w_xt = jnp.transpose(w_x, (0, 2, 1))
        conv_t = jnp.transpose(conv_state, (0, 2, 1, 3))
        weights = (norm_w, w_in, conv_w, conv_b, w_xt, w_dt, b_dt, a_log, d_skip, w_out)
        shapes = (ssm_state.shape, conv_t.shape)
        st, cw, ua, ub, upa, va, vpa = layer_call(0, residual, None, weights, conv_t, ssm_state)
        vb = lax.ppermute(ub, 'tp', CROSS)
        *written, z_a, xc_a, p_a, cw_a, r_a = mid_call(0, st, cw, residual, (ua, upa, va, vpa), weights, conv_t, shapes)
        ready = (ub, vb, z_a, xc_a, p_a)
        st, cw_b, ua, ub, upa, va, vpa, r_b = layer_call(1, residual, ready, weights, conv_t, ssm_state)
        vb = lax.ppermute(ub, 'tp', CROSS)
        upb = lax.ppermute(ub, 'tp', PART)
        ssm_out, conv_out = w_call(1, st, cw_a, cw_b, written)
        vpb = lax.ppermute(vb, 'tp', PART)
        out = fin_call(r_a, r_b, ((ua, upa, va, vpa), (ub, upb, vb, vpb)))
        return out, jnp.transpose(conv_out, (0, 2, 1, 3)), ssm_out

    cache_spec = P(None, 'dp', None, 'tp')
    in_specs = (P('dp', None), P(None, None), P(None, None, None, 'tp'), P(None, None, 'tp'), P(None, 'tp'), P(None, 'tp', None), P(None, None, 'tp'), P(None, 'tp'), P(None, None, 'tp'), P(None, 'tp'), P(None, 'tp', None), cache_spec, cache_spec)
    out_specs = (P('dp', None), cache_spec, cache_spec)
    return jax.shard_map(step, mesh=mesh, in_specs=in_specs, out_specs=out_specs, check_vma=False)
```

```python
import functools
import math

import jax
import jax.numpy as jnp
from jax import lax
from jax.experimental import pallas as pl
from jax.experimental.pallas import tpu as pltpu
from jax.sharding import PartitionSpec as P


F32 = jnp.float32
BF16 = jnp.bfloat16
ANY = pl.BlockSpec(memory_space=pltpu.HBM)
VMEM = pl.BlockSpec(memory_space=pltpu.VMEM)
NCH = 256
SB = 16
HALF = 128
LOG2E = math.log2(math.e)
MESH = pl.DeviceIdType.MESH


def silu(v):
    return v * jax.nn.sigmoid(v)


def expand_matrix():
    row = lax.broadcasted_iota(jnp.int32, (128, 512), 0)
    col = lax.broadcasted_iota(jnp.int32, (128, 512), 1)
    target = 2 * row + jnp.where(col < 256, 0, 257)
    return jnp.where(col == target, 1.0, 0.0).astype(BF16)


def rms0(v):
    return v * lax.rsqrt(jnp.mean(v * v, axis=0, keepdims=True) + 1e-6)


def sublane_sums(parts):
    sub = lax.broadcasted_iota(jnp.int32, parts[0].shape, 0)
    for step in (4, 2, 1):
        keep = (sub & step) == 0
        half = len(parts) // 2
        parts = [jnp.where(keep, parts[k], parts[k + half])
                 + pltpu.roll(jnp.where(keep, parts[k + half], parts[k]), step, 0) if step == 4 else
                 jnp.where(keep, parts[k], parts[k + half])
                 + jnp.where(keep, pltpu.roll(parts[k], 8 - step, 0), pltpu.roll(parts[k + half], step, 0))
                 for k in range(half)]
    return parts[0]


def add_pieces(rbuf, start, sides, u, up, v, vp):
    lo, hi = sides

    def add(i, carry):
        src = pl.ds(pl.multiple_of(i * 32, 32), 32)
        dst = pl.ds(pl.multiple_of(i * 32, 32) + start, 32)
        rbuf[dst, lo] = rbuf[dst, lo] + (u[src, :].astype(F32) + v[src, :].astype(F32))
        rbuf[dst, hi] = rbuf[dst, hi] + (up[src, :].astype(F32) + vp[src, :].astype(F32))
        return carry

    lax.fori_loop(0, HALF // 32, add, 0)


def norm_expand(rbuf, start, norm_row, hbuf, ex_s, hx):
    nw = norm_row.astype(F32)
    feat = rbuf.shape[1]

    def norm(i, carry):
        off = pl.multiple_of(i * 32, 32)
        r = rbuf[pl.ds(off + start, 32), :]
        inv = lax.rsqrt(jnp.mean(r * r, axis=-1, keepdims=True) + 1e-5)
        hbuf[pl.ds(off, 32), :] = (r * inv * nw).astype(BF16)
        return carry

    lax.fori_loop(0, HALF // 32, norm, 0)

    def expand(j, carry):
        for t in range(4):
            src = pl.ds(pl.multiple_of(j * 512 + t * 128, 128), 128)
            e = jnp.dot(hbuf[:, src], ex_s[...], preferred_element_type=F32).astype(BF16)
            cols = pl.ds(pl.multiple_of(j * 1024 + t * 256, 256), 256)
            hx[0:HALF, cols] = e[:, :256]
            hx[HALF:2 * HALF, cols] = e[:, 256:]
        return carry

    lax.fori_loop(0, feat // 512, expand, 0)


def cols_of(c):
    return pl.ds(pl.multiple_of(c * NCH, NCH), NCH)


def in_chunk(layer, c, hx, wbuf, conv_w, conv_b, window, z_out, xc_out):
    old0, old1, old2, x_out = window
    sl = cols_of(c)
    acc = jnp.dot(hx[...], wbuf[c], preferred_element_type=F32)
    x = acc[:HALF].astype(BF16)
    z_out[:, sl] = acc[HALF:].astype(BF16)
    x_out[:, sl] = x
    taps = conv_w[layer, :, sl].astype(F32)
    pre = old0[:, sl].astype(F32) * taps[0:1] + old1[:, sl].astype(F32) * taps[1:2]
    pre = pre + old2[:, sl].astype(F32) * taps[2:3] + x.astype(F32) * taps[3:4]
    pre = pre + conv_b[layer:layer + 1, sl].astype(F32)
    xc_out[:, sl] = silu(pre).astype(BF16)


def x_project(w_x_layer, xc):
    return lax.dot_general(w_x_layer, xc, (((1,), (1,)), ((), ())), preferred_element_type=F32).astype(BF16)


def halves_of(core, half):
    return (pl.ds(pl.multiple_of(core * half, 128), half), pl.ds(pl.multiple_of((1 - core) * half, 128), half))


def layer_kernel(layer, first, *refs):
    refs = list(refs)
    res = refs.pop(0)
    if not first:
        ub_in, vb_in, z_a, xc_a, p_a = refs[:5]
        refs = refs[5:]
    (norm_w, w_in, conv_w, conv_b, w_x, conv_st, w_dt, b_dt, a_log, d_skip, w_out, state) = refs[:12]
    refs = refs[12:]
    st, cw, ua, ub, upa, va, vpa = refs[:7]
    refs = refs[7:]
    r_out = None if first else refs.pop(0)
    (wbuf, hx, hbuf, ex_s, p_own, p_sw, p_cs, p_v, rbuf, cold, z_s, xc_s, dt_s, bc_s, a_s, y_s, part,
     mine_a, mine_b, theirs_a, theirs_b, got_a, got_b, upb, vpb, lsem, wsem, stsem, osem, ssem, rsem) = refs
    feat = rbuf.shape[1]
    nchunk = wbuf.shape[0]
    chan = z_s.shape[1]
    rank = w_dt.shape[1]
    nst = a_s.shape[0]
    nblk = HALF // SB
    half = feat // 2
    quarter = HALF // 2
    w_flat = w_in.reshape(w_in.shape[0], 2 * feat, w_in.shape[3])
    in_halves = (0, 1) if first else (1,)

    me = lax.axis_index('tp')
    core = lax.rem(me, 2)
    partner = me + 1 - 2 * core
    other = lax.rem(me + 2, 4)
    barrier = pltpu.get_barrier_semaphore()
    for dev in (partner, other):
        pl.semaphore_signal(barrier, inc=1, device_id={'tp': dev}, device_id_type=MESH)

    def send(src, dst, k, dev):
        return pltpu.make_async_remote_copy(src_ref=src, dst_ref=dst, send_sem=ssem.at[k], recv_sem=rsem.at[k],
                                            device_id={'tp': dev}, device_id_type=MESH)

    def half_rows(k):
        return pl.ds(k * HALF, HALF)

    def held_rows(k):
        return pl.ds(k * HALF if first else 0, HALF)

    def r_copy(k):
        return pltpu.make_async_copy(res.at[half_rows(k)], rbuf.at[held_rows(k)], lsem.at[k])

    nwin = cold.shape[0]
    win_rows = pl.ds(0 if first else HALF, nwin)
    old_copy = pltpu.make_async_copy(conv_st.at[layer, 0, win_rows], cold, lsem.at[2])
    win_copy = pltpu.make_async_copy(conv_st.at[layer, pl.ds(1, 2), win_rows], cw.at[pl.ds(0, 2)], lsem.at[3])

    def w_copy(c):
        return pltpu.make_async_copy(w_flat.at[layer, :, cols_of(c)], wbuf.at[c], wsem.at[c])

    def st_copy(i):
        rs = pl.ds(i * SB, SB)
        return pltpu.make_async_copy(state.at[layer, rs], st.at[rs], stsem.at[i])

    def out_tile(j):
        return wbuf.at[j // 4, pl.ds(pl.multiple_of(lax.rem(j, 4) * chan, 128), chan)]

    def o_copy(j):
        return pltpu.make_async_copy(w_out.at[layer, :, cols_of(j)], out_tile(j), osem.at[j])

    r_copy(in_halves[0]).start()
    w_copy(0).start()
    if first:
        r_copy(1).start()
    w_copy(1).start()
    old_copy.start()
    win_copy.start()
    w_copy(2).start()
    ex_s[...] = expand_matrix()
    a_s[...] = -jnp.exp(a_log[layer]) * LOG2E
    pl.semaphore_wait(barrier, 2)
    relays = []
    if not first:
        relays = [send(vb_in, vpb, 11, partner), send(ub_in, upb, 14, partner)]
        for c in relays:
            c.start()

    def p_first(k):
        return send(p_own.at[k], p_sw.at[k], k, partner)

    def p_second(k):
        return send(p_cs.at[k], p_v.at[k], 2 + k, other)

    def p_middle(k):
        p_first(k).wait_recv()
        p_cs[k] = (p_own[k].astype(F32) + p_sw[k].astype(F32)).astype(BF16)
        p_second(k).start()

    if not first:
        p_own[0] = p_a[...]
        p_first(0).start()
        xc_s[0:HALF, :] = xc_a[...]
        z_s[0:HALF, :] = z_a[...]
    for k in in_halves:
        start = k * HALF if first else 0
        r_copy(k).wait()
        if not first:
            for c in relays:
                c.wait_recv()
            add_pieces(rbuf, start, halves_of(core, half), ub_in, upb, vb_in, vpb)
            pltpu.make_async_copy(rbuf, r_out, lsem.at[4]).start()
        norm_expand(rbuf, start, norm_w[layer:layer + 1, :], hbuf, ex_s, hx)
        if k == in_halves[0]:
            old_copy.wait()
            win_copy.wait()

        def chunk(c, carry, k=k):
            if k == in_halves[0]:
                w_copy(c).wait()

                @pl.when(c + 3 < nchunk)
                def _():
                    w_copy(c + 3).start()

            if k == 1:
                for t in range(3):
                    st_copy(3 * c + t).start()
            held = held_rows(k)
            window = (cold.at[held], cw.at[0, held], cw.at[1, held], cw.at[2, held])
            in_chunk(layer, c, hx, wbuf, conv_w, conv_b, window, z_s.at[half_rows(k)], xc_s.at[half_rows(k)])
            if k == 1:
                @pl.when(c < 2)
                def _():
                    for t in range(4):
                        o_copy(4 * c + t).start()

                @pl.when(c == 2)
                def _():
                    for t in range(2):
                        o_copy(8 + t).start()
                    p_middle(0)

            return carry

        lax.fori_loop(0, nchunk, chunk, 0)
        p_own[k] = x_project(w_x[layer], xc_s[half_rows(k), :])
        p_first(k).start()
    st_copy(2 * nblk - 1).start()

    def red_a(q):
        return send(theirs_a.at[q], got_a.at[q], 4 + q, partner)

    red_b = send(theirs_b, got_b, 6, partner)

    def quarter_rows(q):
        return pl.ds(q * quarter, quarter)

    def cross(q):
        return send(ua.at[quarter_rows(q)], va.at[quarter_rows(q)], 7 + q, other)

    def up_a(q):
        return send(ua.at[quarter_rows(q)], upa.at[quarter_rows(q)], 9 + q, partner)

    def forward(q):
        return send(va.at[quarter_rows(q)], vpa.at[quarter_rows(q)], 12 + q, partner)

    def reduce_a(q):
        red_a(q).wait_recv()
        ua[quarter_rows(q), :] = (mine_a[q] + got_a[q].astype(F32)).astype(BF16)
        cross(q).start()
        up_a(q).start()

    lane = lax.broadcasted_iota(jnp.int32, (nst, 128), 1)
    row = lax.broadcasted_iota(jnp.int32, (nst, 128), 0)

    def gated(rs, y):
        y = y + d_skip[layer:layer + 1, :] * xc_s[rs, :].astype(F32)
        return (y * silu(z_s[rs, :].astype(F32))).astype(BF16)

    def project(yg, first, dst, dtype):
        for t in range(half // NCH):
            j = first * (half // NCH) + t
            dst[:, t * NCH:(t + 1) * NCH] = jnp.dot(yg, out_tile(j)[...], preferred_element_type=F32).astype(dtype)

    for k in range(2):
        p_second(k).wait_recv()
        p = p_cs[k].astype(F32) + p_v[k].astype(F32)
        low = rms0(p[:rank]).astype(BF16)
        pre = lax.dot_general(low, w_dt[layer], (((0,), (0,)), ((), ())), preferred_element_type=F32)
        pre = pre + b_dt[layer:layer + 1, :]
        dt_s[...] = jnp.maximum(pre, 0.0) + jnp.log1p(jnp.exp(-jnp.abs(pre)))
        bc = jnp.concatenate([rms0(p[rank:rank + nst]), rms0(p[rank + nst:])], axis=0)
        bc_s[:, 0:2 * nst] = jnp.transpose(bc)
        if k == 1:
            reduce_a(1)

        def block(i, carry, k=k):
            st_copy(i + k * nblk).wait()
            local = pl.multiple_of(i * SB, SB)
            base = local + k * HALF
            dt = dt_s[pl.ds(local, SB), :]
            dtx = dt * xc_s[pl.ds(base, SB), :].astype(F32)
            bc = bc_s[pl.ds(local, SB), :]
            a2 = a_s[...]
            for b in range(SB):
                bcb = jnp.broadcast_to(bc[b:b + 1, :], (nst, 128))
                bcol = jnp.sum(jnp.where(lane == row, bcb, 0.0), axis=1, keepdims=True)
                ccol = jnp.sum(jnp.where(lane == row + nst, bcb, 0.0), axis=1, keepdims=True)
                s = jnp.exp2(dt[b:b + 1, :] * a2) * st[base + b] + dtx[b:b + 1, :] * bcol
                st[base + b] = s
                t = s * ccol
                part[b] = t[0:8] + t[8:16]
            for g in range(SB // 8):
                y_s[pl.ds(local + 8 * g, 8), :] = sublane_sums([part[8 * g + n] for n in range(8)])

            if k == 0:
                @pl.when(i == 2)
                def _():
                    p_middle(1)

                @pl.when(i == nblk // 2 - 1)
                def _():
                    for j in range(feat // NCH):
                        o_copy(j).wait()

                @pl.when(lax.rem(i, nblk // 2) == nblk // 2 - 1)
                def _():
                    q = i // (nblk // 2)
                    rs = pl.ds(pl.multiple_of(q * quarter, quarter), quarter)
                    yg = gated(rs, y_s[rs, :])
                    project(yg, 1 - core, theirs_a.at[q], BF16)
                    red_a(q).start()
                    project(yg, core, mine_a.at[q], F32)

                @pl.when(i == nblk // 2)
                def _():
                    reduce_a(0)

            return carry

        lax.fori_loop(0, nblk, block, 0)

    yg = gated(half_rows(1), y_s[...])
    project(yg, 1 - core, theirs_b, BF16)
    red_b.start()
    project(yg, core, mine_b, F32)
    cross(0).wait_recv()
    forward(0).start()
    red_b.wait_recv()
    ub[...] = (mine_b[...] + got_b[...].astype(F32)).astype(BF16)
    cross(1).wait_recv()
    forward(1).start()
    for q in range(2):
        up_a(q).wait_recv()
    for q in range(2):
        forward(q).wait_recv()
    for k in range(2):
        p_first(k).wait_send()
        p_second(k).wait_send()
        red_a(k).wait_send()
        cross(k).wait_send()
        up_a(k).wait_send()
        forward(k).wait_send()
    red_b.wait_send()
    for c in relays:
        c.wait_send()
    if not first:
        pltpu.make_async_copy(rbuf, r_out, lsem.at[4]).wait()


def layer_call(layer, residual, ready, weights, conv_st, state):
    norm_w, w_in, conv_w, conv_b, w_x, w_dt, b_dt, a_log, d_skip, w_out = weights
    first = ready is None
    rows, feat = residual.shape
    chan = w_in.shape[3]
    nst = a_log.shape[1]
    half = feat // 2
    nproj = w_x.shape[1]
    nchunk = chan // NCH
    flat = [] if first else [pltpu.with_memory_space_constraint(a, pltpu.VMEM) for a in ready]
    held = rows if first else HALF
    args = [residual] + flat + [norm_w, w_in, conv_w, conv_b, w_x, conv_st, w_dt, b_dt, a_log, d_skip, w_out, state]
    specs = [ANY] + [VMEM] * len(flat) + [VMEM, ANY, VMEM, VMEM, VMEM, ANY, VMEM, VMEM, VMEM, VMEM, ANY, ANY]
    piece = pltpu.VMEM((HALF, half), BF16)
    outs = [pltpu.VMEM((rows, nst, chan), F32), pltpu.VMEM((3, held, chan), BF16)] + [piece] * 5
    out_specs = [VMEM] * 7
    if not first:
        outs.append(jax.ShapeDtypeStruct((HALF, feat), F32))
        out_specs.append(ANY)
    vm = pltpu.VMEM
    dma = pltpu.SemaphoreType.DMA
    quarter = HALF // 2
    return pl.pallas_call(
        functools.partial(layer_kernel, layer, first),
        out_shape=outs, in_specs=specs, out_specs=out_specs,
        scratch_shapes=[
            vm((nchunk, 2 * feat, NCH), BF16), vm((2 * HALF, 2 * feat), BF16), vm((HALF, feat), BF16), vm((128, 512), BF16),
            vm((2, nproj, HALF), BF16), vm((2, nproj, HALF), BF16), vm((2, nproj, HALF), BF16),
            vm((2, nproj, HALF), BF16), vm((held, feat), F32), vm((held, chan), BF16), vm((rows, chan), BF16),
            vm((rows, chan), BF16), vm((HALF, chan), F32), vm((HALF, 128), F32), vm((nst, chan), F32), vm((HALF, chan), F32),
            vm((SB, 8, chan), F32), vm((2, quarter, half), F32), vm((HALF, half), F32), vm((2, quarter, half), BF16),
            vm((HALF, half), BF16), vm((2, quarter, half), BF16), vm((HALF, half), BF16), vm((HALF, half), BF16),
            vm((HALF, half), BF16),
            dma((5,)), dma((nchunk,)), dma((rows // SB,)), dma((feat // NCH,)), dma((15,)), dma((15,)),
        ],
        compiler_params=pltpu.CompilerParams(vmem_limit_bytes=34 * 2 ** 20, collective_id=layer, has_side_effects=True),
        cost_estimate=pl.CostEstimate(flops=2 * 10 ** 10, bytes_accessed=46 * 2 ** 20, transcendentals=0),
    )(*args)


def mid_kernel(layer, st, cw, res, ua, upa, va, vpa, norm_w, w_in, conv_w, conv_b, w_x, conv_st,
               ssm_out, conv_out, z_a, xc_a, p_a, cw_a, r_a,
               wbuf, hx, hbuf, ex_s, rbuf, cold, lsem, wsem, sem):
    feat = rbuf.shape[1]
    nchunk = wbuf.shape[0]
    nxt = layer + 1
    w_flat = w_in.reshape(w_in.shape[0], 2 * feat, w_in.shape[3])
    rows_a = pl.ds(0, HALF)

    def w_copy(c):
        return pltpu.make_async_copy(w_flat.at[nxt, :, cols_of(c)], wbuf.at[c], wsem.at[c])

    def st_copy(i):
        rs = pl.ds(i * SB, SB)
        return pltpu.make_async_copy(st.at[rs], ssm_out.at[layer, rs], sem.at[i])

    nst = st.shape[0] // SB
    r_copy = pltpu.make_async_copy(res.at[rows_a], rbuf, lsem.at[0])
    old_copy = pltpu.make_async_copy(conv_st.at[nxt, 0, rows_a], cold, lsem.at[1])
    win_copy = pltpu.make_async_copy(conv_st.at[nxt, pl.ds(1, 2), rows_a], cw_a.at[pl.ds(0, 2)], lsem.at[2])
    r_back = pltpu.make_async_copy(rbuf, r_a, lsem.at[3])
    c_copy = pltpu.make_async_copy(cw, conv_out.at[layer], lsem.at[4])
    r_copy.start()
    w_copy(0).start()
    old_copy.start()
    win_copy.start()
    w_copy(1).start()
    w_copy(2).start()
    ex_s[...] = expand_matrix()
    core = lax.rem(lax.axis_index('tp'), 2)
    r_copy.wait()
    w_copy(3).start()
    st_copy(nst - 1).start()
    c_copy.start()
    add_pieces(rbuf, 0, halves_of(core, feat // 2), ua, upa, va, vpa)
    r_back.start()
    norm_expand(rbuf, 0, norm_w[nxt:nxt + 1, :], hbuf, ex_s, hx)
    old_copy.wait()
    win_copy.wait()
    window = (cold, cw_a.at[0], cw_a.at[1], cw_a.at[2])

    def chunk(c, carry):
        w_copy(c).wait()

        @pl.when(c + 4 < nchunk)
        def _():
            w_copy(c + 4).start()

        for t in range(3):
            st_copy(3 * c + t).start()
        in_chunk(nxt, c, hx, wbuf, conv_w, conv_b, window, z_a, xc_a)
        return carry

    lax.fori_loop(0, nchunk, chunk, 0)
    p_a[...] = x_project(w_x[nxt], xc_a[...])
    c_copy.wait()
    r_back.wait()
    for i in range(nst):
        st_copy(i).wait()


def mid_call(layer, st, cw, residual, pieces, weights, conv_st, shapes):
    norm_w, w_in, conv_w, conv_b, w_x = weights[:5]
    feat = residual.shape[1]
    chan = w_in.shape[3]
    nchunk = chan // NCH
    vm = pltpu.VMEM
    dma = pltpu.SemaphoreType.DMA
    st, cw, *pieces = [pltpu.with_memory_space_constraint(a, pltpu.VMEM) for a in (st, cw, *pieces)]
    args = [st, cw, residual, *pieces, norm_w, w_in, conv_w, conv_b, w_x, conv_st]
    return pl.pallas_call(
        functools.partial(mid_kernel, layer),
        out_shape=[jax.ShapeDtypeStruct(shapes[0], F32), jax.ShapeDtypeStruct(shapes[1], BF16),
                   vm((HALF, chan), BF16), vm((HALF, chan), BF16), vm((w_x.shape[1], HALF), BF16),
                   vm((3, HALF, chan), BF16), jax.ShapeDtypeStruct((HALF, feat), F32)],
        in_specs=[VMEM, VMEM, ANY] + [VMEM] * 4 + [VMEM, ANY, VMEM, VMEM, VMEM, ANY],
        out_specs=[ANY, ANY, VMEM, VMEM, VMEM, VMEM, ANY],
        scratch_shapes=[vm((nchunk, 2 * feat, NCH), BF16), vm((2 * HALF, 2 * feat), BF16), vm((HALF, feat), BF16),
                        vm((128, 512), BF16), vm((HALF, feat), F32), vm((HALF, chan), BF16),
                        dma((5,)), dma((nchunk,)), dma((st.shape[0] // SB,))],
        compiler_params=pltpu.CompilerParams(vmem_limit_bytes=34 * 2 ** 20),
        cost_estimate=pl.CostEstimate(flops=2 * 10 ** 10, bytes_accessed=42 * 2 ** 20, transcendentals=0),
    )(*args)


def w_kernel(layer, st, cw_a, cw_b, ssm_prev, conv_prev, ssm_out, conv_out, sem):
    def copy(i):
        rs = pl.ds(i * SB, SB)
        return pltpu.make_async_copy(st.at[rs], ssm_out.at[layer, rs], sem.at[i])

    n = st.shape[0] // SB
    copies = [copy(i) for i in range(n)]
    for k, src in enumerate((cw_a, cw_b)):
        copies.append(pltpu.make_async_copy(src, conv_out.at[layer, :, pl.ds(k * HALF, HALF)], sem.at[n + k]))
    for c in copies:
        c.start()
    for c in copies:
        c.wait()


def w_call(layer, st, cw_a, cw_b, prev):
    args = [pltpu.with_memory_space_constraint(a, pltpu.VMEM) for a in (st, cw_a, cw_b)]
    return pl.pallas_call(
        functools.partial(w_kernel, layer),
        out_shape=[jax.ShapeDtypeStruct(a.shape, a.dtype) for a in prev],
        in_specs=[VMEM, VMEM, VMEM, ANY, ANY], out_specs=[ANY, ANY], input_output_aliases={3: 0, 4: 1},
        scratch_shapes=[pltpu.SemaphoreType.DMA((st.shape[0] // SB + 2,))],
        compiler_params=pltpu.CompilerParams(vmem_limit_bytes=2 ** 20),
        cost_estimate=pl.CostEstimate(flops=2 * 10 ** 10, bytes_accessed=42 * 2 ** 20, transcendentals=0),
    )(*args, *prev)


def fin_kernel(r_a, r_b, *refs):
    out = refs[-1]
    core = lax.rem(lax.axis_index('tp'), 2)
    half = out.shape[1] // 2
    lo = pl.ds(pl.multiple_of(core * half, 128), half)
    hi = pl.ds(pl.multiple_of((1 - core) * half, 128), half)
    for k in range(2):
        u, up, v, vp = refs[4 * k:4 * k + 4]
        rs = slice(k * HALF, (k + 1) * HALF)
        r = (r_a, r_b)[k]
        out[rs, lo] = r[:, lo] + (u[...].astype(F32) + v[...].astype(F32))
        out[rs, hi] = r[:, hi] + (up[...].astype(F32) + vp[...].astype(F32))


def fin_call(r_a, r_b, pieces):
    return pl.pallas_call(
        fin_kernel, out_shape=jax.ShapeDtypeStruct((2 * HALF, r_a.shape[1]), F32), in_specs=[VMEM] * 10, out_specs=VMEM,
        compiler_params=pltpu.CompilerParams(vmem_limit_bytes=16 * 2 ** 20), name="fin",
    )(r_a, r_b, *pieces[0], *pieces[1])


PART = [(0, 1), (1, 0), (2, 3), (3, 2)]
CROSS = [(0, 2), (2, 0), (1, 3), (3, 1)]


def solution(mesh):
    def step(residual, norm_w, w_in, conv_w, conv_b, w_x, w_dt, b_dt, a_log, d_skip, w_out, conv_state, ssm_state):
        w_xt = jnp.transpose(w_x, (0, 2, 1))
        conv_t = jnp.transpose(conv_state, (0, 2, 1, 3))
        weights = (norm_w, w_in, conv_w, conv_b, w_xt, w_dt, b_dt, a_log, d_skip, w_out)
        shapes = (ssm_state.shape, conv_t.shape)
        st, cw, ua, ub, upa, va, vpa = layer_call(0, residual, None, weights, conv_t, ssm_state)
        vb = lax.ppermute(ub, 'tp', CROSS)
        *written, z_a, xc_a, p_a, cw_a, r_a = mid_call(0, st, cw, residual, (ua, upa, va, vpa), weights, conv_t, shapes)
        ready = (ub, vb, z_a, xc_a, p_a)
        st, cw_b, ua, ub, upa, va, vpa, r_b = layer_call(1, residual, ready, weights, conv_t, ssm_state)
        vb = lax.ppermute(ub, 'tp', CROSS)
        upb = lax.ppermute(ub, 'tp', PART)
        ssm_out, conv_out = w_call(1, st, cw_a, cw_b, written)
        vpb = lax.ppermute(vb, 'tp', PART)
        out = fin_call(r_a, r_b, ((ua, upa, va, vpa), (ub, upb, vb, vpb)))
        return out, jnp.transpose(conv_out, (0, 2, 1, 3)), ssm_out

    cache_spec = P(None, 'dp', None, 'tp')
    in_specs = (P('dp', None), P(None, None), P(None, None, None, 'tp'), P(None, None, 'tp'), P(None, 'tp'), P(None, 'tp', None), P(None, None, 'tp'), P(None, 'tp'), P(None, None, 'tp'), P(None, 'tp'), P(None, 'tp', None), cache_spec, cache_spec)
    out_specs = (P('dp', None), cache_spec, cache_spec)
    return jax.shard_map(step, mesh=mesh, in_specs=in_specs, out_specs=out_specs, check_vma=False)
```

```python
import functools
import math

import jax
import jax.numpy as jnp
from jax import lax
from jax.experimental import pallas as pl
from jax.experimental.pallas import tpu as pltpu
from jax.sharding import PartitionSpec as P


F32 = jnp.float32
BF16 = jnp.bfloat16
ANY = pl.BlockSpec(memory_space=pltpu.HBM)
VMEM = pl.BlockSpec(memory_space=pltpu.VMEM)
NCH = 256
SB = 16
HALF = 128
SPLIT = 512
LOG2E = math.log2(math.e)
MESH = pl.DeviceIdType.MESH


def silu(v):
    return v * jax.nn.sigmoid(v)


def order_matrix():
    row = lax.broadcasted_iota(jnp.int32, (128, 128), 0)
    col = lax.broadcasted_iota(jnp.int32, (128, 128), 1)
    low = col & 7
    source = col - low + (low >> 1) + 4 * (low & 1)
    return jnp.where(row == source, 1.0, 0.0).astype(BF16)


def split_rows(wbuf, c):
    even = (lax.broadcasted_iota(jnp.int32, (SPLIT // 16, 8, NCH), 1) & 1) == 0

    def block(b, carry):
        start = b * SPLIT
        v = wbuf[c, pl.ds(start, SPLIT), :].astype(F32).reshape(SPLIT // 16, 2, 8, NCH)
        first, second = v[:, 0], v[:, 1]
        x = jnp.where(even, first, pltpu.roll(second, 1, 1))
        z = jnp.where(even, pltpu.roll(first, 7, 1), second)
        wbuf[c, pl.ds(start, SPLIT // 2), :] = x.reshape(SPLIT // 2, NCH).astype(BF16)
        wbuf[c, pl.ds(start + SPLIT // 2, SPLIT // 2), :] = z.reshape(SPLIT // 2, NCH).astype(BF16)
        return carry

    for b in range(wbuf.shape[1] // SPLIT):
        block(b, 0)


def split_half(wbuf, c, side):
    half = SPLIT // 2
    return jnp.concatenate([wbuf[c, b * SPLIT + side * half:b * SPLIT + (side + 1) * half, :]
                            for b in range(wbuf.shape[1] // SPLIT)], axis=0)


def rms0(v):
    return v * lax.rsqrt(jnp.mean(v * v, axis=0, keepdims=True) + 1e-6)


def sublane_sums(parts):
    sub = lax.broadcasted_iota(jnp.int32, parts[0].shape, 0)
    for step in (4, 2, 1):
        keep = (sub & step) == 0
        half = len(parts) // 2
        parts = [jnp.where(keep, parts[k], parts[k + half])
                 + pltpu.roll(jnp.where(keep, parts[k + half], parts[k]), step, 0) if step == 4 else
                 jnp.where(keep, parts[k], parts[k + half])
                 + jnp.where(keep, pltpu.roll(parts[k], 8 - step, 0), pltpu.roll(parts[k + half], step, 0))
                 for k in range(half)]
    return parts[0]


def add_pieces(rbuf, start, sides, u, up, v, vp):
    lo, hi = sides

    def add(i, carry):
        src = pl.ds(pl.multiple_of(i * 32, 32), 32)
        dst = pl.ds(pl.multiple_of(i * 32, 32) + start, 32)
        rbuf[dst, lo] = rbuf[dst, lo] + (u[src, :].astype(F32) + v[src, :].astype(F32))
        rbuf[dst, hi] = rbuf[dst, hi] + (up[src, :].astype(F32) + vp[src, :].astype(F32))
        return carry

    lax.fori_loop(0, HALF // 32, add, 0)


def norm_expand(rbuf, start, norm_row, hbuf, ex_s, hx):
    nw = norm_row.astype(F32)
    feat = rbuf.shape[1]

    def norm(i, carry):
        off = pl.multiple_of(i * 32, 32)
        r = rbuf[pl.ds(off + start, 32), :]
        inv = lax.rsqrt(jnp.mean(r * r, axis=-1, keepdims=True) + 1e-5)
        hbuf[pl.ds(off, 32), :] = (r * inv * nw).astype(BF16)
        return carry

    lax.fori_loop(0, HALF // 32, norm, 0)

    def expand(j, carry):
        for t in range(4):
            cols = pl.ds(pl.multiple_of(j * 512 + t * 128, 128), 128)
            hx[:, cols] = jnp.dot(hbuf[:, cols], ex_s[...], preferred_element_type=F32).astype(BF16)
        return carry

    lax.fori_loop(0, feat // 512, expand, 0)


def cols_of(c):
    return pl.ds(pl.multiple_of(c * NCH, NCH), NCH)


def in_chunk(layer, c, hx, wbuf, conv_w, conv_b, window, z_out, xc_out):
    old0, old1, old2, x_out = window
    sl = cols_of(c)
    x = jnp.dot(hx[...], split_half(wbuf, c, 0), preferred_element_type=F32).astype(BF16)
    z_out[:, sl] = jnp.dot(hx[...], split_half(wbuf, c, 1), preferred_element_type=F32).astype(BF16)
    x_out[:, sl] = x
    taps = conv_w[layer, :, sl].astype(F32)
    pre = old0[:, sl].astype(F32) * taps[0:1] + old1[:, sl].astype(F32) * taps[1:2]
    pre = pre + old2[:, sl].astype(F32) * taps[2:3] + x.astype(F32) * taps[3:4]
    pre = pre + conv_b[layer:layer + 1, sl].astype(F32)
    xc_out[:, sl] = silu(pre).astype(BF16)


def x_project(w_x_layer, xc):
    return lax.dot_general(w_x_layer, xc, (((1,), (1,)), ((), ())), preferred_element_type=F32).astype(BF16)


def halves_of(core, half):
    return (pl.ds(pl.multiple_of(core * half, 128), half), pl.ds(pl.multiple_of((1 - core) * half, 128), half))


def layer_kernel(layer, first, *refs):
    refs = list(refs)
    res = refs.pop(0)
    if not first:
        ub_in, vb_in, z_a, xc_a, p_a = refs[:5]
        refs = refs[5:]
    (norm_w, w_in, conv_w, conv_b, w_x, conv_st, w_dt, b_dt, a_log, d_skip, w_out, state) = refs[:12]
    refs = refs[12:]
    st, cw, ua, ub, upa, va, vpa = refs[:7]
    refs = refs[7:]
    r_out = None if first else refs.pop(0)
    (wbuf, hx, hbuf, ex_s, p_own, p_sw, p_cs, p_v, rbuf, cold, z_s, xc_s, dt_s, bc_s, a_s, y_s, part,
     mine_a, mine_b, theirs_a, theirs_b, got_a, got_b, upb, vpb, lsem, wsem, stsem, osem, ssem, rsem) = refs
    feat = rbuf.shape[1]
    nchunk = wbuf.shape[0]
    chan = z_s.shape[1]
    rank = w_dt.shape[1]
    nst = a_s.shape[0]
    nblk = HALF // SB
    half = feat // 2
    quarter = HALF // 2
    w_flat = w_in.reshape(w_in.shape[0], 2 * feat, w_in.shape[3])
    in_halves = (0, 1) if first else (1,)

    me = lax.axis_index('tp')
    core = lax.rem(me, 2)
    partner = me + 1 - 2 * core
    other = lax.rem(me + 2, 4)
    barrier = pltpu.get_barrier_semaphore()
    for dev in (partner, other):
        pl.semaphore_signal(barrier, inc=1, device_id={'tp': dev}, device_id_type=MESH)

    def send(src, dst, k, dev):
        return pltpu.make_async_remote_copy(src_ref=src, dst_ref=dst, send_sem=ssem.at[k], recv_sem=rsem.at[k],
                                            device_id={'tp': dev}, device_id_type=MESH)

    def half_rows(k):
        return pl.ds(k * HALF, HALF)

    def held_rows(k):
        return pl.ds(k * HALF if first else 0, HALF)

    def r_copy(k):
        return pltpu.make_async_copy(res.at[half_rows(k)], rbuf.at[held_rows(k)], lsem.at[k])

    nwin = cold.shape[0]
    win_rows = pl.ds(0 if first else HALF, nwin)
    old_copy = pltpu.make_async_copy(conv_st.at[layer, 0, win_rows], cold, lsem.at[2])
    win_copy = pltpu.make_async_copy(conv_st.at[layer, pl.ds(1, 2), win_rows], cw.at[pl.ds(0, 2)], lsem.at[3])

    def w_copy(c):
        return pltpu.make_async_copy(w_flat.at[layer, :, cols_of(c)], wbuf.at[c], wsem.at[c])

    def st_copy(i):
        rs = pl.ds(i * SB, SB)
        return pltpu.make_async_copy(state.at[layer, rs], st.at[rs], stsem.at[i])

    def out_tile(j):
        return wbuf.at[j // 4, pl.ds(pl.multiple_of(lax.rem(j, 4) * chan, 128), chan)]

    def o_copy(j):
        return pltpu.make_async_copy(w_out.at[layer, :, cols_of(j)], out_tile(j), osem.at[j])

    r_copy(in_halves[0]).start()
    w_copy(0).start()
    if first:
        r_copy(1).start()
    w_copy(1).start()
    old_copy.start()
    win_copy.start()
    w_copy(2).start()
    ex_s[...] = order_matrix()
    a_s[...] = -jnp.exp(a_log[layer]) * LOG2E
    pl.semaphore_wait(barrier, 2)
    relays = []
    if not first:
        relays = [send(vb_in, vpb, 11, partner), send(ub_in, upb, 14, partner)]
        for c in relays:
            c.start()

    def p_first(k):
        return send(p_own.at[k], p_sw.at[k], k, partner)

    def p_second(k):
        return send(p_cs.at[k], p_v.at[k], 2 + k, other)

    def p_middle(k):
        p_first(k).wait_recv()
        p_cs[k] = (p_own[k].astype(F32) + p_sw[k].astype(F32)).astype(BF16)
        p_second(k).start()

    if not first:
        p_own[0] = p_a[...]
        p_first(0).start()
        xc_s[0:HALF, :] = xc_a[...]
        z_s[0:HALF, :] = z_a[...]
    for k in in_halves:
        start = k * HALF if first else 0
        r_copy(k).wait()
        if not first:
            for c in relays:
                c.wait_recv()
            add_pieces(rbuf, start, halves_of(core, half), ub_in, upb, vb_in, vpb)
            pltpu.make_async_copy(rbuf, r_out, lsem.at[4]).start()
        norm_expand(rbuf, start, norm_w[layer:layer + 1, :], hbuf, ex_s, hx)
        if k == in_halves[0]:
            old_copy.wait()
            win_copy.wait()

        def chunk(c, carry, k=k):
            if k == in_halves[0]:
                w_copy(c).wait()

                @pl.when(c + 3 < nchunk)
                def _():
                    w_copy(c + 3).start()

                split_rows(wbuf, c)

            if k == 1:
                for t in range(3):
                    st_copy(3 * c + t).start()
            held = held_rows(k)
            window = (cold.at[held], cw.at[0, held], cw.at[1, held], cw.at[2, held])
            in_chunk(layer, c, hx, wbuf, conv_w, conv_b, window, z_s.at[half_rows(k)], xc_s.at[half_rows(k)])
            if k == 1:
                @pl.when(c < 2)
                def _():
                    for t in range(4):
                        o_copy(4 * c + t).start()

                @pl.when(c == 2)
                def _():
                    for t in range(2):
                        o_copy(8 + t).start()
                    p_middle(0)

            return carry

        lax.fori_loop(0, nchunk, chunk, 0)
        p_own[k] = x_project(w_x[layer], xc_s[half_rows(k), :])
        p_first(k).start()
    st_copy(2 * nblk - 1).start()

    def red_a(q):
        return send(theirs_a.at[q], got_a.at[q], 4 + q, partner)

    red_b = send(theirs_b, got_b, 6, partner)

    def quarter_rows(q):
        return pl.ds(q * quarter, quarter)

    def cross(q):
        return send(ua.at[quarter_rows(q)], va.at[quarter_rows(q)], 7 + q, other)

    def up_a(q):
        return send(ua.at[quarter_rows(q)], upa.at[quarter_rows(q)], 9 + q, partner)

    def forward(q):
        return send(va.at[quarter_rows(q)], vpa.at[quarter_rows(q)], 12 + q, partner)

    def reduce_a(q):
        red_a(q).wait_recv()
        ua[quarter_rows(q), :] = (mine_a[q] + got_a[q].astype(F32)).astype(BF16)
        cross(q).start()
        up_a(q).start()

    lane = lax.broadcasted_iota(jnp.int32, (nst, 128), 1)
    row = lax.broadcasted_iota(jnp.int32, (nst, 128), 0)

    def gated(rs, y):
        y = y + d_skip[layer:layer + 1, :] * xc_s[rs, :].astype(F32)
        return (y * silu(z_s[rs, :].astype(F32))).astype(BF16)

    def project(yg, first, dst, dtype):
        for t in range(half // NCH):
            j = first * (half // NCH) + t
            dst[:, t * NCH:(t + 1) * NCH] = jnp.dot(yg, out_tile(j)[...], preferred_element_type=F32).astype(dtype)

    for k in range(2):
        p_second(k).wait_recv()
        p = p_cs[k].astype(F32) + p_v[k].astype(F32)
        low = rms0(p[:rank]).astype(BF16)
        pre = lax.dot_general(low, w_dt[layer], (((0,), (0,)), ((), ())), preferred_element_type=F32)
        pre = pre + b_dt[layer:layer + 1, :]
        dt_s[...] = jnp.maximum(pre, 0.0) + jnp.log1p(jnp.exp(-jnp.abs(pre)))
        bc = jnp.concatenate([rms0(p[rank:rank + nst]), rms0(p[rank + nst:])], axis=0)
        bc_s[:, 0:2 * nst] = jnp.transpose(bc)
        if k == 1:
            reduce_a(1)

        def block(i, carry, k=k):
            st_copy(i + k * nblk).wait()
            local = pl.multiple_of(i * SB, SB)
            base = local + k * HALF
            dt = dt_s[pl.ds(local, SB), :]
            dtx = dt * xc_s[pl.ds(base, SB), :].astype(F32)
            bc = bc_s[pl.ds(local, SB), :]
            a2 = a_s[...]
            for b in range(SB):
                bcb = jnp.broadcast_to(bc[b:b + 1, :], (nst, 128))
                bcol = jnp.sum(jnp.where(lane == row, bcb, 0.0), axis=1, keepdims=True)
                ccol = jnp.sum(jnp.where(lane == row + nst, bcb, 0.0), axis=1, keepdims=True)
                s = jnp.exp2(dt[b:b + 1, :] * a2) * st[base + b] + dtx[b:b + 1, :] * bcol
                st[base + b] = s
                t = s * ccol
                part[b] = t[0:8] + t[8:16]
            for g in range(SB // 8):
                y_s[pl.ds(local + 8 * g, 8), :] = sublane_sums([part[8 * g + n] for n in range(8)])

            if k == 0:
                @pl.when(i == 2)
                def _():
                    p_middle(1)

                @pl.when(i == nblk // 2 - 1)
                def _():
                    for j in range(feat // NCH):
                        o_copy(j).wait()

                @pl.when(lax.rem(i, nblk // 2) == nblk // 2 - 1)
                def _():
                    q = i // (nblk // 2)
                    rs = pl.ds(pl.multiple_of(q * quarter, quarter), quarter)
                    yg = gated(rs, y_s[rs, :])
                    project(yg, 1 - core, theirs_a.at[q], BF16)
                    red_a(q).start()
                    project(yg, core, mine_a.at[q], F32)

                @pl.when(i == nblk // 2)
                def _():
                    reduce_a(0)

            return carry

        lax.fori_loop(0, nblk, block, 0)

    yg = gated(half_rows(1), y_s[...])
    project(yg, 1 - core, theirs_b, BF16)
    red_b.start()
    project(yg, core, mine_b, F32)
    cross(0).wait_recv()
    forward(0).start()
    red_b.wait_recv()
    ub[...] = (mine_b[...] + got_b[...].astype(F32)).astype(BF16)
    cross(1).wait_recv()
    forward(1).start()
    for q in range(2):
        up_a(q).wait_recv()
    for q in range(2):
        forward(q).wait_recv()
    for k in range(2):
        p_first(k).wait_send()
        p_second(k).wait_send()
        red_a(k).wait_send()
        cross(k).wait_send()
        up_a(k).wait_send()
        forward(k).wait_send()
    red_b.wait_send()
    for c in relays:
        c.wait_send()
    if not first:
        pltpu.make_async_copy(rbuf, r_out, lsem.at[4]).wait()


def layer_call(layer, residual, ready, weights, conv_st, state):
    norm_w, w_in, conv_w, conv_b, w_x, w_dt, b_dt, a_log, d_skip, w_out = weights
    first = ready is None
    rows, feat = residual.shape
    chan = w_in.shape[3]
    nst = a_log.shape[1]
    half = feat // 2
    nproj = w_x.shape[1]
    nchunk = chan // NCH
    flat = [] if first else [pltpu.with_memory_space_constraint(a, pltpu.VMEM) for a in ready]
    held = rows if first else HALF
    args = [residual] + flat + [norm_w, w_in, conv_w, conv_b, w_x, conv_st, w_dt, b_dt, a_log, d_skip, w_out, state]
    specs = [ANY] + [VMEM] * len(flat) + [VMEM, ANY, VMEM, VMEM, VMEM, ANY, VMEM, VMEM, VMEM, VMEM, ANY, ANY]
    piece = pltpu.VMEM((HALF, half), BF16)
    outs = [pltpu.VMEM((rows, nst, chan), F32), pltpu.VMEM((3, held, chan), BF16)] + [piece] * 5
    out_specs = [VMEM] * 7
    if not first:
        outs.append(jax.ShapeDtypeStruct((HALF, feat), F32))
        out_specs.append(ANY)
    vm = pltpu.VMEM
    dma = pltpu.SemaphoreType.DMA
    quarter = HALF // 2
    return pl.pallas_call(
        functools.partial(layer_kernel, layer, first),
        out_shape=outs, in_specs=specs, out_specs=out_specs,
        scratch_shapes=[
            vm((nchunk, 2 * feat, NCH), BF16), vm((HALF, feat), BF16), vm((HALF, feat), BF16), vm((128, 128), BF16),
            vm((2, nproj, HALF), BF16), vm((2, nproj, HALF), BF16), vm((2, nproj, HALF), BF16),
            vm((2, nproj, HALF), BF16), vm((held, feat), F32), vm((held, chan), BF16), vm((rows, chan), BF16),
            vm((rows, chan), BF16), vm((HALF, chan), F32), vm((HALF, 128), F32), vm((nst, chan), F32), vm((HALF, chan), F32),
            vm((SB, 8, chan), F32), vm((2, quarter, half), F32), vm((HALF, half), F32), vm((2, quarter, half), BF16),
            vm((HALF, half), BF16), vm((2, quarter, half), BF16), vm((HALF, half), BF16), vm((HALF, half), BF16),
            vm((HALF, half), BF16),
            dma((5,)), dma((nchunk,)), dma((rows // SB,)), dma((feat // NCH,)), dma((15,)), dma((15,)),
        ],
        compiler_params=pltpu.CompilerParams(vmem_limit_bytes=34 * 2 ** 20, collective_id=layer, has_side_effects=True),
        cost_estimate=pl.CostEstimate(flops=2 * 10 ** 10, bytes_accessed=46 * 2 ** 20, transcendentals=0),
    )(*args)


def mid_kernel(layer, st, cw, res, ua, upa, va, vpa, norm_w, w_in, conv_w, conv_b, w_x, conv_st,
               ssm_out, conv_out, z_a, xc_a, p_a, cw_a, r_a,
               wbuf, hx, hbuf, ex_s, rbuf, cold, lsem, wsem, sem):
    feat = rbuf.shape[1]
    nchunk = wbuf.shape[0]
    nxt = layer + 1
    w_flat = w_in.reshape(w_in.shape[0], 2 * feat, w_in.shape[3])
    rows_a = pl.ds(0, HALF)

    def w_copy(c):
        return pltpu.make_async_copy(w_flat.at[nxt, :, cols_of(c)], wbuf.at[c], wsem.at[c])

    def st_copy(i):
        rs = pl.ds(i * SB, SB)
        return pltpu.make_async_copy(st.at[rs], ssm_out.at[layer, rs], sem.at[i])

    nst = st.shape[0] // SB
    r_copy = pltpu.make_async_copy(res.at[rows_a], rbuf, lsem.at[0])
    old_copy = pltpu.make_async_copy(conv_st.at[nxt, 0, rows_a], cold, lsem.at[1])
    win_copy = pltpu.make_async_copy(conv_st.at[nxt, pl.ds(1, 2), rows_a], cw_a.at[pl.ds(0, 2)], lsem.at[2])
    r_back = pltpu.make_async_copy(rbuf, r_a, lsem.at[3])
    c_copy = pltpu.make_async_copy(cw, conv_out.at[layer], lsem.at[4])
    r_copy.start()
    w_copy(0).start()
    old_copy.start()
    win_copy.start()
    w_copy(1).start()
    w_copy(2).start()
    ex_s[...] = order_matrix()
    core = lax.rem(lax.axis_index('tp'), 2)
    r_copy.wait()
    w_copy(3).start()
    st_copy(nst - 1).start()
    c_copy.start()
    add_pieces(rbuf, 0, halves_of(core, feat // 2), ua, upa, va, vpa)
    r_back.start()
    norm_expand(rbuf, 0, norm_w[nxt:nxt + 1, :], hbuf, ex_s, hx)
    old_copy.wait()
    win_copy.wait()
    window = (cold, cw_a.at[0], cw_a.at[1], cw_a.at[2])

    def chunk(c, carry):
        w_copy(c).wait()

        @pl.when(c + 4 < nchunk)
        def _():
            w_copy(c + 4).start()

        split_rows(wbuf, c)
        for t in range(3):
            st_copy(3 * c + t).start()
        in_chunk(nxt, c, hx, wbuf, conv_w, conv_b, window, z_a, xc_a)
        return carry

    lax.fori_loop(0, nchunk, chunk, 0)
    p_a[...] = x_project(w_x[nxt], xc_a[...])
    c_copy.wait()
    r_back.wait()
    for i in range(nst):
        st_copy(i).wait()


def mid_call(layer, st, cw, residual, pieces, weights, conv_st, shapes):
    norm_w, w_in, conv_w, conv_b, w_x = weights[:5]
    feat = residual.shape[1]
    chan = w_in.shape[3]
    nchunk = chan // NCH
    vm = pltpu.VMEM
    dma = pltpu.SemaphoreType.DMA
    st, cw, *pieces = [pltpu.with_memory_space_constraint(a, pltpu.VMEM) for a in (st, cw, *pieces)]
    args = [st, cw, residual, *pieces, norm_w, w_in, conv_w, conv_b, w_x, conv_st]
    return pl.pallas_call(
        functools.partial(mid_kernel, layer),
        out_shape=[jax.ShapeDtypeStruct(shapes[0], F32), jax.ShapeDtypeStruct(shapes[1], BF16),
                   vm((HALF, chan), BF16), vm((HALF, chan), BF16), vm((w_x.shape[1], HALF), BF16),
                   vm((3, HALF, chan), BF16), jax.ShapeDtypeStruct((HALF, feat), F32)],
        in_specs=[VMEM, VMEM, ANY] + [VMEM] * 4 + [VMEM, ANY, VMEM, VMEM, VMEM, ANY],
        out_specs=[ANY, ANY, VMEM, VMEM, VMEM, VMEM, ANY],
        scratch_shapes=[vm((nchunk, 2 * feat, NCH), BF16), vm((HALF, feat), BF16), vm((HALF, feat), BF16),
                        vm((128, 128), BF16), vm((HALF, feat), F32), vm((HALF, chan), BF16),
                        dma((5,)), dma((nchunk,)), dma((st.shape[0] // SB,))],
        compiler_params=pltpu.CompilerParams(vmem_limit_bytes=34 * 2 ** 20),
        cost_estimate=pl.CostEstimate(flops=2 * 10 ** 10, bytes_accessed=42 * 2 ** 20, transcendentals=0),
    )(*args)


def w_kernel(layer, st, cw_a, cw_b, ssm_prev, conv_prev, ssm_out, conv_out, sem):
    def copy(i):
        rs = pl.ds(i * SB, SB)
        return pltpu.make_async_copy(st.at[rs], ssm_out.at[layer, rs], sem.at[i])

    n = st.shape[0] // SB
    copies = [copy(i) for i in range(n)]
    for k, src in enumerate((cw_a, cw_b)):
        copies.append(pltpu.make_async_copy(src, conv_out.at[layer, :, pl.ds(k * HALF, HALF)], sem.at[n + k]))
    for c in copies:
        c.start()
    for c in copies:
        c.wait()


def w_call(layer, st, cw_a, cw_b, prev):
    args = [pltpu.with_memory_space_constraint(a, pltpu.VMEM) for a in (st, cw_a, cw_b)]
    return pl.pallas_call(
        functools.partial(w_kernel, layer),
        out_shape=[jax.ShapeDtypeStruct(a.shape, a.dtype) for a in prev],
        in_specs=[VMEM, VMEM, VMEM, ANY, ANY], out_specs=[ANY, ANY], input_output_aliases={3: 0, 4: 1},
        scratch_shapes=[pltpu.SemaphoreType.DMA((st.shape[0] // SB + 2,))],
        compiler_params=pltpu.CompilerParams(vmem_limit_bytes=2 ** 20),
        cost_estimate=pl.CostEstimate(flops=2 * 10 ** 10, bytes_accessed=42 * 2 ** 20, transcendentals=0),
    )(*args, *prev)


def fin_kernel(r_a, r_b, *refs):
    out = refs[-1]
    core = lax.rem(lax.axis_index('tp'), 2)
    half = out.shape[1] // 2
    lo = pl.ds(pl.multiple_of(core * half, 128), half)
    hi = pl.ds(pl.multiple_of((1 - core) * half, 128), half)
    for k in range(2):
        u, up, v, vp = refs[4 * k:4 * k + 4]
        rs = slice(k * HALF, (k + 1) * HALF)
        r = (r_a, r_b)[k]
        out[rs, lo] = r[:, lo] + (u[...].astype(F32) + v[...].astype(F32))
        out[rs, hi] = r[:, hi] + (up[...].astype(F32) + vp[...].astype(F32))


def fin_call(r_a, r_b, pieces):
    return pl.pallas_call(
        fin_kernel, out_shape=jax.ShapeDtypeStruct((2 * HALF, r_a.shape[1]), F32), in_specs=[VMEM] * 10, out_specs=VMEM,
        compiler_params=pltpu.CompilerParams(vmem_limit_bytes=16 * 2 ** 20), name="fin",
    )(r_a, r_b, *pieces[0], *pieces[1])


PART = [(0, 1), (1, 0), (2, 3), (3, 2)]
CROSS = [(0, 2), (2, 0), (1, 3), (3, 1)]


def solution(mesh):
    def step(residual, norm_w, w_in, conv_w, conv_b, w_x, w_dt, b_dt, a_log, d_skip, w_out, conv_state, ssm_state):
        w_xt = jnp.transpose(w_x, (0, 2, 1))
        conv_t = jnp.transpose(conv_state, (0, 2, 1, 3))
        weights = (norm_w, w_in, conv_w, conv_b, w_xt, w_dt, b_dt, a_log, d_skip, w_out)
        shapes = (ssm_state.shape, conv_t.shape)
        st, cw, ua, ub, upa, va, vpa = layer_call(0, residual, None, weights, conv_t, ssm_state)
        vb = lax.ppermute(ub, 'tp', CROSS)
        *written, z_a, xc_a, p_a, cw_a, r_a = mid_call(0, st, cw, residual, (ua, upa, va, vpa), weights, conv_t, shapes)
        ready = (ub, vb, z_a, xc_a, p_a)
        st, cw_b, ua, ub, upa, va, vpa, r_b = layer_call(1, residual, ready, weights, conv_t, ssm_state)
        vb = lax.ppermute(ub, 'tp', CROSS)
        upb = lax.ppermute(ub, 'tp', PART)
        ssm_out, conv_out = w_call(1, st, cw_a, cw_b, written)
        vpb = lax.ppermute(vb, 'tp', PART)
        out = fin_call(r_a, r_b, ((ua, upa, va, vpa), (ub, upb, vb, vpb)))
        return out, jnp.transpose(conv_out, (0, 2, 1, 3)), ssm_out

    cache_spec = P(None, 'dp', None, 'tp')
    in_specs = (P('dp', None), P(None, None), P(None, None, None, 'tp'), P(None, None, 'tp'), P(None, 'tp'), P(None, 'tp', None), P(None, None, 'tp'), P(None, 'tp'), P(None, None, 'tp'), P(None, 'tp'), P(None, 'tp', None), cache_spec, cache_spec)
    out_specs = (P('dp', None), cache_spec, cache_spec)
    return jax.shard_map(step, mesh=mesh, in_specs=in_specs, out_specs=out_specs, check_vma=False)
```

```python
import functools
import math

import jax
import jax.numpy as jnp
from jax import lax
from jax.experimental import pallas as pl
from jax.experimental.pallas import tpu as pltpu
from jax.sharding import PartitionSpec as P


F32 = jnp.float32
BF16 = jnp.bfloat16
ANY = pl.BlockSpec(memory_space=pltpu.HBM)
VMEM = pl.BlockSpec(memory_space=pltpu.VMEM)
NCH = 256
SB = 16
HALF = 128
SPLIT = 512
LOG2E = math.log2(math.e)
MESH = pl.DeviceIdType.MESH


def silu(v):
    return v * jax.nn.sigmoid(v)


def order_matrix():
    row = lax.broadcasted_iota(jnp.int32, (128, 128), 0)
    col = lax.broadcasted_iota(jnp.int32, (128, 128), 1)
    low = col & 7
    source = col - low + (low >> 1) + 4 * (low & 1)
    return jnp.where(row == source, 1.0, 0.0).astype(BF16)


def split_rows(wbuf, c):
    even = (lax.broadcasted_iota(jnp.int32, (SPLIT // 16, 8, NCH), 1) & 1) == 0

    def block(b, carry):
        start = b * SPLIT
        v = wbuf[c, pl.ds(start, SPLIT), :].astype(F32).reshape(SPLIT // 16, 2, 8, NCH)
        first, second = v[:, 0], v[:, 1]
        x = jnp.where(even, first, pltpu.roll(second, 1, 1))
        z = jnp.where(even, pltpu.roll(first, 7, 1), second)
        wbuf[c, pl.ds(start, SPLIT // 2), :] = x.reshape(SPLIT // 2, NCH).astype(BF16)
        wbuf[c, pl.ds(start + SPLIT // 2, SPLIT // 2), :] = z.reshape(SPLIT // 2, NCH).astype(BF16)
        return carry

    for b in range(wbuf.shape[1] // SPLIT):
        block(b, 0)


def split_half(wbuf, c, side):
    half = SPLIT // 2
    return jnp.concatenate([wbuf[c, b * SPLIT + side * half:b * SPLIT + (side + 1) * half, :]
                            for b in range(wbuf.shape[1] // SPLIT)], axis=0)


def rms0(v):
    return v * lax.rsqrt(jnp.mean(v * v, axis=0, keepdims=True) + 1e-6)


def sublane_sums(parts):
    sub = lax.broadcasted_iota(jnp.int32, parts[0].shape, 0)
    for step in (4, 2, 1):
        keep = (sub & step) == 0
        half = len(parts) // 2
        parts = [jnp.where(keep, parts[k], parts[k + half])
                 + pltpu.roll(jnp.where(keep, parts[k + half], parts[k]), step, 0) if step == 4 else
                 jnp.where(keep, parts[k], parts[k + half])
                 + jnp.where(keep, pltpu.roll(parts[k], 8 - step, 0), pltpu.roll(parts[k + half], step, 0))
                 for k in range(half)]
    return parts[0]


def add_pieces(rbuf, start, sides, u, up, v, vp):
    lo, hi = sides

    def add(i, carry):
        src = pl.ds(pl.multiple_of(i * 32, 32), 32)
        dst = pl.ds(pl.multiple_of(i * 32, 32) + start, 32)
        rbuf[dst, lo] = rbuf[dst, lo] + (u[src, :].astype(F32) + v[src, :].astype(F32))
        rbuf[dst, hi] = rbuf[dst, hi] + (up[src, :].astype(F32) + vp[src, :].astype(F32))
        return carry

    lax.fori_loop(0, HALF // 32, add, 0, unroll=True)


def norm_expand(rbuf, start, norm_row, hbuf, ex_s, hx):
    nw = norm_row.astype(F32)
    feat = rbuf.shape[1]

    def norm(i, carry):
        off = pl.multiple_of(i * 32, 32)
        r = rbuf[pl.ds(off + start, 32), :]
        inv = lax.rsqrt(jnp.mean(r * r, axis=-1, keepdims=True) + 1e-5)
        hbuf[pl.ds(off, 32), :] = (r * inv * nw).astype(BF16)
        return carry

    lax.fori_loop(0, HALF // 32, norm, 0, unroll=True)

    def expand(j, carry):
        for t in range(4):
            cols = pl.ds(pl.multiple_of(j * 512 + t * 128, 128), 128)
            hx[:, cols] = jnp.dot(hbuf[:, cols], ex_s[...], preferred_element_type=F32).astype(BF16)
        return carry

    lax.fori_loop(0, feat // 512, expand, 0, unroll=True)


def cols_of(c):
    return pl.ds(pl.multiple_of(c * NCH, NCH), NCH)


def in_chunk(layer, c, hx, wbuf, conv_w, conv_b, window, z_out, xc_out):
    old0, old1, old2, x_out = window
    sl = cols_of(c)
    x = jnp.dot(hx[...], split_half(wbuf, c, 0), preferred_element_type=F32).astype(BF16)
    z_out[:, sl] = jnp.dot(hx[...], split_half(wbuf, c, 1), preferred_element_type=F32).astype(BF16)
    x_out[:, sl] = x
    taps = conv_w[layer, :, sl].astype(F32)
    pre = old0[:, sl].astype(F32) * taps[0:1] + old1[:, sl].astype(F32) * taps[1:2]
    pre = pre + old2[:, sl].astype(F32) * taps[2:3] + x.astype(F32) * taps[3:4]
    pre = pre + conv_b[layer:layer + 1, sl].astype(F32)
    xc_out[:, sl] = silu(pre).astype(BF16)


def x_project(w_x_layer, xc):
    return lax.dot_general(w_x_layer, xc, (((1,), (1,)), ((), ())), preferred_element_type=F32).astype(BF16)


def halves_of(core, half):
    return (pl.ds(pl.multiple_of(core * half, 128), half), pl.ds(pl.multiple_of((1 - core) * half, 128), half))


def layer_kernel(layer, first, *refs):
    refs = list(refs)
    res = refs.pop(0)
    if not first:
        ub_in, vb_in, z_a, xc_a, p_a = refs[:5]
        refs = refs[5:]
    (norm_w, w_in, conv_w, conv_b, w_x, conv_st, w_dt, b_dt, a_log, d_skip, w_out, state) = refs[:12]
    refs = refs[12:]
    st, cw, ua, ub, upa, va, vpa = refs[:7]
    refs = refs[7:]
    r_out = None if first else refs.pop(0)
    (wbuf, hx, hbuf, ex_s, p_own, p_sw, p_cs, p_v, rbuf, cold, z_s, xc_s, dt_s, bc_s, a_s, y_s, part,
     mine_a, mine_b, theirs_a, theirs_b, got_a, got_b, upb, vpb, lsem, wsem, stsem, osem, ssem, rsem) = refs
    feat = rbuf.shape[1]
    nchunk = wbuf.shape[0]
    chan = z_s.shape[1]
    rank = w_dt.shape[1]
    nst = a_s.shape[0]
    nblk = HALF // SB
    half = feat // 2
    quarter = HALF // 2
    w_flat = w_in.reshape(w_in.shape[0], 2 * feat, w_in.shape[3])
    in_halves = (0, 1) if first else (1,)

    me = lax.axis_index('tp')
    core = lax.rem(me, 2)
    partner = me + 1 - 2 * core
    other = lax.rem(me + 2, 4)
    barrier = pltpu.get_barrier_semaphore()
    for dev in (partner, other):
        pl.semaphore_signal(barrier, inc=1, device_id={'tp': dev}, device_id_type=MESH)

    def send(src, dst, k, dev):
        return pltpu.make_async_remote_copy(src_ref=src, dst_ref=dst, send_sem=ssem.at[k], recv_sem=rsem.at[k],
                                            device_id={'tp': dev}, device_id_type=MESH)

    def half_rows(k):
        return pl.ds(k * HALF, HALF)

    def held_rows(k):
        return pl.ds(k * HALF if first else 0, HALF)

    def r_copy(k):
        return pltpu.make_async_copy(res.at[half_rows(k)], rbuf.at[held_rows(k)], lsem.at[k])

    nwin = cold.shape[0]
    win_rows = pl.ds(0 if first else HALF, nwin)
    old_copy = pltpu.make_async_copy(conv_st.at[layer, 0, win_rows], cold, lsem.at[2])
    win_copy = pltpu.make_async_copy(conv_st.at[layer, pl.ds(1, 2), win_rows], cw.at[pl.ds(0, 2)], lsem.at[3])

    def w_copy(c):
        return pltpu.make_async_copy(w_flat.at[layer, :, cols_of(c)], wbuf.at[c], wsem.at[c])

    def st_copy(i):
        rs = pl.ds(i * SB, SB)
        return pltpu.make_async_copy(state.at[layer, rs], st.at[rs], stsem.at[i])

    def out_tile(j):
        return wbuf.at[j // 4, pl.ds(pl.multiple_of(lax.rem(j, 4) * chan, 128), chan)]

    def o_copy(j):
        return pltpu.make_async_copy(w_out.at[layer, :, cols_of(j)], out_tile(j), osem.at[j])

    r_copy(in_halves[0]).start()
    w_copy(0).start()
    if first:
        r_copy(1).start()
    w_copy(1).start()
    old_copy.start()
    win_copy.start()
    w_copy(2).start()
    ex_s[...] = order_matrix()
    a_s[...] = -jnp.exp(a_log[layer]) * LOG2E
    pl.semaphore_wait(barrier, 2)
    relays = []
    if not first:
        relays = [send(vb_in, vpb, 11, partner), send(ub_in, upb, 14, partner)]
        for c in relays:
            c.start()

    def p_first(k):
        return send(p_own.at[k], p_sw.at[k], k, partner)

    def p_second(k):
        return send(p_cs.at[k], p_v.at[k], 2 + k, other)

    def p_middle(k):
        p_first(k).wait_recv()
        p_cs[k] = (p_own[k].astype(F32) + p_sw[k].astype(F32)).astype(BF16)
        p_second(k).start()

    if not first:
        p_own[0] = p_a[...]
        p_first(0).start()
        xc_s[0:HALF, :] = xc_a[...]
        z_s[0:HALF, :] = z_a[...]
    for k in in_halves:
        start = k * HALF if first else 0
        r_copy(k).wait()
        if not first:
            for c in relays:
                c.wait_recv()
            add_pieces(rbuf, start, halves_of(core, half), ub_in, upb, vb_in, vpb)
            pltpu.make_async_copy(rbuf, r_out, lsem.at[4]).start()
        norm_expand(rbuf, start, norm_w[layer:layer + 1, :], hbuf, ex_s, hx)
        if k == in_halves[0]:
            old_copy.wait()
            win_copy.wait()

        def chunk(c, carry, k=k):
            if k == in_halves[0]:
                w_copy(c).wait()

                @pl.when(c + 3 < nchunk)
                def _():
                    w_copy(c + 3).start()

                split_rows(wbuf, c)

            if k == 1:
                for t in range(3):
                    st_copy(3 * c + t).start()
            held = held_rows(k)
            window = (cold.at[held], cw.at[0, held], cw.at[1, held], cw.at[2, held])
            in_chunk(layer, c, hx, wbuf, conv_w, conv_b, window, z_s.at[half_rows(k)], xc_s.at[half_rows(k)])
            if k == 1:
                @pl.when(c < 2)
                def _():
                    for t in range(4):
                        o_copy(4 * c + t).start()

                @pl.when(c == 2)
                def _():
                    for t in range(2):
                        o_copy(8 + t).start()
                    p_middle(0)

            return carry

        lax.fori_loop(0, nchunk, chunk, 0)
        p_own[k] = x_project(w_x[layer], xc_s[half_rows(k), :])
        p_first(k).start()
    st_copy(2 * nblk - 1).start()

    def red_a(q):
        return send(theirs_a.at[q], got_a.at[q], 4 + q, partner)

    red_b = send(theirs_b, got_b, 6, partner)

    def quarter_rows(q):
        return pl.ds(q * quarter, quarter)

    def cross(q):
        return send(ua.at[quarter_rows(q)], va.at[quarter_rows(q)], 7 + q, other)

    def up_a(q):
        return send(ua.at[quarter_rows(q)], upa.at[quarter_rows(q)], 9 + q, partner)

    def forward(q):
        return send(va.at[quarter_rows(q)], vpa.at[quarter_rows(q)], 12 + q, partner)

    def reduce_a(q):
        red_a(q).wait_recv()
        ua[quarter_rows(q), :] = (mine_a[q] + got_a[q].astype(F32)).astype(BF16)
        cross(q).start()
        up_a(q).start()

    lane = lax.broadcasted_iota(jnp.int32, (nst, 128), 1)
    row = lax.broadcasted_iota(jnp.int32, (nst, 128), 0)

    def gated(rs, y):
        y = y + d_skip[layer:layer + 1, :] * xc_s[rs, :].astype(F32)
        return (y * silu(z_s[rs, :].astype(F32))).astype(BF16)

    def project(yg, first, dst, dtype):
        for t in range(half // NCH):
            j = first * (half // NCH) + t
            dst[:, t * NCH:(t + 1) * NCH] = jnp.dot(yg, out_tile(j)[...], preferred_element_type=F32).astype(dtype)

    for k in range(2):
        p_second(k).wait_recv()
        p = p_cs[k].astype(F32) + p_v[k].astype(F32)
        low = rms0(p[:rank]).astype(BF16)
        pre = lax.dot_general(low, w_dt[layer], (((0,), (0,)), ((), ())), preferred_element_type=F32)
        pre = pre + b_dt[layer:layer + 1, :]
        dt_s[...] = jnp.maximum(pre, 0.0) + jnp.log1p(jnp.exp(-jnp.abs(pre)))
        bc = jnp.concatenate([rms0(p[rank:rank + nst]), rms0(p[rank + nst:])], axis=0)
        bc_s[:, 0:2 * nst] = jnp.transpose(bc)
        if k == 1:
            reduce_a(1)

        def block(i, carry, k=k):
            st_copy(i + k * nblk).wait()
            local = pl.multiple_of(i * SB, SB)
            base = local + k * HALF
            dt = dt_s[pl.ds(local, SB), :]
            dtx = dt * xc_s[pl.ds(base, SB), :].astype(F32)
            bc = bc_s[pl.ds(local, SB), :]
            a2 = a_s[...]
            for b in range(SB):
                bcb = jnp.broadcast_to(bc[b:b + 1, :], (nst, 128))
                bcol = jnp.sum(jnp.where(lane == row, bcb, 0.0), axis=1, keepdims=True)
                ccol = jnp.sum(jnp.where(lane == row + nst, bcb, 0.0), axis=1, keepdims=True)
                s = jnp.exp2(dt[b:b + 1, :] * a2) * st[base + b] + dtx[b:b + 1, :] * bcol
                st[base + b] = s
                t = s * ccol
                part[b] = t[0:8] + t[8:16]
            for g in range(SB // 8):
                y_s[pl.ds(local + 8 * g, 8), :] = sublane_sums([part[8 * g + n] for n in range(8)])

            if k == 0:
                @pl.when(i == 2)
                def _():
                    p_middle(1)

                @pl.when(i == nblk // 2 - 1)
                def _():
                    for j in range(feat // NCH):
                        o_copy(j).wait()

                @pl.when(lax.rem(i, nblk // 2) == nblk // 2 - 1)
                def _():
                    q = i // (nblk // 2)
                    rs = pl.ds(pl.multiple_of(q * quarter, quarter), quarter)
                    yg = gated(rs, y_s[rs, :])
                    project(yg, 1 - core, theirs_a.at[q], BF16)
                    red_a(q).start()
                    project(yg, core, mine_a.at[q], F32)

                @pl.when(i == nblk // 2)
                def _():
                    reduce_a(0)

            return carry

        lax.fori_loop(0, nblk, block, 0)

    yg = gated(half_rows(1), y_s[...])
    project(yg, 1 - core, theirs_b, BF16)
    red_b.start()
    project(yg, core, mine_b, F32)
    cross(0).wait_recv()
    forward(0).start()
    red_b.wait_recv()
    ub[...] = (mine_b[...] + got_b[...].astype(F32)).astype(BF16)
    cross(1).wait_recv()
    forward(1).start()
    for q in range(2):
        up_a(q).wait_recv()
    for q in range(2):
        forward(q).wait_recv()
    for k in range(2):
        p_first(k).wait_send()
        p_second(k).wait_send()
        red_a(k).wait_send()
        cross(k).wait_send()
        up_a(k).wait_send()
        forward(k).wait_send()
    red_b.wait_send()
    for c in relays:
        c.wait_send()
    if not first:
        pltpu.make_async_copy(rbuf, r_out, lsem.at[4]).wait()


def layer_call(layer, residual, ready, weights, conv_st, state):
    norm_w, w_in, conv_w, conv_b, w_x, w_dt, b_dt, a_log, d_skip, w_out = weights
    first = ready is None
    rows, feat = residual.shape
    chan = w_in.shape[3]
    nst = a_log.shape[1]
    half = feat // 2
    nproj = w_x.shape[1]
    nchunk = chan // NCH
    flat = [] if first else [pltpu.with_memory_space_constraint(a, pltpu.VMEM) for a in ready]
    held = rows if first else HALF
    args = [residual] + flat + [norm_w, w_in, conv_w, conv_b, w_x, conv_st, w_dt, b_dt, a_log, d_skip, w_out, state]
    specs = [ANY] + [VMEM] * len(flat) + [VMEM, ANY, VMEM, VMEM, VMEM, ANY, VMEM, VMEM, VMEM, VMEM, ANY, ANY]
    piece = pltpu.VMEM((HALF, half), BF16)
    outs = [pltpu.VMEM((rows, nst, chan), F32), pltpu.VMEM((3, held, chan), BF16)] + [piece] * 5
    out_specs = [VMEM] * 7
    if not first:
        outs.append(jax.ShapeDtypeStruct((HALF, feat), F32))
        out_specs.append(ANY)
    vm = pltpu.VMEM
    dma = pltpu.SemaphoreType.DMA
    quarter = HALF // 2
    return pl.pallas_call(
        functools.partial(layer_kernel, layer, first),
        out_shape=outs, in_specs=specs, out_specs=out_specs,
        scratch_shapes=[
            vm((nchunk, 2 * feat, NCH), BF16), vm((HALF, feat), BF16), vm((HALF, feat), BF16), vm((128, 128), BF16),
            vm((2, nproj, HALF), BF16), vm((2, nproj, HALF), BF16), vm((2, nproj, HALF), BF16),
            vm((2, nproj, HALF), BF16), vm((held, feat), F32), vm((held, chan), BF16), vm((rows, chan), BF16),
            vm((rows, chan), BF16), vm((HALF, chan), F32), vm((HALF, 128), F32), vm((nst, chan), F32), vm((HALF, chan), F32),
            vm((SB, 8, chan), F32), vm((2, quarter, half), F32), vm((HALF, half), F32), vm((2, quarter, half), BF16),
            vm((HALF, half), BF16), vm((2, quarter, half), BF16), vm((HALF, half), BF16), vm((HALF, half), BF16),
            vm((HALF, half), BF16),
            dma((5,)), dma((nchunk,)), dma((rows // SB,)), dma((feat // NCH,)), dma((15,)), dma((15,)),
        ],
        compiler_params=pltpu.CompilerParams(vmem_limit_bytes=34 * 2 ** 20, collective_id=layer, has_side_effects=True),
        cost_estimate=pl.CostEstimate(flops=2 * 10 ** 10, bytes_accessed=46 * 2 ** 20, transcendentals=0),
    )(*args)


def mid_kernel(layer, st, cw, res, ua, upa, va, vpa, norm_w, w_in, conv_w, conv_b, w_x, conv_st,
               ssm_out, conv_out, z_a, xc_a, p_a, cw_a, r_a,
               wbuf, hx, hbuf, ex_s, rbuf, cold, lsem, wsem, sem):
    feat = rbuf.shape[1]
    nchunk = wbuf.shape[0]
    nxt = layer + 1
    w_flat = w_in.reshape(w_in.shape[0], 2 * feat, w_in.shape[3])
    rows_a = pl.ds(0, HALF)

    def w_copy(c):
        return pltpu.make_async_copy(w_flat.at[nxt, :, cols_of(c)], wbuf.at[c], wsem.at[c])

    def st_copy(i):
        rs = pl.ds(i * SB, SB)
        return pltpu.make_async_copy(st.at[rs], ssm_out.at[layer, rs], sem.at[i])

    nst = st.shape[0] // SB
    r_copy = pltpu.make_async_copy(res.at[rows_a], rbuf, lsem.at[0])
    old_copy = pltpu.make_async_copy(conv_st.at[nxt, 0, rows_a], cold, lsem.at[1])
    win_copy = pltpu.make_async_copy(conv_st.at[nxt, pl.ds(1, 2), rows_a], cw_a.at[pl.ds(0, 2)], lsem.at[2])
    r_back = pltpu.make_async_copy(rbuf, r_a, lsem.at[3])
    c_copy = pltpu.make_async_copy(cw, conv_out.at[layer], lsem.at[4])
    r_copy.start()
    w_copy(0).start()
    old_copy.start()
    win_copy.start()
    w_copy(1).start()
    w_copy(2).start()
    ex_s[...] = order_matrix()
    core = lax.rem(lax.axis_index('tp'), 2)
    r_copy.wait()
    w_copy(3).start()
    st_copy(nst - 1).start()
    c_copy.start()
    add_pieces(rbuf, 0, halves_of(core, feat // 2), ua, upa, va, vpa)
    r_back.start()
    norm_expand(rbuf, 0, norm_w[nxt:nxt + 1, :], hbuf, ex_s, hx)
    old_copy.wait()
    win_copy.wait()
    window = (cold, cw_a.at[0], cw_a.at[1], cw_a.at[2])

    def chunk(c, carry):
        w_copy(c).wait()

        @pl.when(c + 4 < nchunk)
        def _():
            w_copy(c + 4).start()

        split_rows(wbuf, c)
        for t in range(3):
            st_copy(3 * c + t).start()
        in_chunk(nxt, c, hx, wbuf, conv_w, conv_b, window, z_a, xc_a)
        return carry

    lax.fori_loop(0, nchunk, chunk, 0)
    p_a[...] = x_project(w_x[nxt], xc_a[...])
    c_copy.wait()
    r_back.wait()
    for i in range(nst):
        st_copy(i).wait()


def mid_call(layer, st, cw, residual, pieces, weights, conv_st, shapes):
    norm_w, w_in, conv_w, conv_b, w_x = weights[:5]
    feat = residual.shape[1]
    chan = w_in.shape[3]
    nchunk = chan // NCH
    vm = pltpu.VMEM
    dma = pltpu.SemaphoreType.DMA
    st, cw, *pieces = [pltpu.with_memory_space_constraint(a, pltpu.VMEM) for a in (st, cw, *pieces)]
    args = [st, cw, residual, *pieces, norm_w, w_in, conv_w, conv_b, w_x, conv_st]
    return pl.pallas_call(
        functools.partial(mid_kernel, layer),
        out_shape=[jax.ShapeDtypeStruct(shapes[0], F32), jax.ShapeDtypeStruct(shapes[1], BF16),
                   vm((HALF, chan), BF16), vm((HALF, chan), BF16), vm((w_x.shape[1], HALF), BF16),
                   vm((3, HALF, chan), BF16), jax.ShapeDtypeStruct((HALF, feat), F32)],
        in_specs=[VMEM, VMEM, ANY] + [VMEM] * 4 + [VMEM, ANY, VMEM, VMEM, VMEM, ANY],
        out_specs=[ANY, ANY, VMEM, VMEM, VMEM, VMEM, ANY],
        scratch_shapes=[vm((nchunk, 2 * feat, NCH), BF16), vm((HALF, feat), BF16), vm((HALF, feat), BF16),
                        vm((128, 128), BF16), vm((HALF, feat), F32), vm((HALF, chan), BF16),
                        dma((5,)), dma((nchunk,)), dma((st.shape[0] // SB,))],
        compiler_params=pltpu.CompilerParams(vmem_limit_bytes=34 * 2 ** 20),
        cost_estimate=pl.CostEstimate(flops=2 * 10 ** 10, bytes_accessed=42 * 2 ** 20, transcendentals=0),
    )(*args)


def w_kernel(layer, st, cw_a, cw_b, ssm_prev, conv_prev, ssm_out, conv_out, sem):
    def copy(i):
        rs = pl.ds(i * SB, SB)
        return pltpu.make_async_copy(st.at[rs], ssm_out.at[layer, rs], sem.at[i])

    n = st.shape[0] // SB
    copies = [copy(i) for i in range(n)]
    for k, src in enumerate((cw_a, cw_b)):
        copies.append(pltpu.make_async_copy(src, conv_out.at[layer, :, pl.ds(k * HALF, HALF)], sem.at[n + k]))
    for c in copies:
        c.start()
    for c in copies:
        c.wait()


def w_call(layer, st, cw_a, cw_b, prev):
    args = [pltpu.with_memory_space_constraint(a, pltpu.VMEM) for a in (st, cw_a, cw_b)]
    return pl.pallas_call(
        functools.partial(w_kernel, layer),
        out_shape=[jax.ShapeDtypeStruct(a.shape, a.dtype) for a in prev],
        in_specs=[VMEM, VMEM, VMEM, ANY, ANY], out_specs=[ANY, ANY], input_output_aliases={3: 0, 4: 1},
        scratch_shapes=[pltpu.SemaphoreType.DMA((st.shape[0] // SB + 2,))],
        compiler_params=pltpu.CompilerParams(vmem_limit_bytes=2 ** 20),
        cost_estimate=pl.CostEstimate(flops=2 * 10 ** 10, bytes_accessed=42 * 2 ** 20, transcendentals=0),
    )(*args, *prev)


def fin_kernel(r_a, r_b, *refs):
    out = refs[-1]
    core = lax.rem(lax.axis_index('tp'), 2)
    half = out.shape[1] // 2
    lo = pl.ds(pl.multiple_of(core * half, 128), half)
    hi = pl.ds(pl.multiple_of((1 - core) * half, 128), half)
    for k in range(2):
        u, up, v, vp = refs[4 * k:4 * k + 4]
        rs = slice(k * HALF, (k + 1) * HALF)
        r = (r_a, r_b)[k]
        out[rs, lo] = r[:, lo] + (u[...].astype(F32) + v[...].astype(F32))
        out[rs, hi] = r[:, hi] + (up[...].astype(F32) + vp[...].astype(F32))


def fin_call(r_a, r_b, pieces):
    return pl.pallas_call(
        fin_kernel, out_shape=jax.ShapeDtypeStruct((2 * HALF, r_a.shape[1]), F32), in_specs=[VMEM] * 10, out_specs=VMEM,
        compiler_params=pltpu.CompilerParams(vmem_limit_bytes=16 * 2 ** 20), name="fin",
    )(r_a, r_b, *pieces[0], *pieces[1])


PART = [(0, 1), (1, 0), (2, 3), (3, 2)]
CROSS = [(0, 2), (2, 0), (1, 3), (3, 1)]


def solution(mesh):
    def step(residual, norm_w, w_in, conv_w, conv_b, w_x, w_dt, b_dt, a_log, d_skip, w_out, conv_state, ssm_state):
        w_xt = jnp.transpose(w_x, (0, 2, 1))
        conv_t = jnp.transpose(conv_state, (0, 2, 1, 3))
        weights = (norm_w, w_in, conv_w, conv_b, w_xt, w_dt, b_dt, a_log, d_skip, w_out)
        shapes = (ssm_state.shape, conv_t.shape)
        st, cw, ua, ub, upa, va, vpa = layer_call(0, residual, None, weights, conv_t, ssm_state)
        vb = lax.ppermute(ub, 'tp', CROSS)
        *written, z_a, xc_a, p_a, cw_a, r_a = mid_call(0, st, cw, residual, (ua, upa, va, vpa), weights, conv_t, shapes)
        ready = (ub, vb, z_a, xc_a, p_a)
        st, cw_b, ua, ub, upa, va, vpa, r_b = layer_call(1, residual, ready, weights, conv_t, ssm_state)
        vb = lax.ppermute(ub, 'tp', CROSS)
        upb = lax.ppermute(ub, 'tp', PART)
        ssm_out, conv_out = w_call(1, st, cw_a, cw_b, written)
        vpb = lax.ppermute(vb, 'tp', PART)
        out = fin_call(r_a, r_b, ((ua, upa, va, vpa), (ub, upb, vb, vpb)))
        return out, jnp.transpose(conv_out, (0, 2, 1, 3)), ssm_out

    cache_spec = P(None, 'dp', None, 'tp')
    in_specs = (P('dp', None), P(None, None), P(None, None, None, 'tp'), P(None, None, 'tp'), P(None, 'tp'), P(None, 'tp', None), P(None, None, 'tp'), P(None, 'tp'), P(None, None, 'tp'), P(None, 'tp'), P(None, 'tp', None), cache_spec, cache_spec)
    out_specs = (P('dp', None), cache_spec, cache_spec)
    return jax.shard_map(step, mesh=mesh, in_specs=in_specs, out_specs=out_specs, check_vma=False)
```
